128 devices in a mesh: z: 4 (over z), y: 4 (over y), xc: 8 (over x, core).
Axes of the slice: x: 4, y: 4, z: 4, core: 2. Of those that a mesh axis runs over, the one named last changes fastest.
Arguments:
- tokens_x: bfloat16 [32768, 1536], P(('z', 'y', 'xc'))
- grad_y: bfloat16 [32768, 1536], P(('z', 'y', 'xc'))
- w_one: bfloat16 [1536, 6144], replicated
- w_two: bfloat16 [6144, 1536], replicated
- w_three: bfloat16 [1536, 6144], replicated
- w_four: bfloat16 [6144, 1536], replicated
Outputs:
- output 1: float32 [1536, 6144], replicated
- output 2: float32 [6144, 1536], replicated
- output 3: float32 [1536, 6144], replicated
- output 4: float32 [6144, 1536], replicated
All inputs are finite; a program needn't handle non-finite values.
Results may differ from the reference program's by a relative error of at most 0.00433.
Values are sent between devices in bfloat16 or wider.
A program may use at most 1 GiB of HBM per device.

```python
import math
import jax
import jax.numpy as jnp
from jax import lax

D = 1536
FF = 6144
TOKENS_DEV = 256
DEVICES = 128

TOKENS = DEVICES * TOKENS_DEV
GELU_SCALE = math.sqrt(2.0 / math.pi)
GELU_CUBIC = 0.044715


def gelu_value(pre_act):
    return 0.5 * pre_act * (1.0 + jnp.tanh(GELU_SCALE * (pre_act + GELU_CUBIC * pre_act * pre_act * pre_act)))


def gelu_grad(pre_act):
    tanh_val = jnp.tanh(GELU_SCALE * (pre_act + GELU_CUBIC * pre_act * pre_act * pre_act))
    return 0.5 * (1.0 + tanh_val) + 0.5 * pre_act * (1.0 - tanh_val * tanh_val) * GELU_SCALE * (1.0 + 3.0 * GELU_CUBIC * pre_act * pre_act)


def setup_inputs(seed: int = 0) -> dict:
    root_key = jax.random.key(seed)
    key_list = jax.random.split(root_key, 8)
    scale_x = jax.random.uniform(key_list[0], (DEVICES, 1, 1), jnp.float32, 0.7, 1.3)
    scale_g = jax.random.uniform(key_list[1], (DEVICES, 1, 1), jnp.float32, 0.7, 1.3)
    x_rows = jax.random.normal(key_list[2], (DEVICES, TOKENS_DEV, D), jnp.float32) * scale_x
    g_rows = jax.random.normal(key_list[3], (DEVICES, TOKENS_DEV, D), jnp.float32) * scale_g
    w_one = jax.random.normal(key_list[4], (D, FF), jnp.float32) * D ** -0.5
    w_two = jax.random.normal(key_list[5], (FF, D), jnp.float32) * FF ** -0.5
    w_three = jax.random.normal(key_list[6], (D, FF), jnp.float32) * D ** -0.5
    w_four = jax.random.normal(key_list[7], (FF, D), jnp.float32) * FF ** -0.5
    return {
        "tokens_x": x_rows.reshape(TOKENS, D).astype(jnp.bfloat16),
        "grad_y": g_rows.reshape(TOKENS, D).astype(jnp.bfloat16),
        "w_one": w_one.astype(jnp.bfloat16),
        "w_two": w_two.astype(jnp.bfloat16),
        "w_three": w_three.astype(jnp.bfloat16),
        "w_four": w_four.astype(jnp.bfloat16),
    }


def local_grads(x_loc, g_loc, w_one, w_two, w_three, w_four):
    a_one = jnp.dot(x_loc, w_one, preferred_element_type=jnp.float32).astype(jnp.bfloat16)
    h_one = gelu_value(a_one.astype(jnp.float32)).astype(jnp.bfloat16)
    h_two = (jnp.dot(h_one, w_two, preferred_element_type=jnp.float32) + x_loc.astype(jnp.float32)).astype(jnp.bfloat16)
    a_three = jnp.dot(h_two, w_three, preferred_element_type=jnp.float32).astype(jnp.bfloat16)
    h_three = gelu_value(a_three.astype(jnp.float32)).astype(jnp.bfloat16)
    d_w4 = jnp.dot(h_three.T, g_loc, preferred_element_type=jnp.float32)
    d_a3 = (jnp.dot(g_loc, w_four.T, preferred_element_type=jnp.float32) * gelu_grad(a_three.astype(jnp.float32))).astype(jnp.bfloat16)
    d_w3 = jnp.dot(h_two.T, d_a3, preferred_element_type=jnp.float32)
    d_h2 = (jnp.dot(d_a3, w_three.T, preferred_element_type=jnp.float32) + g_loc.astype(jnp.float32)).astype(jnp.bfloat16)
    d_w2 = jnp.dot(h_one.T, d_h2, preferred_element_type=jnp.float32)
    d_a1 = (jnp.dot(d_h2, w_two.T, preferred_element_type=jnp.float32) * gelu_grad(a_one.astype(jnp.float32))).astype(jnp.bfloat16)
    d_w1 = jnp.dot(x_loc.T, d_a1, preferred_element_type=jnp.float32)
    return d_w1, d_w2, d_w3, d_w4


def reference(tokens_x, grad_y, w_one, w_two, w_three, w_four):
    x_shards = tokens_x.reshape(DEVICES, TOKENS_DEV, D)
    g_shards = grad_y.reshape(DEVICES, TOKENS_DEV, D)

    def accumulate(running, pair):
        x_loc, g_loc = pair
        grads = local_grads(x_loc, g_loc, w_one, w_two, w_three, w_four)
        return tuple(acc + new for acc, new in zip(running, grads)), None

    start_sums = (
        jnp.zeros((D, FF), jnp.float32),
        jnp.zeros((FF, D), jnp.float32),
        jnp.zeros((D, FF), jnp.float32),
        jnp.zeros((FF, D), jnp.float32),
    )
    totals, _ = lax.scan(accumulate, start_sums, (x_shards, g_shards))
    return (totals[0] / DEVICES, totals[1] / DEVICES, totals[2] / DEVICES, totals[3] / DEVICES)
```

```python
import functools
import math
import jax
import jax.numpy as jnp
from jax import lax
from jax.experimental import pallas as pl
from jax.experimental.pallas import tpu as pltpu
from jax.sharding import PartitionSpec as P

GELU_SCALE = math.sqrt(2.0 / math.pi)
GELU_CUBIC = 0.044715


def gelu_value(pre_act):
    return 0.5 * pre_act * (1.0 + jnp.tanh(GELU_SCALE * (pre_act + GELU_CUBIC * pre_act * pre_act * pre_act)))


def gelu_grad(pre_act):
    tanh_val = jnp.tanh(GELU_SCALE * (pre_act + GELU_CUBIC * pre_act * pre_act * pre_act))
    return 0.5 * (1.0 + tanh_val) + 0.5 * pre_act * (1.0 - tanh_val * tanh_val) * GELU_SCALE * (1.0 + 3.0 * GELU_CUBIC * pre_act * pre_act)


def place_kernel(moves, depth, *refs):
    n_src = len({m[0] for m in moves})
    srcs, dsts = refs[:n_src], refs[n_src:-3]
    slots, in_sem, out_sem = refs[-3:]

    def load(step):
        src, src_row, _, _, rows = moves[step]
        return pltpu.make_async_copy(srcs[src].at[pl.ds(src_row, rows)], slots.at[step % depth], in_sem.at[step % depth])

    def store(step):
        _, _, dst, dst_row, rows = moves[step]
        return pltpu.make_async_copy(slots.at[step % depth], dsts[dst].at[pl.ds(dst_row, rows)], out_sem.at[step % depth])

    ahead = depth // 2
    for step in range(min(ahead, len(moves))):
        load(step).start()
    for step in range(len(moves)):
        if step + ahead < len(moves):
            if step + ahead >= depth:
                store(step + ahead - depth).wait()
            load(step + ahead).start()
        load(step).wait()
        store(step).start()
    for step in range(max(0, len(moves) - depth), len(moves)):
        store(step).wait()


def place(src, n_dst, rows):
    total, width = src.shape
    out_rows = total // n_dst
    moves = [(0, row, row // out_rows, row % out_rows, rows) for row in range(0, total, rows)]
    depth = 6
    return pl.pallas_call(
        functools.partial(place_kernel, moves, depth),
        out_shape=[jax.ShapeDtypeStruct((out_rows, width), src.dtype)] * n_dst,
        in_specs=[pl.BlockSpec(memory_space=pl.ANY)],
        out_specs=[pl.BlockSpec(memory_space=pl.ANY)] * n_dst,
        scratch_shapes=[pltpu.VMEM((depth, rows, width), src.dtype), pltpu.SemaphoreType.DMA((depth,)), pltpu.SemaphoreType.DMA((depth,))],
        cost_estimate=pl.CostEstimate(flops=8 * src.size, bytes_accessed=8 * src.size, transcendentals=0),
    )(src)


def solution(mesh):
    n_dev = math.prod(mesh.shape.values())
    batch_spec = P(("z", "y", "xc"), None)
    whole_spec = P(None, None)

    axes = ("z", "y", "xc")

    def scatter_sum(local_grad):
        return lax.psum_scatter(local_grad, axes, scatter_dimension=0, tiled=True) * (1.0 / n_dev)

    def gather(part):
        return lax.all_gather(part, axes, axis=0, tiled=True)

    def device_step(x_loc, g_loc, w_one, w_two, w_three, w_four):
        a_one = jnp.dot(x_loc, w_one, preferred_element_type=jnp.float32).astype(jnp.bfloat16)
        h_one = gelu_value(a_one.astype(jnp.float32)).astype(jnp.bfloat16)
        h_two = (jnp.dot(h_one, w_two, preferred_element_type=jnp.float32) + x_loc.astype(jnp.float32)).astype(jnp.bfloat16)
        a_three = jnp.dot(h_two, w_three, preferred_element_type=jnp.float32).astype(jnp.bfloat16)
        h_three = gelu_value(a_three.astype(jnp.float32)).astype(jnp.bfloat16)
        part_w4 = scatter_sum(jnp.einsum("nf,nd->fd", h_three, g_loc, preferred_element_type=jnp.float32))
        d_a3 = (jnp.einsum("nd,fd->nf", g_loc, w_four, preferred_element_type=jnp.float32) * gelu_grad(a_three.astype(jnp.float32))).astype(jnp.bfloat16)
        local_w3 = jnp.einsum("nd,nf->df", h_two, d_a3, preferred_element_type=jnp.float32)
        d_h2 = (jnp.einsum("nf,df->nd", d_a3, w_three, preferred_element_type=jnp.float32) + g_loc.astype(jnp.float32)).astype(jnp.bfloat16)
        local_w2 = jnp.einsum("nf,nd->fd", h_one, d_h2, preferred_element_type=jnp.float32)
        d_a1 = (jnp.einsum("nd,fd->nf", d_h2, w_two, preferred_element_type=jnp.float32) * gelu_grad(a_one.astype(jnp.float32))).astype(jnp.bfloat16)
        local_w1 = jnp.einsum("nd,nf->df", x_loc, d_a1, preferred_element_type=jnp.float32)
        part_w4, local_w2 = lax.optimization_barrier((part_w4, local_w2))
        part_w2 = scatter_sum(local_w2)
        part_w2, local_w13 = lax.optimization_barrier((part_w2, jnp.concatenate([local_w1, local_w3], axis=0)))
        part_w13 = scatter_sum(local_w13)
        grad_w13 = gather(part_w13)
        part_w4, grad_w13 = lax.optimization_barrier((part_w4, grad_w13))
        grad_w4 = gather(part_w4)
        part_w2, grad_w4 = lax.optimization_barrier((part_w2, grad_w4))
        grad_w2 = gather(part_w2)
        grad_w1, grad_w3 = place(grad_w13, 2, 96)
        (grad_w4,) = place(grad_w4, 1, 384)
        (grad_w2,) = place(grad_w2, 1, 384)
        return grad_w1, grad_w2, grad_w3, grad_w4

    return jax.shard_map(
        device_step,
        mesh=mesh,
        in_specs=(batch_spec, batch_spec, whole_spec, whole_spec, whole_spec, whole_spec),
        out_specs=(whole_spec, whole_spec, whole_spec, whole_spec),
        check_vma=False,
    )
```

```python
import functools
import math
import jax
import jax.numpy as jnp
from jax import lax
from jax.experimental import pallas as pl
from jax.experimental.pallas import tpu as pltpu
from jax.sharding import PartitionSpec as P

GELU_SCALE = math.sqrt(2.0 / math.pi)
GELU_CUBIC = 0.044715
MESH = pl.DeviceIdType.MESH
RING = 4
PARTS = 3
CHUNKS = 4
BLOCKS = 3
PIECES = 3
LAST = 1


def gelu_value(pre_act):
    return 0.5 * pre_act * (1.0 + jnp.tanh(GELU_SCALE * (pre_act + GELU_CUBIC * pre_act * pre_act * pre_act)))


def gelu_grad(pre_act):
    tanh_val = jnp.tanh(GELU_SCALE * (pre_act + GELU_CUBIC * pre_act * pre_act * pre_act))
    return 0.5 * (1.0 + tanh_val) + 0.5 * pre_act * (1.0 - tanh_val * tanh_val) * GELU_SCALE * (1.0 + 3.0 * GELU_CUBIC * pre_act * pre_act)


def pick(index, values):
    chosen = values[-1]
    for k in range(len(values) - 2, -1, -1):
        chosen = jnp.where(index == k, values[k], chosen)
    return chosen


def reduce_kernel(rows, bm, scale, *refs):
    bn = 2 * bm
    hid, wid = refs[0:4], refs[4:8]
    out_refs = refs[8:10]
    relay_wid, relay_hid = refs[10:12]
    hid_v, wid_v, acc, stage, ring1, ring2, result = refs[12:19]
    (own_sem, near_send, near_recv, hop_send, hop_recv, fwd_send, fwd_recv,
     stage_send, stage_recv, r1_send, r1_recv, r2_send, r2_recv, out_sem) = refs[19:]
    n_stage = stage.shape[0]
    half_rows = rows // 2

    z, y, xc = lax.axis_index("z"), lax.axis_index("y"), lax.axis_index("xc")
    x, core = lax.div(xc, 2), lax.rem(xc, 2)
    coord = (x, y, z)
    partner = (z, y, x * 2 + (1 - core))

    def shifted(axis, direction):
        to = lax.rem(coord[axis] + (1 if direction == 0 else RING - 1), RING)
        return ((z, y, to * 2 + core), (z, to, xc), (to, y, xc))[axis]

    barrier = pltpu.get_barrier_semaphore()
    for axis in range(3):
        for direction in range(2):
            pl.semaphore_signal(barrier, inc=1, device_id=shifted(axis, direction), device_id_type=MESH)
    pl.semaphore_signal(barrier, inc=1, device_id=partner, device_id_type=MESH)
    pl.semaphore_wait(barrier, 7)

    def source(piece, part, which, row, n):
        if piece == 0:
            return wid[which].at[pl.ds(row, n)]
        side = 1 - core if piece == 1 else core
        return hid[which].at[pl.ds(row, n), pl.ds(pl.multiple_of((8 * part + 4 * side) * bm, 4 * bm), 4 * bm)]

    def landing(piece, part, slot, row, n):
        if piece == 0:
            return wid_v.at[part, pl.ds(slot * rows + row, n)]
        return hid_v.at[piece - 1, part, pl.ds(slot * rows + row, n)]

    def relay(piece, part, direction):
        if piece == 0:
            return relay_wid.at[part, direction]
        return relay_hid.at[piece - 1, part, direction]

    def own(piece, part, which):
        return pltpu.make_async_copy(source(piece, part, which, 0, rows), landing(piece, part, 0, 0, rows), own_sem.at[piece, part])

    def near(piece, part, direction, which):
        return pltpu.make_async_remote_copy(
            src_ref=source(piece, part, which, 0, rows), dst_ref=landing(piece, part, 1 + 2 * direction, 0, rows),
            send_sem=near_send.at[piece, part, direction], recv_sem=near_recv.at[piece, part, direction],
            device_id=shifted(part, direction), device_id_type=MESH)

    def hop(piece, part, direction, which):
        return pltpu.make_async_remote_copy(
            src_ref=source(piece, part, which, direction * half_rows, half_rows), dst_ref=relay(piece, part, direction),
            send_sem=hop_send.at[piece, part, direction], recv_sem=hop_recv.at[piece, part, direction],
            device_id=shifted(part, direction), device_id_type=MESH)

    def forward(piece, part, direction):
        return pltpu.make_async_remote_copy(
            src_ref=relay(piece, part, direction), dst_ref=landing(piece, part, 2, direction * half_rows, half_rows),
            send_sem=fwd_send.at[piece, part, direction], recv_sem=fwd_recv.at[piece, part, direction],
            device_id=shifted(part, direction), device_id_type=MESH)

    def start_for(copy, owner):
        for which in range(4):
            @pl.when(owner == which)
            def _():
                copy(which).start()

    def start_hops(piece):
        for part in range(PARTS):
            for direction in range(2):
                start_for(functools.partial(hop, piece, part, direction), lax.rem(coord[part] + 2, RING))

    def start_nears(piece):
        for part in range(PARTS):
            for direction in range(2):
                start_for(functools.partial(near, piece, part, direction), lax.rem(coord[part] + (1 if direction == 0 else 3), RING))

    def pass_on(piece):
        for part in range(PARTS):
            for direction in range(2):
                hop(piece, part, direction, 0).wait_recv()
                forward(piece, part, direction).start()

    def arrived(piece, part):
        own(piece, part, 0).wait()
        for direction in range(2):
            near(piece, part, direction, 0).wait_recv()
            forward(piece, part, direction).wait_recv()

    start_hops(0)
    start_hops(1)
    for piece in range(PIECES):
        for part in range(PARTS):
            start_for(functools.partial(own, piece, part), coord[part])
    start_nears(0)
    start_nears(1)
    pass_on(0)
    pass_on(1)
    start_hops(2)
    start_nears(2)

    def product(side, part, chunk, block, store):
        odd = lax.rem(pick(part, coord), 2)
        dims = (((0,), (0,)), ((), ()))

        @pl.when(odd == 1)
        def _():
            left = hid_v[side, part, :, pl.ds(pl.multiple_of(chunk * bm, bm), bm)]
            right = wid_v[part, :, pl.ds(pl.multiple_of(block * bn, bn), bn)]
            store(lax.dot_general(left, right, dims, preferred_element_type=jnp.float32))

        @pl.when(odd == 0)
        def _():
            index = 3 * chunk + block
            left = wid_v[part, :, pl.ds(pl.multiple_of(lax.div(index, 2) * bm, bm), bm)]
            right = hid_v[side, part, :, pl.ds(pl.multiple_of(lax.rem(index, 2) * bn, bn), bn)]
            store(lax.dot_general(left, right, dims, preferred_element_type=jnp.float32))

    def hand_over(part, chunk, block, slot):
        return pltpu.make_async_remote_copy(
            src_ref=stage.at[slot], dst_ref=acc.at[part, chunk, block], send_sem=stage_send.at[slot],
            recv_sem=stage_recv.at[part, chunk, block], device_id=partner, device_id_type=MESH)

    for part in range(PARTS):
        arrived(0, part)
        arrived(1, part)

        def other_half(step, carry):
            chunk, block = lax.div(step, BLOCKS), lax.rem(step, BLOCKS)
            count = part * CHUNKS * BLOCKS + step
            slot = lax.rem(count, n_stage)

            @pl.when(count >= n_stage)
            def _():
                hand_over(0, 0, 0, slot).wait_send()

            def store(value):
                stage[slot] = value

            product(0, part, chunk, block, store)
            hand_over(part, chunk, block, slot).start()
            return carry

        lax.fori_loop(0, CHUNKS * BLOCKS, other_half, 0)
        if part == 0:
            pass_on(2)

    first = (y, z, x)
    second = (z, x, y)
    top, low = bm // 2, bm // 8

    def ring1_copy(part, direction, step, block):
        chunk = lax.rem(first[part] + (RING - 1 - step if direction == 0 else 1 + step), RING)
        return pltpu.make_async_remote_copy(
            src_ref=acc.at[part, chunk, block, pl.ds(direction * top, top)], dst_ref=ring1.at[part, direction, step, block],
            send_sem=r1_send.at[part, direction, block], recv_sem=r1_recv.at[part, direction, step, block],
            device_id=shifted((part + 1) % 3, direction), device_id_type=MESH)

    for part in range(PARTS):
        arrived(2, part)

    for order, offset in enumerate((3, 1, 2, 0)):

        def own_half(step, carry):
            part, block = lax.div(step, BLOCKS), lax.rem(step, BLOCKS)
            chunk = lax.rem(pick(part, first) + offset, RING)
            hand_over(part, chunk, block, 0).wait_recv()

            def store(value):
                acc[part, chunk, block] = acc[part, chunk, block] + value

            product(1, part, chunk, block, store)
            return carry

        lax.fori_loop(0, PARTS * BLOCKS, own_half, 0)
        if order < 2:
            for block in range(BLOCKS):
                for part in range(PARTS):
                    ring1_copy(part, order, 0, block).start()

    for step in range(RING - 1):
        for block in range(BLOCKS):
            for part in range(PARTS):
                for direction in range(2):
                    ring1_copy(part, direction, step, block).wait_recv()
                    chunk = lax.rem(first[part] + (RING - 2 - step if direction == 0 else 2 + step), RING)
                    share = acc.at[part, chunk, block, pl.ds(direction * top, top)]
                    share[...] = share[...] + ring1[part, direction, step, block]
                    ring1_copy(part, direction, step, block).wait_send()
                    if step < RING - 2:
                        ring1_copy(part, direction, step + 1, block).start()

    def ring2_share(part, direction, place):
        row = pl.multiple_of(2 * low * place + direction * low, low)
        return acc.at[part, first[part], :, pl.ds(row, low)]

    def ring2_copy(part, direction, step):
        place = lax.rem(second[part] + (RING - 1 - step if direction == 0 else 1 + step), RING)
        return pltpu.make_async_remote_copy(
            src_ref=ring2_share(part, direction, place), dst_ref=ring2.at[part, direction, step],
            send_sem=r2_send.at[part, direction], recv_sem=r2_recv.at[part, direction, step],
            device_id=shifted((part + 2) % 3, direction), device_id_type=MESH)

    for part in range(PARTS):
        for direction in range(2):
            ring2_copy(part, direction, 0).start()
    for step in range(RING - 1):
        for part in range(PARTS):
            for direction in range(2):
                ring2_copy(part, direction, step).wait_recv()
                place = lax.rem(second[part] + (RING - 2 - step if direction == 0 else 2 + step), RING)
                share = ring2_share(part, direction, place)
                total = share[...] + ring2[part, direction, step]
                ring2_copy(part, direction, step).wait_send()
                if step < RING - 2:
                    share[...] = total
                    ring2_copy(part, direction, step + 1).start()
                else:
                    result[pl.ds(part * BLOCKS, BLOCKS), pl.ds(direction * low, low)] = total * scale

    n_main = PARTS * BLOCKS - LAST
    outs = (pltpu.make_async_copy(result.at[pl.ds(0, n_main)], out_refs[0], out_sem.at[0]),
            pltpu.make_async_copy(result.at[pl.ds(n_main, LAST)], out_refs[1], out_sem.at[1]))
    for copy in outs:
        copy.start()
    for piece in range(PIECES):
        for part in range(PARTS):
            for direction in range(2):
                near(piece, part, direction, 0).wait_send()
                hop(piece, part, direction, 0).wait_send()
                forward(piece, part, direction).wait_send()
    for slot in range(n_stage):
        hand_over(0, 0, 0, slot).wait_send()
    for copy in outs:
        copy.wait()


def reduce_grads(hid, wid, n_dev):
    rows, width = wid[0].shape
    bm = width // 6
    bn = 2 * bm
    dma = pltpu.SemaphoreType.DMA
    any_spec = pl.BlockSpec(memory_space=pl.ANY)
    f32, bf16 = jnp.float32, jnp.bfloat16
    n_main = PARTS * BLOCKS - LAST
    n_stage = 2
    outs = pl.pallas_call(
        functools.partial(reduce_kernel, rows, bm, 1.0 / n_dev),
        name="reduce_grads",
        out_shape=[
            jax.ShapeDtypeStruct((n_main, bm // 4, bn), f32),
            jax.ShapeDtypeStruct((LAST, bm // 4, bn), f32),
            jax.ShapeDtypeStruct((PARTS, 2, rows // 2, width), bf16),
            jax.ShapeDtypeStruct((2, PARTS, 2, rows // 2, 4 * bm), bf16),
        ],
        in_specs=[any_spec] * 8,
        out_specs=[any_spec] * 4,
        scratch_shapes=[
            pltpu.VMEM((2, PARTS, RING * rows, 4 * bm), bf16),
            pltpu.VMEM((PARTS, RING * rows, width), bf16),
            pltpu.VMEM((PARTS, CHUNKS, BLOCKS, bm, bn), f32),
            pltpu.VMEM((n_stage, bm, bn), f32),
            pltpu.VMEM((PARTS, 2, RING - 1, BLOCKS, bm // 2, bn), f32),
            pltpu.VMEM((PARTS, 2, RING - 1, BLOCKS, bm // 8, bn), f32),
            pltpu.VMEM((PARTS * BLOCKS, bm // 4, bn), f32),
            dma((PIECES, PARTS)),
            dma((PIECES, PARTS, 2)), dma((PIECES, PARTS, 2)),
            dma((PIECES, PARTS, 2)), dma((PIECES, PARTS, 2)),
            dma((PIECES, PARTS, 2)), dma((PIECES, PARTS, 2)),
            dma((n_stage,)), dma((PARTS, CHUNKS, BLOCKS)),
            dma((PARTS, 2, BLOCKS)), dma((PARTS, 2, RING - 1, BLOCKS)),
            dma((PARTS, 2)), dma((PARTS, 2, RING - 1)),
            dma((2,)),
        ],
        compiler_params=pltpu.CompilerParams(collective_id=0, has_side_effects=True, vmem_limit_bytes=67043328),
        cost_estimate=pl.CostEstimate(flops=16 * rows * 24 * bm * width, bytes_accessed=200_000_000, transcendentals=0),
    )(*hid, *wid)
    return outs[0], outs[1]


def place_kernel(shape, first_block, n_blocks, depth, *refs):
    n_z, n_y, n_xc, bm = shape
    bn = 2 * bm
    n_dev = n_z * n_y * n_xc
    gathered, dsts = refs[0], refs[-7:-3]
    slots, in_sem, out_sem = refs[-3:]
    ahead = depth // 2

    def load(dev):
        slot = lax.rem(dev, depth)
        return pltpu.make_async_copy(gathered.at[dev], slots.at[slot], in_sem.at[slot])

    def drain(dev):
        slot = lax.rem(dev, depth)
        return pltpu.make_async_copy(slots.at[slot], gathered.at[0], out_sem.at[slot])

    def store(dev):
        slot = lax.rem(dev, depth)
        xc, y, z = lax.rem(dev, n_xc), lax.rem(lax.div(dev, n_xc), n_y), lax.div(dev, n_xc * n_y)
        x, core = lax.div(xc, 2), lax.rem(xc, 2)
        for part in sorted({(first_block + k) // BLOCKS for k in range(n_blocks)}):
            owner, chunk, quarter = ((x, y, z), (y, z, x), (z, x, y))[part]
            for which in range(4):
                @pl.when(owner == which)
                def _():
                    for k in range(n_blocks):
                        if (first_block + k) // BLOCKS != part:
                            continue
                        block = (first_block + k) % BLOCKS
                        if which % 2 == 1:
                            row = (8 * part + 4 * core + chunk) * bm + quarter * (bm // 4)
                            col = block * bn
                        else:
                            index = 3 * chunk + block
                            row = lax.div(index, 2) * bm + quarter * (bm // 4)
                            col = (4 * part + 2 * core + lax.rem(index, 2)) * bn
                        row = pl.multiple_of(row, bm // 4)
                        col = pl.multiple_of(col, bn)
                        pltpu.make_async_copy(
                            slots.at[slot, k], dsts[which].at[pl.ds(row, bm // 4), pl.ds(col, bn)], out_sem.at[slot]).start()

    def prime(dev, carry):
        load(dev).start()
        return carry

    def turn(dev, carry):
        @pl.when(dev + ahead < n_dev)
        def _():
            @pl.when(dev + ahead >= depth)
            def _():
                drain(dev + ahead - depth).wait()

            load(dev + ahead).start()

        load(dev).wait()
        store(dev)
        return carry

    def finish(dev, carry):
        drain(dev).wait()
        return carry

    lax.fori_loop(0, ahead, prime, 0)
    lax.fori_loop(0, n_dev, turn, 0)
    lax.fori_loop(n_dev - depth, n_dev, finish, 0)


def place(gathered, first_block, mesh_shape, shapes, earlier=()):
    n_dev, n_blocks, quarter, bn = gathered.shape
    depth = 16
    return pl.pallas_call(
        functools.partial(place_kernel, (*mesh_shape, bn // 2), first_block, n_blocks, depth),
        name="place_grads",
        out_shape=[jax.ShapeDtypeStruct(s, jnp.float32) for s in shapes],
        in_specs=[pl.BlockSpec(memory_space=pl.ANY)] * (1 + len(earlier)),
        out_specs=[pl.BlockSpec(memory_space=pl.ANY)] * 4,
        scratch_shapes=[pltpu.VMEM((depth, n_blocks, quarter, bn), jnp.float32), pltpu.SemaphoreType.DMA((depth,)), pltpu.SemaphoreType.DMA((depth,))],
        input_output_aliases={1 + k: k for k in range(len(earlier))},
        cost_estimate=pl.CostEstimate(flops=8 * gathered.size, bytes_accessed=8 * gathered.size, transcendentals=0),
    )(gathered, *earlier)


def solution(mesh):
    n_dev = math.prod(mesh.shape.values())
    axes = ("z", "y", "xc")
    batch_spec = P(axes, None)
    whole_spec = P(None, None)

    def device_step(x_loc, g_loc, w_one, w_two, w_three, w_four):
        a_one = jnp.dot(x_loc, w_one, preferred_element_type=jnp.float32).astype(jnp.bfloat16)
        h_one = gelu_value(a_one.astype(jnp.float32)).astype(jnp.bfloat16)
        h_two = (jnp.dot(h_one, w_two, preferred_element_type=jnp.float32) + x_loc.astype(jnp.float32)).astype(jnp.bfloat16)
        a_three = jnp.dot(h_two, w_three, preferred_element_type=jnp.float32).astype(jnp.bfloat16)
        h_three = gelu_value(a_three.astype(jnp.float32)).astype(jnp.bfloat16)
        d_a3 = (jnp.einsum("nd,fd->nf", g_loc, w_four, preferred_element_type=jnp.float32) * gelu_grad(a_three.astype(jnp.float32))).astype(jnp.bfloat16)
        d_h2 = (jnp.einsum("nf,df->nd", d_a3, w_three, preferred_element_type=jnp.float32) + g_loc.astype(jnp.float32)).astype(jnp.bfloat16)
        d_a1 = (jnp.einsum("nd,fd->nf", d_h2, w_two, preferred_element_type=jnp.float32) * gelu_grad(a_one.astype(jnp.float32))).astype(jnp.bfloat16)
        main, last = reduce_grads((d_a1, h_one, d_a3, h_three), (x_loc, d_h2, h_two, g_loc), n_dev)
        all_main = lax.all_gather(main, axes, axis=0)
        last, all_main = lax.optimization_barrier((last, all_main))
        all_last = lax.all_gather(last, axes, axis=0)
        shapes = (w_one.shape, w_two.shape, w_three.shape, w_four.shape)
        mesh_shape = tuple(mesh.shape[name] for name in axes)
        grads = place(all_main, 0, mesh_shape, shapes)
        return tuple(place(all_last, PARTS * BLOCKS - LAST, mesh_shape, shapes, grads))

    return jax.shard_map(
        device_step,
        mesh=mesh,
        in_specs=(batch_spec, batch_spec, whole_spec, whole_spec, whole_spec, whole_spec),
        out_specs=(whole_spec, whole_spec, whole_spec, whole_spec),
        check_vma=False,
    )
```

```python
import functools
import math
import jax
import jax.numpy as jnp
from jax import lax
from jax.experimental import pallas as pl
from jax.experimental.pallas import tpu as pltpu
from jax.sharding import PartitionSpec as P

GELU_SCALE = math.sqrt(2.0 / math.pi)
GELU_CUBIC = 0.044715
MESH = pl.DeviceIdType.MESH
RING = 4
PARTS = 3
CHUNKS = 4
BLOCKS = 3
PIECES = 3


def gelu_value(pre_act):
    return 0.5 * pre_act * (1.0 + jnp.tanh(GELU_SCALE * (pre_act + GELU_CUBIC * pre_act * pre_act * pre_act)))


def gelu_grad(pre_act):
    tanh_val = jnp.tanh(GELU_SCALE * (pre_act + GELU_CUBIC * pre_act * pre_act * pre_act))
    return 0.5 * (1.0 + tanh_val) + 0.5 * pre_act * (1.0 - tanh_val * tanh_val) * GELU_SCALE * (1.0 + 3.0 * GELU_CUBIC * pre_act * pre_act)


def pick(index, values):
    chosen = values[-1]
    for k in range(len(values) - 2, -1, -1):
        chosen = jnp.where(index == k, values[k], chosen)
    return chosen


def reduce_kernel(rows, bm, scale, *refs):
    bn = 2 * bm
    hid, wid = refs[0:4], refs[4:8]
    gath, rest, relay_wid, relay_hid = refs[8:12]
    hid_v, wid_v, acc, stage, ring1, ring2, result = refs[12:19]
    (own_sem, near_send, near_recv, hop_send, hop_recv, fwd_send, fwd_recv,
     stage_send, stage_recv, r1_send, r1_recv, r2_send, r2_recv,
     local_sem, g_send, g1_recv, g2_recv, g3_recv, cross_send, cross_recv) = refs[19:]
    n_stage = stage.shape[0]
    half_rows = rows // 2

    z, y, xc = lax.axis_index("z"), lax.axis_index("y"), lax.axis_index("xc")
    x, core = lax.div(xc, 2), lax.rem(xc, 2)
    coord = (x, y, z)
    partner = (z, y, x * 2 + (1 - core))

    def shifted(axis, direction):
        to = lax.rem(coord[axis] + (1 if direction == 0 else RING - 1), RING)
        return ((z, y, to * 2 + core), (z, to, xc), (to, y, xc))[axis]

    barrier = pltpu.get_barrier_semaphore()
    for axis in range(3):
        for direction in range(2):
            pl.semaphore_signal(barrier, inc=1, device_id=shifted(axis, direction), device_id_type=MESH)
    pl.semaphore_signal(barrier, inc=1, device_id=partner, device_id_type=MESH)
    pl.semaphore_wait(barrier, 7)

    def source(piece, part, which, row, n):
        if piece == 0:
            return wid[which].at[pl.ds(row, n)]
        side = 1 - core if piece == 1 else core
        return hid[which].at[pl.ds(row, n), pl.ds(pl.multiple_of((8 * part + 4 * side) * bm, 4 * bm), 4 * bm)]

    def landing(piece, part, slot, row, n):
        if piece == 0:
            return wid_v.at[part, pl.ds(slot * rows + row, n)]
        return hid_v.at[piece - 1, part, pl.ds(slot * rows + row, n)]

    def relay(piece, part, direction):
        if piece == 0:
            return relay_wid.at[part, direction]
        return relay_hid.at[piece - 1, part, direction]

    def own(piece, part, which):
        return pltpu.make_async_copy(source(piece, part, which, 0, rows), landing(piece, part, 0, 0, rows), own_sem.at[piece, part])

    def near(piece, part, direction, which):
        return pltpu.make_async_remote_copy(
            src_ref=source(piece, part, which, 0, rows), dst_ref=landing(piece, part, 1 + 2 * direction, 0, rows),
            send_sem=near_send.at[piece, part, direction], recv_sem=near_recv.at[piece, part, direction],
            device_id=shifted(part, direction), device_id_type=MESH)

    def hop(piece, part, direction, which):
        return pltpu.make_async_remote_copy(
            src_ref=source(piece, part, which, direction * half_rows, half_rows), dst_ref=relay(piece, part, direction),
            send_sem=hop_send.at[piece, part, direction], recv_sem=hop_recv.at[piece, part, direction],
            device_id=shifted(part, direction), device_id_type=MESH)

    def forward(piece, part, direction):
        return pltpu.make_async_remote_copy(
            src_ref=relay(piece, part, direction), dst_ref=landing(piece, part, 2, direction * half_rows, half_rows),
            send_sem=fwd_send.at[piece, part, direction], recv_sem=fwd_recv.at[piece, part, direction],
            device_id=shifted(part, direction), device_id_type=MESH)

    def start_for(copy, owner):
        for which in range(4):
            @pl.when(owner == which)
            def _():
                copy(which).start()

    def start_hops(piece):
        for part in range(PARTS):
            for direction in range(2):
                start_for(functools.partial(hop, piece, part, direction), lax.rem(coord[part] + 2, RING))

    def start_nears(piece):
        for part in range(PARTS):
            for direction in range(2):
                start_for(functools.partial(near, piece, part, direction), lax.rem(coord[part] + (1 if direction == 0 else 3), RING))

    def pass_on(piece):
        for part in range(PARTS):
            for direction in range(2):
                hop(piece, part, direction, 0).wait_recv()
                forward(piece, part, direction).start()

    def arrived(piece, part):
        own(piece, part, 0).wait()
        for direction in range(2):
            near(piece, part, direction, 0).wait_recv()
            forward(piece, part, direction).wait_recv()

    start_hops(0)
    start_hops(1)
    for piece in range(PIECES):
        for part in range(PARTS):
            start_for(functools.partial(own, piece, part), coord[part])
    start_nears(0)
    start_nears(1)
    pass_on(0)
    pass_on(1)
    start_hops(2)
    start_nears(2)

    def product(side, part, chunk, block, store):
        odd = lax.rem(pick(part, coord), 2)
        dims = (((0,), (0,)), ((), ()))

        @pl.when(odd == 1)
        def _():
            left = hid_v[side, part, :, pl.ds(pl.multiple_of(chunk * bm, bm), bm)]
            right = wid_v[part, :, pl.ds(pl.multiple_of(block * bn, bn), bn)]
            store(lax.dot_general(left, right, dims, preferred_element_type=jnp.float32))

        @pl.when(odd == 0)
        def _():
            index = 3 * chunk + block
            left = wid_v[part, :, pl.ds(pl.multiple_of(lax.div(index, 2) * bm, bm), bm)]
            right = hid_v[side, part, :, pl.ds(pl.multiple_of(lax.rem(index, 2) * bn, bn), bn)]
            store(lax.dot_general(left, right, dims, preferred_element_type=jnp.float32))

    def hand_over(part, chunk, block, slot):
        return pltpu.make_async_remote_copy(
            src_ref=stage.at[slot], dst_ref=acc.at[part, chunk, block], send_sem=stage_send.at[slot],
            recv_sem=stage_recv.at[part, chunk, block], device_id=partner, device_id_type=MESH)

    for part in range(PARTS):
        arrived(0, part)
        arrived(1, part)

        def other_half(step, carry):
            chunk, block = lax.div(step, BLOCKS), lax.rem(step, BLOCKS)
            count = part * CHUNKS * BLOCKS + step
            slot = lax.rem(count, n_stage)

            @pl.when(count >= n_stage)
            def _():
                hand_over(0, 0, 0, slot).wait_send()

            def store(value):
                stage[slot] = value

            product(0, part, chunk, block, store)
            hand_over(part, chunk, block, slot).start()
            return carry

        lax.fori_loop(0, CHUNKS * BLOCKS, other_half, 0)
        if part == 0:
            pass_on(2)

    first = (y, z, x)
    second = (z, x, y)
    top, low = bm // 2, bm // 8

    def ring1_copy(part, direction, step, block):
        chunk = lax.rem(first[part] + (RING - 1 - step if direction == 0 else 1 + step), RING)
        return pltpu.make_async_remote_copy(
            src_ref=acc.at[part, chunk, block, pl.ds(direction * top, top)], dst_ref=ring1.at[part, direction, step, block],
            send_sem=r1_send.at[part, direction, block], recv_sem=r1_recv.at[part, direction, step, block],
            device_id=shifted((part + 1) % 3, direction), device_id_type=MESH)

    for part in range(PARTS):
        arrived(2, part)

    for order, offset in enumerate((3, 1, 2, 0)):

        def own_half(step, carry):
            part, block = lax.div(step, BLOCKS), lax.rem(step, BLOCKS)
            chunk = lax.rem(pick(part, first) + offset, RING)
            hand_over(part, chunk, block, 0).wait_recv()

            def store(value):
                acc[part, chunk, block] = acc[part, chunk, block] + value

            product(1, part, chunk, block, store)
            return carry

        lax.fori_loop(0, PARTS * BLOCKS, own_half, 0)
        if order < 2:
            for block in range(BLOCKS):
                for part in range(PARTS):
                    ring1_copy(part, order, 0, block).start()

    for step in range(RING - 1):
        for block in range(BLOCKS):
            for part in range(PARTS):
                for direction in range(2):
                    ring1_copy(part, direction, step, block).wait_recv()
                    chunk = lax.rem(first[part] + (RING - 2 - step if direction == 0 else 2 + step), RING)
                    share = acc.at[part, chunk, block, pl.ds(direction * top, top)]
                    share[...] = share[...] + ring1[part, direction, step, block]
                    ring1_copy(part, direction, step, block).wait_send()
                    if step < RING - 2:
                        ring1_copy(part, direction, step + 1, block).start()

    def ring2_share(part, direction, place):
        row = pl.multiple_of(2 * low * place + direction * low, low)
        return acc.at[part, first[part], :, pl.ds(row, low)]

    def ring2_copy(part, direction, step):
        place = lax.rem(second[part] + (RING - 1 - step if direction == 0 else 1 + step), RING)
        return pltpu.make_async_remote_copy(
            src_ref=ring2_share(part, direction, place), dst_ref=ring2.at[part, direction, step],
            send_sem=r2_send.at[part, direction], recv_sem=r2_recv.at[part, direction, step],
            device_id=shifted((part + 2) % 3, direction), device_id_type=MESH)

    for part in range(PARTS):
        for direction in range(2):
            ring2_copy(part, direction, 0).start()
    for step in range(RING - 1):
        for part in range(PARTS):
            for direction in range(2):
                ring2_copy(part, direction, step).wait_recv()
                place = lax.rem(second[part] + (RING - 2 - step if direction == 0 else 2 + step), RING)
                share = ring2_share(part, direction, place)
                total = share[...] + ring2[part, direction, step]
                ring2_copy(part, direction, step).wait_send()
                if step < RING - 2:
                    share[...] = total
                    ring2_copy(part, direction, step + 1).start()
                else:
                    for block in range(BLOCKS):
                        result[part, pl.ds(2 * low * block + direction * low, low)] = total[block] * scale

    main, piece_rows = gath.shape[5], result.shape[1]
    cut = main // 16 * 8

    def after(place, by):
        return lax.rem(place + by, RING)

    def at(part, owner, chunk, quarter=None):
        view = gath.at[core, part, owner, chunk]
        return view if quarter is None else view.at[quarter]

    def send(src, dst, sem, recv, axis, direction):
        return pltpu.make_async_remote_copy(
            src_ref=src, dst_ref=dst, send_sem=sem, recv_sem=recv, device_id=shifted(axis, direction), device_id_type=MESH)

    def quarter_copy(part, direction, leg):
        sem, recv = g_send.at[0, part], g1_recv.at[part, direction, leg]
        axis = (part + 2) % 3
        if leg == 0:
            src, dst = result.at[part, pl.ds(0, main)], at(part, coord[part], first[part], second[part])
            return send(src, dst, sem, recv, axis, direction)
        view = at(part, coord[part], first[part], after(second[part], 3 - 2 * direction))
        view = view.at[pl.ds(0, cut)] if direction == 0 else view.at[pl.ds(cut, main - cut)]
        return send(view, view, sem, recv, axis, direction)

    def chunk_copy(part, direction, leg):
        sem, recv = g_send.at[1, part], g2_recv.at[part, direction, leg]
        axis = (part + 1) % 3
        view = at(part, coord[part], first[part])
        if leg == 1:
            view = at(part, coord[part], after(first[part], 3 - 2 * direction)).at[pl.ds(2 * direction, 2)]
        return send(view, view, sem, recv, axis, direction)

    def owner_copy(part, direction, leg, order):
        sem, recv = g_send.at[2, part], g3_recv.at[part, direction, leg, order]
        chunk = after(first[part], (0, 3, 1, 2)[order])
        view = at(part, coord[part], chunk)
        if leg == 1:
            view = at(part, after(coord[part], 3 - 2 * direction), chunk).at[pl.ds(2 * direction, 2)]
        return send(view, view, sem, recv, part, direction)

    def cross(part, owner_by, order):
        view = at(part, after(coord[part], owner_by), after(first[part], (0, 3, 1, 2)[order]))
        return pltpu.make_async_remote_copy(
            src_ref=view, dst_ref=view, send_sem=cross_send, recv_sem=cross_recv, device_id=partner, device_id_type=MESH)

    def keep(part):
        return pltpu.make_async_copy(
            result.at[part, pl.ds(0, main)], at(part, coord[part], first[part], second[part]), local_sem.at[part])

    spare = pltpu.make_async_copy(result.at[:, pl.ds(main, piece_rows - main)], rest, local_sem.at[PARTS])
    for part in range(PARTS):
        for direction in range(2):
            quarter_copy(part, direction, 0).start()
        keep(part).start()
    spare.start()
    for part in range(PARTS):
        for direction in range(2):
            quarter_copy(part, direction, 0).wait_recv()
            quarter_copy(part, direction, 1).start()
    for part in range(PARTS):
        keep(part).wait()
        for direction in range(2):
            quarter_copy(part, direction, 1).wait_recv()
        for direction in range(2):
            chunk_copy(part, direction, 0).start()
        for direction in range(2):
            owner_copy(part, direction, 0, 0).start()
        cross(part, 0, 0).start()
    for part in range(PARTS):
        for direction in range(2):
            chunk_copy(part, direction, 0).wait_recv()
            chunk_copy(part, direction, 1).start()
        for order in (1, 2):
            for direction in range(2):
                owner_copy(part, direction, 0, order).start()
            cross(part, 0, order).start()
    for part in range(PARTS):
        for direction in range(2):
            chunk_copy(part, direction, 1).wait_recv()
        for direction in range(2):
            owner_copy(part, direction, 0, 3).start()
        cross(part, 0, 3).start()
    for order in range(CHUNKS):
        for part in range(PARTS):
            for direction in range(2):
                owner_copy(part, direction, 0, order).wait_recv()
                owner_copy(part, direction, 1, order).start()
                cross(part, 3 - 2 * direction, order).start()
    for order in range(CHUNKS):
        for part in range(PARTS):
            for direction in range(2):
                owner_copy(part, direction, 1, order).wait_recv()
            cross(part, 2, order).start()

    for piece in range(PIECES):
        for part in range(PARTS):
            for direction in range(2):
                near(piece, part, direction, 0).wait_send()
                hop(piece, part, direction, 0).wait_send()
                forward(piece, part, direction).wait_send()
    for slot in range(n_stage):
        hand_over(0, 0, 0, slot).wait_send()
    spare.wait()

    def drain(view, sem):
        pltpu.make_async_copy(view, view, sem).wait()

    for part in range(PARTS):
        drain(gath.at[core, part, 0, 0, pl.ds(0, 3)], g_send.at[0, part])
        drain(gath.at[core, part, 0, pl.ds(0, 3)], g_send.at[1, part])
        drain(gath.at[core, part, pl.ds(0, 3)], g_send.at[2, part])
    drain(gath.at[core], cross_send)
    drain(gath.at[1 - core], cross_recv)


def reduce_grads(hid, wid, n_dev):
    rows, width = wid[0].shape
    bm = width // 6
    bn = 2 * bm
    dma = pltpu.SemaphoreType.DMA
    any_spec = pl.BlockSpec(memory_space=pl.ANY)
    f32, bf16 = jnp.float32, jnp.bfloat16
    n_stage = 2
    piece_rows = BLOCKS * (bm // 4)
    main = piece_rows * 7 // 64 * 8
    outs = pl.pallas_call(
        functools.partial(reduce_kernel, rows, bm, 1.0 / n_dev),
        name="reduce_grads",
        out_shape=[
            jax.ShapeDtypeStruct((2, PARTS, RING, CHUNKS, RING, main, bn), f32),
            jax.ShapeDtypeStruct((PARTS, piece_rows - main, bn), f32),
            jax.ShapeDtypeStruct((PARTS, 2, rows // 2, width), bf16),
            jax.ShapeDtypeStruct((2, PARTS, 2, rows // 2, 4 * bm), bf16),
        ],
        in_specs=[any_spec] * 8,
        out_specs=[any_spec] * 4,
        scratch_shapes=[
            pltpu.VMEM((2, PARTS, RING * rows, 4 * bm), bf16),
            pltpu.VMEM((PARTS, RING * rows, width), bf16),
            pltpu.VMEM((PARTS, CHUNKS, BLOCKS, bm, bn), f32),
            pltpu.VMEM((n_stage, bm, bn), f32),
            pltpu.VMEM((PARTS, 2, RING - 1, BLOCKS, bm // 2, bn), f32),
            pltpu.VMEM((PARTS, 2, RING - 1, BLOCKS, bm // 8, bn), f32),
            pltpu.VMEM((PARTS, piece_rows, bn), f32),
            dma((PIECES, PARTS)),
            dma((PIECES, PARTS, 2)), dma((PIECES, PARTS, 2)),
            dma((PIECES, PARTS, 2)), dma((PIECES, PARTS, 2)),
            dma((PIECES, PARTS, 2)), dma((PIECES, PARTS, 2)),
            dma((n_stage,)), dma((PARTS, CHUNKS, BLOCKS)),
            dma((PARTS, 2, BLOCKS)), dma((PARTS, 2, RING - 1, BLOCKS)),
            dma((PARTS, 2)), dma((PARTS, 2, RING - 1)),
            dma((PARTS + 1,)), dma((3, PARTS)),
            dma((PARTS, 2, 2)), dma((PARTS, 2, 2)), dma((PARTS, 2, 2, CHUNKS)),
            dma, dma,
        ],
        compiler_params=pltpu.CompilerParams(collective_id=0, has_side_effects=True, vmem_limit_bytes=67043328),
        cost_estimate=pl.CostEstimate(flops=16 * rows * 24 * bm * width, bytes_accessed=200_000_000, transcendentals=0),
    )(*hid, *wid)
    return outs[0], outs[1]


def place_kernel(n_turns, depth, load_view, spots, *refs):
    gathered, dsts = refs[0], refs[-7:-3]
    slots, in_sem, out_sem = refs[-3:]
    ahead = depth // 2

    def load(turn):
        slot = lax.rem(turn, depth)
        return pltpu.make_async_copy(load_view(gathered, turn), slots.at[slot], in_sem.at[slot])

    def drain(turn):
        slot = lax.rem(turn, depth)
        return pltpu.make_async_copy(slots.at[slot], load_view(gathered, 0), out_sem.at[slot])

    def store(turn):
        slot = lax.rem(turn, depth)
        for owner, moves in spots(turn):
            for which in range(4):
                @pl.when(owner == which)
                def _():
                    for view, rows, cols in moves(which):
                        pltpu.make_async_copy(view(slots.at[slot]), dsts[which].at[rows, cols], out_sem.at[slot]).start()

    def prime(turn, carry):
        load(turn).start()
        return carry

    def body(turn, carry):
        @pl.when(turn + ahead < n_turns)
        def _():
            @pl.when(turn + ahead >= depth)
            def _():
                drain(turn + ahead - depth).wait()

            load(turn + ahead).start()

        load(turn).wait()
        store(turn)
        return carry

    def finish(turn, carry):
        drain(turn).wait()
        return carry

    lax.fori_loop(0, ahead, prime, 0)
    lax.fori_loop(0, n_turns, body, 0)
    lax.fori_loop(n_turns - depth, n_turns, finish, 0)


def spot(bm, which, part, core, chunk, quarter, block, row, n):
    bn = 2 * bm
    if which % 2 == 1:
        start = (8 * part + 4 * core + chunk) * bm
        col = block * bn
    else:
        index = 3 * chunk + block
        start = lax.div(index, 2) * bm
        col = (4 * part + 2 * core + lax.rem(index, 2)) * bn
    start = start + quarter * (bm // 4) + row
    return pl.ds(pl.multiple_of(start, 8), n), pl.ds(pl.multiple_of(col, bn), bn)


def ranges(bm, begin, end):
    quarter = bm // 4
    for block in range(BLOCKS):
        low, high = max(begin, block * quarter), min(end, (block + 1) * quarter)
        if low < high:
            yield low, block, low - block * quarter, high - low


def place_main(gathered, shapes):
    main, bn = gathered.shape[5:]
    bm = bn // 2
    depth = 12

    def unpack(turn):
        chunk = lax.rem(turn, CHUNKS)
        owner = lax.rem(lax.div(turn, CHUNKS), RING)
        part = lax.rem(lax.div(turn, CHUNKS * RING), PARTS)
        return lax.div(turn, CHUNKS * RING * PARTS), part, owner, chunk

    def load_view(ref, turn):
        return ref.at[unpack(turn)]

    def spots(turn):
        core, part, owner, chunk = unpack(turn)

        def moves(which):
            for quarter in range(RING):
                for begin, block, row, n in ranges(bm, 0, main):
                    yield (lambda ref, q=quarter, b=begin, n=n: ref.at[q, pl.ds(b, n)], *spot(bm, which, part, core, chunk, quarter, block, row, n))

        return [(owner, moves)]

    return place(gathered, shapes, 2 * PARTS * RING * CHUNKS, depth, load_view, spots, (RING, main, bn))


def place_rest(gathered, mesh_shape, shapes, earlier):
    n_dev, _, n_rows, bn = gathered.shape
    bm = bn // 2
    n_z, n_y, n_xc = mesh_shape
    begin_row = BLOCKS * (bm // 4) - n_rows
    group = 8
    depth = 8

    def load_view(ref, turn):
        return ref.at[pl.ds(turn * group, group)]

    def spots(turn):
        found = []
        for k in range(group):
            dev = turn * group + k
            xc, y, z = lax.rem(dev, n_xc), lax.rem(lax.div(dev, n_xc), n_y), lax.div(dev, n_xc * n_y)
            x, core = lax.div(xc, 2), lax.rem(xc, 2)
            for part in range(PARTS):
                owner, chunk, quarter = ((x, y, z), (y, z, x), (z, x, y))[part]

                def moves(which, k=k, part=part, core=core, chunk=chunk, quarter=quarter):
                    for begin, block, row, n in ranges(bm, begin_row, begin_row + n_rows):
                        yield (lambda ref, b=begin - begin_row, n=n: ref.at[k, part, pl.ds(b, n)], *spot(bm, which, part, core, chunk, quarter, block, row, n))

                found.append((owner, moves))
        return found

    return place(gathered, shapes, n_dev // group, depth, load_view, spots, (group, PARTS, n_rows, bn), earlier)


def place(gathered, shapes, n_turns, depth, load_view, spots, slot_shape, earlier=()):
    return pl.pallas_call(
        functools.partial(place_kernel, n_turns, depth, load_view, spots),
        name="place_grads",
        out_shape=[jax.ShapeDtypeStruct(s, jnp.float32) for s in shapes],
        in_specs=[pl.BlockSpec(memory_space=pl.ANY)] * (1 + len(earlier)),
        out_specs=[pl.BlockSpec(memory_space=pl.ANY)] * 4,
        scratch_shapes=[pltpu.VMEM((depth, *slot_shape), jnp.float32), pltpu.SemaphoreType.DMA((depth,)), pltpu.SemaphoreType.DMA((depth,))],
        input_output_aliases={1 + k: k for k in range(len(earlier))},
        cost_estimate=pl.CostEstimate(flops=8 * gathered.size, bytes_accessed=8 * gathered.size, transcendentals=0),
    )(gathered, *earlier)


def solution(mesh):
    n_dev = math.prod(mesh.shape.values())
    axes = ("z", "y", "xc")
    batch_spec = P(axes, None)
    whole_spec = P(None, None)

    def device_step(x_loc, g_loc, w_one, w_two, w_three, w_four):
        a_one = jnp.dot(x_loc, w_one, preferred_element_type=jnp.float32).astype(jnp.bfloat16)
        h_one = gelu_value(a_one.astype(jnp.float32)).astype(jnp.bfloat16)
        h_two = (jnp.dot(h_one, w_two, preferred_element_type=jnp.float32) + x_loc.astype(jnp.float32)).astype(jnp.bfloat16)
        a_three = jnp.dot(h_two, w_three, preferred_element_type=jnp.float32).astype(jnp.bfloat16)
        h_three = gelu_value(a_three.astype(jnp.float32)).astype(jnp.bfloat16)
        d_a3 = (jnp.einsum("nd,fd->nf", g_loc, w_four, preferred_element_type=jnp.float32) * gelu_grad(a_three.astype(jnp.float32))).astype(jnp.bfloat16)
        d_h2 = (jnp.einsum("nf,df->nd", d_a3, w_three, preferred_element_type=jnp.float32) + g_loc.astype(jnp.float32)).astype(jnp.bfloat16)
        d_a1 = (jnp.einsum("nd,fd->nf", d_h2, w_two, preferred_element_type=jnp.float32) * gelu_grad(a_one.astype(jnp.float32))).astype(jnp.bfloat16)
        main, rest = reduce_grads((d_a1, h_one, d_a3, h_three), (x_loc, d_h2, h_two, g_loc), n_dev)
        all_rest = lax.all_gather(rest, axes, axis=0)
        shapes = (w_one.shape, w_two.shape, w_three.shape, w_four.shape)
        mesh_shape = tuple(mesh.shape[name] for name in axes)
        return tuple(place_rest(all_rest, mesh_shape, shapes, place_main(main, shapes)))

    return jax.shard_map(
        device_step,
        mesh=mesh,
        in_specs=(batch_spec, batch_spec, whole_spec, whole_spec, whole_spec, whole_spec),
        out_specs=(whole_spec, whole_spec, whole_spec, whole_spec),
        check_vma=False,
    )
```

```python
import functools
import math
import jax
import jax.numpy as jnp
from jax import lax
from jax.experimental import pallas as pl
from jax.experimental.pallas import tpu as pltpu
from jax.sharding import PartitionSpec as P

GELU_SCALE = math.sqrt(2.0 / math.pi)
GELU_CUBIC = 0.044715
MESH = pl.DeviceIdType.MESH
RING = 4
PARTS = 3
CHUNKS = 4
BLOCKS = 3
WAYS = (0, 1)
PIECES = 3


def gelu_value(pre_act):
    return 0.5 * pre_act * (1.0 + jnp.tanh(GELU_SCALE * (pre_act + GELU_CUBIC * pre_act * pre_act * pre_act)))


def gelu_grad(pre_act):
    tanh_val = jnp.tanh(GELU_SCALE * (pre_act + GELU_CUBIC * pre_act * pre_act * pre_act))
    return 0.5 * (1.0 + tanh_val) + 0.5 * pre_act * (1.0 - tanh_val * tanh_val) * GELU_SCALE * (1.0 + 3.0 * GELU_CUBIC * pre_act * pre_act)


def pick(index, values):
    chosen = values[-1]
    for k in range(len(values) - 2, -1, -1):
        chosen = jnp.where(index == k, values[k], chosen)
    return chosen


def reduce_kernel(rows, bm, scale, *refs):
    bn = 2 * bm
    x_in, g_in, w_one, w_two, w_three, w_four = refs[0:6]
    gath, rest, relay_wid, relay_hid, hid_out, wid_out, a_one = refs[6:13]
    hid = tuple(hid_out.at[which] for which in range(4))
    wid = (x_in, wid_out.at[0], wid_out.at[1], g_in)
    hid_v, wid_v, stage, ring2, result = refs[13:18]
    (free_sem, act_sem, weight_sem, tile_sem, own_sem, near_send, near_recv, hop_send, hop_recv, fwd_send, fwd_recv,
     stage_send, stage_recv, r1_send, r1_recv, r2_send, r2_recv,
     local_sem, g_send, g1_recv, g2_recv, g3_recv, cross_send, cross_recv) = refs[18:]
    n_stage = stage.shape[0]
    half_rows = rows // 2

    z, y, xc = lax.axis_index("z"), lax.axis_index("y"), lax.axis_index("xc")
    x, core = lax.div(xc, 2), lax.rem(xc, 2)
    coord = (x, y, z)
    first, second = (y, z, x), (z, x, y)
    partner = (z, y, x * 2 + (1 - core))

    def shifted(axis, direction):
        to = lax.rem(coord[axis] + (1 if direction == 0 else RING - 1), RING)
        return ((z, y, to * 2 + core), (z, to, xc), (to, y, xc))[axis]

    def tell_neighbours(sem):
        for axis in range(3):
            for direction in WAYS:
                pl.semaphore_signal(sem, inc=1, device_id=shifted(axis, direction), device_id_type=MESH)
        pl.semaphore_signal(sem, inc=1, device_id=partner, device_id_type=MESH)

    barrier = pltpu.get_barrier_semaphore()
    tell_neighbours(barrier)

    def source(piece, part, which, row, n):
        if piece == 0:
            return wid[which].at[pl.ds(row, n)]
        side = 1 - core if piece == 1 else core
        return hid[which].at[pl.ds(row, n), pl.ds(pl.multiple_of((8 * part + 4 * side) * bm, 4 * bm), 4 * bm)]

    def landing(piece, part, slot, row, n):
        if piece == 0:
            return wid_v.at[part, pl.ds(slot * rows + row, n)]
        return hid_v.at[(piece - 1) * PARTS + part, pl.ds(slot * rows + row, n)]

    def relay(piece, part, direction):
        if piece == 0:
            return relay_wid.at[part, direction]
        return relay_hid.at[piece - 1, part, direction]

    def own(piece, part, which):
        return pltpu.make_async_copy(source(piece, part, which, 0, rows), landing(piece, part, 0, 0, rows), own_sem.at[piece, part])

    def near(piece, part, direction, which):
        return pltpu.make_async_remote_copy(
            src_ref=source(piece, part, which, 0, rows), dst_ref=landing(piece, part, 1 + 2 * direction, 0, rows),
            send_sem=near_send.at[piece, part, direction], recv_sem=near_recv.at[piece, part, direction],
            device_id=shifted(part, direction), device_id_type=MESH)

    def hop(piece, part, direction, which):
        return pltpu.make_async_remote_copy(
            src_ref=source(piece, part, which, direction * half_rows, half_rows), dst_ref=relay(piece, part, direction),
            send_sem=hop_send.at[piece, part, direction], recv_sem=hop_recv.at[piece, part, direction],
            device_id=shifted(part, direction), device_id_type=MESH)

    def forward(piece, part, direction):
        return pltpu.make_async_remote_copy(
            src_ref=relay(piece, part, direction), dst_ref=landing(piece, part, 2, direction * half_rows, half_rows),
            send_sem=fwd_send.at[piece, part, direction], recv_sem=fwd_recv.at[piece, part, direction],
            device_id=shifted(part, direction), device_id_type=MESH)

    def start_for(copy, owner, ready):
        for which in ready:
            @pl.when(owner == which)
            def _():
                copy(which).start()

    def send_out(piece, ready=(0, 1, 2, 3)):
        for part in range(PARTS):
            for direction in WAYS:
                start_for(functools.partial(hop, piece, part, direction), lax.rem(coord[part] + 2, RING), ready)
        for part in range(PARTS):
            for direction in WAYS:
                start_for(functools.partial(near, piece, part, direction), lax.rem(coord[part] + (1 if direction == 0 else 3), RING), ready)

    def start_own(piece):
        for part in range(PARTS):
            start_for(functools.partial(own, piece, part), coord[part], (0, 1, 2, 3))

    def pass_on(piece, ready=None):
        for part in range(PARTS):
            for direction in WAYS:
                def relay_one():
                    hop(piece, part, direction, 0).wait_recv()
                    forward(piece, part, direction).start()

                if ready is None:
                    relay_one()
                    continue
                owner = lax.rem(coord[part] + (1 if direction == 0 else 3), RING)
                for which in ready:
                    pl.when(owner == which)(relay_one)

    def arrived(piece, part):
        own(piece, part, 0).wait()
        for direction in WAYS:
            near(piece, part, direction, 0).wait_recv()
            forward(piece, part, direction).wait_recv()

    tiles = 12

    def hidden(tile):
        return pl.ds(pl.multiple_of(tile * bn, bn), bn)

    def rounded(value):
        return value.astype(jnp.bfloat16)

    def widened(value):
        return value.astype(jnp.float32)

    def mm(left, right, transposed=False):
        return lax.dot_general(left, right, (((1,), (1 if transposed else 0,)), ((), ())), preferred_element_type=jnp.float32)

    def products(columns_v, rows_v, acts, out_tiles, total):
        def weight_copy(kind, weight, tile):
            slot = lax.rem(tile, 2)
            if kind == 0:
                return pltpu.make_async_copy(weight.at[:, hidden(tile)], columns_v.at[slot], weight_sem.at[kind, slot])
            return pltpu.make_async_copy(weight.at[hidden(tile)], rows_v.at[slot], weight_sem.at[kind, slot])

        def tile_copy(index, ref, tile, out=True):
            ends = (out_tiles.at[index], ref.at[:, hidden(tile)])
            return pltpu.make_async_copy(*(ends if out else ends[::-1]), tile_sem.at[index])

        def close_total(base, index, ref, sem):
            acts[index] = rounded(total[...] + widened(acts[base]))
            copy = pltpu.make_async_copy(acts.at[index], ref, act_sem.at[sem])
            copy.start()
            copy.wait()

        def sweep(weights, following, step, outs):
            def turn(tile, carry):
                for kind, weight in weights:
                    @pl.when(tile < tiles - 1)
                    def _():
                        weight_copy(kind, weight, tile + 1).start()

                for kind, weight in following:
                    @pl.when(tile == tiles - 1)
                    def _():
                        weight_copy(kind, weight, 0).start()

                for kind, weight in weights:
                    weight_copy(kind, weight, tile).wait()
                slot = lax.rem(tile, 2)

                @pl.when(tile >= 2)
                def _():
                    for k, ref in enumerate(outs):
                        tile_copy(2 * k + slot, ref, tile).wait()

                step(tile, slot)
                for k, ref in enumerate(outs):
                    tile_copy(2 * k + slot, ref, tile).start()
                return carry

            lax.fori_loop(0, tiles, turn, 0)
            for slot in WAYS:
                for k, ref in enumerate(outs):
                    tile_copy(2 * k + slot, ref, slot).wait()

        weight_copy(0, w_one, 0).start()
        weight_copy(1, w_two, 0).start()
        loads = [pltpu.make_async_copy(ref, acts.at[k], act_sem.at[k]) for k, ref in enumerate((x_in, g_in))]
        for copy in loads:
            copy.start()
        total[...] = jnp.zeros(total.shape, jnp.float32)
        pl.semaphore_wait(barrier, 7)
        send_out(0, (0, 3))
        for copy in loads:
            copy.wait()

        def first_forward(tile, slot):
            pre = rounded(mm(acts[0], columns_v[slot]))
            out_tiles[slot] = pre
            act = rounded(gelu_value(widened(pre)))
            out_tiles[2 + slot] = act
            total[...] = total[...] + mm(act, rows_v[slot])

        with jax.named_scope("first_forward"):
            sweep(((0, w_one), (1, w_two)), ((0, w_three), (1, w_four)), first_forward, (a_one, hid[1]))
            close_total(0, 2, wid[2], 2)
        total[...] = jnp.zeros(total.shape, jnp.float32)
        send_out(0, (2,))
        send_out(1, (1,))
        send_out(2, (1,))
        pass_on(0, (0, 3))

        def second_block(tile, slot):
            pre = widened(rounded(mm(acts[2], columns_v[slot])))
            back = mm(acts[1], rows_v[slot], True)
            tanh_val = jnp.tanh(GELU_SCALE * (pre + GELU_CUBIC * pre * pre * pre))
            out_tiles[slot] = rounded(0.5 * pre * (1.0 + tanh_val))
            slope = 0.5 * (1.0 + tanh_val) + 0.5 * pre * (1.0 - tanh_val * tanh_val) * GELU_SCALE * (1.0 + 3.0 * GELU_CUBIC * pre * pre)
            grad = rounded(back * slope)
            out_tiles[2 + slot] = grad
            total[...] = total[...] + mm(grad, columns_v[slot], True)

        with jax.named_scope("second_block"):
            sweep(((0, w_three), (1, w_four)), ((1, w_two),), second_block, (hid[3], hid[2]))
            close_total(1, 0, wid[1], 3)
        send_out(0, (1,))
        send_out(1, (2, 3))
        send_out(2, (2, 3))
        pass_on(0, (2,))
        pass_on(1, (1,))
        pass_on(2, (1,))

        def reload(tile):
            return tile_copy(2 + lax.rem(tile, 2), a_one, tile, out=False)

        reload(0).start()

        def first_backward(tile, slot):
            @pl.when(tile < tiles - 1)
            def _():
                reload(tile + 1).start()

            reload(tile).wait()
            back = mm(acts[0], rows_v[slot], True)
            out_tiles[slot] = rounded(back * gelu_grad(widened(out_tiles[2 + slot])))

        with jax.named_scope("first_backward"):
            sweep(((1, w_two),), (), first_backward, (hid[0],))

    width = wid_v.shape[-1]
    pl.run_scoped(
        products, pltpu.VMEM((2, width, bn), jnp.bfloat16), pltpu.VMEM((2, bn, width), jnp.bfloat16),
        pltpu.VMEM((3, rows, width), jnp.bfloat16), pltpu.VMEM((4, rows, bn), jnp.bfloat16), pltpu.VMEM((rows, width), jnp.float32))

    def sums(acc, ring1):
        def product(side, part, chunk, block, store):
            odd = lax.rem(pick(part, coord), 2)
            dims = (((0,), (0,)), ((), ()))

            @pl.when(odd == 1)
            def _():
                left = hid_v[side * PARTS + part, :, pl.ds(pl.multiple_of(chunk * bm, bm), bm)]
                right = wid_v[part, :, pl.ds(pl.multiple_of(block * bn, bn), bn)]
                store(lax.dot_general(left, right, dims, preferred_element_type=jnp.float32))

            @pl.when(odd == 0)
            def _():
                index = 3 * chunk + block
                left = wid_v[part, :, pl.ds(pl.multiple_of(lax.div(index, 2) * bm, bm), bm)]
                right = hid_v[side * PARTS + part, :, pl.ds(pl.multiple_of(lax.rem(index, 2) * bn, bn), bn)]
                store(lax.dot_general(left, right, dims, preferred_element_type=jnp.float32))

        def hand_over(part, chunk, block, slot):
            return pltpu.make_async_remote_copy(
                src_ref=stage.at[slot], dst_ref=acc.at[part, chunk, block], send_sem=stage_send.at[slot],
                recv_sem=stage_recv.at[part, chunk, block], device_id=partner, device_id_type=MESH)

        tell_neighbours(free_sem)
        send_out(1, (0,))
        send_out(2, (0,))
        pass_on(0, (1,))
        pass_on(1, (2, 3))
        pass_on(1, (0,))
        for piece in range(PIECES):
            start_own(piece)
        pl.semaphore_wait(free_sem, 7)
        for part in range(PARTS):
            with jax.named_scope(f"await_other#p={part}"):
                arrived(0, part)
                arrived(1, part)

            def other_half(step, carry):
                chunk, block = lax.div(step, BLOCKS), lax.rem(step, BLOCKS)
                count = part * CHUNKS * BLOCKS + step
                slot = lax.rem(count, n_stage)

                @pl.when(count >= n_stage)
                def _():
                    hand_over(0, 0, 0, slot).wait_send()

                def store(value):
                    stage[slot] = value

                product(0, part, chunk, block, store)
                hand_over(part, chunk, block, slot).start()
                return carry

            with jax.named_scope(f"other_half#p={part}"):
                lax.fori_loop(0, CHUNKS * BLOCKS, other_half, 0)
            if part == 0:
                pass_on(2, (2, 3))
                pass_on(2, (0,))

        top, low = bm // 2, bm // 8

        def ring1_copy(part, direction, step, block):
            chunk = lax.rem(first[part] + (RING - 1 - step if direction == 0 else 1 + step), RING)
            return pltpu.make_async_remote_copy(
                src_ref=acc.at[part, chunk, block, pl.ds(direction * top, top)], dst_ref=ring1.at[part, direction, step, block],
                send_sem=r1_send.at[part, direction, block], recv_sem=r1_recv.at[part, direction, step, block],
                device_id=shifted((part + 1) % 3, direction), device_id_type=MESH)

        with jax.named_scope("await_own"):
            for part in range(PARTS):
                arrived(2, part)

        for order, offset in enumerate((3, 1, 2, 0)):

            def own_half(step, carry):
                part, block = lax.div(step, BLOCKS), lax.rem(step, BLOCKS)
                chunk = lax.rem(pick(part, first) + offset, RING)
                hand_over(part, chunk, block, 0).wait_recv()

                def store(value):
                    acc[part, chunk, block] = acc[part, chunk, block] + value

                product(1, part, chunk, block, store)
                return carry

            with jax.named_scope(f"own_half#k={order}"):
                lax.fori_loop(0, PARTS * BLOCKS, own_half, 0)
            if order < 2:
                for block in range(BLOCKS):
                    for part in range(PARTS):
                        ring1_copy(part, order, 0, block).start()

        def ring2_share(part, direction, block, place):
            row = pl.multiple_of(2 * low * place + direction * low, low)
            return acc.at[part, first[part], block, pl.ds(row, low)]

        def ring2_copy(part, direction, step, block):
            place = lax.rem(second[part] + (RING - 1 - step if direction == 0 else 1 + step), RING)
            return pltpu.make_async_remote_copy(
                src_ref=ring2_share(part, direction, block, place), dst_ref=ring2.at[part, direction, step, block],
                send_sem=r2_send.at[part, direction, block], recv_sem=r2_recv.at[part, direction, step, block],
                device_id=shifted((part + 2) % 3, direction), device_id_type=MESH)

        with jax.named_scope("ring1"):
            for step in range(RING - 1):
                for block in range(BLOCKS):
                    for part in range(PARTS):
                        for direction in WAYS:
                            ring1_copy(part, direction, step, block).wait_recv()
                            chunk = lax.rem(first[part] + (RING - 2 - step if direction == 0 else 2 + step), RING)
                            share = acc.at[part, chunk, block, pl.ds(direction * top, top)]
                            share[...] = share[...] + ring1[part, direction, step, block]
                            ring1_copy(part, direction, step, block).wait_send()
                            if step < RING - 2:
                                ring1_copy(part, direction, step + 1, block).start()
                        if step == RING - 2:
                            for direction in WAYS:
                                ring2_copy(part, direction, 0, block).start()

        with jax.named_scope("ring2"):
            for step in range(RING - 1):
                for block in range(BLOCKS):
                    for part in range(PARTS):
                        for direction in WAYS:
                            ring2_copy(part, direction, step, block).wait_recv()
                            place = lax.rem(second[part] + (RING - 2 - step if direction == 0 else 2 + step), RING)
                            share = ring2_share(part, direction, block, place)
                            value = share[...] + ring2[part, direction, step, block]
                            ring2_copy(part, direction, step, block).wait_send()
                            if step < RING - 2:
                                share[...] = value
                                ring2_copy(part, direction, step + 1, block).start()
                            else:
                                result[part, pl.ds(2 * low * block + direction * low, low)] = value * scale

        for slot in range(n_stage):
            hand_over(0, 0, 0, slot).wait_send()

    pl.run_scoped(
        sums, pltpu.VMEM((PARTS, CHUNKS, BLOCKS, bm, bn), jnp.float32),
        pltpu.VMEM((PARTS, 2, RING - 1, BLOCKS, bm // 2, bn), jnp.float32))

    main, piece_rows = gath.shape[5], result.shape[1]
    cut = main // 16 * 8

    def after(place, by):
        return lax.rem(place + by, RING)

    def at(part, owner, chunk, quarter=None):
        view = gath.at[core, part, owner, chunk]
        return view if quarter is None else view.at[quarter]

    def send(src, dst, sem, recv, axis, direction):
        return pltpu.make_async_remote_copy(
            src_ref=src, dst_ref=dst, send_sem=sem, recv_sem=recv, device_id=shifted(axis, direction), device_id_type=MESH)

    def quarter_copy(part, direction, leg):
        sem, recv = g_send.at[0, part], g1_recv.at[part, direction, leg]
        axis = (part + 2) % 3
        if leg == 0:
            src, dst = result.at[part, pl.ds(0, main)], at(part, coord[part], first[part], second[part])
            return send(src, dst, sem, recv, axis, direction)
        view = at(part, coord[part], first[part], after(second[part], 3 - 2 * direction))
        view = view.at[pl.ds(0, cut)] if direction == 0 else view.at[pl.ds(cut, main - cut)]
        return send(view, view, sem, recv, axis, direction)

    def chunk_copy(part, direction, leg):
        sem, recv = g_send.at[1, part], g2_recv.at[part, direction, leg]
        axis = (part + 1) % 3
        view = at(part, coord[part], first[part])
        if leg == 1:
            view = at(part, coord[part], after(first[part], 3 - 2 * direction)).at[pl.ds(2 * direction, 2)]
        return send(view, view, sem, recv, axis, direction)

    def owner_copy(part, direction, leg, order):
        sem, recv = g_send.at[2, part], g3_recv.at[part, direction, leg, order]
        chunk = after(first[part], (0, 3, 1, 2)[order])
        view = at(part, coord[part], chunk)
        if leg == 1:
            view = at(part, after(coord[part], 3 - 2 * direction), chunk).at[pl.ds(2 * direction, 2)]
        return send(view, view, sem, recv, part, direction)

    def cross(part, owner_by, order):
        view = at(part, after(coord[part], owner_by), after(first[part], (0, 3, 1, 2)[order]))
        return pltpu.make_async_remote_copy(
            src_ref=view, dst_ref=view, send_sem=cross_send, recv_sem=cross_recv, device_id=partner, device_id_type=MESH)

    def keep(part):
        return pltpu.make_async_copy(
            result.at[part, pl.ds(0, main)], at(part, coord[part], first[part], second[part]), local_sem.at[part])

    spare = pltpu.make_async_copy(result.at[:, pl.ds(main, piece_rows - main)], rest, local_sem.at[PARTS])
    with jax.named_scope("gather"):
        for part in range(PARTS):
            for direction in WAYS:
                quarter_copy(part, direction, 0).start()
            keep(part).start()
        spare.start()
        for part in range(PARTS):
            for direction in WAYS:
                quarter_copy(part, direction, 0).wait_recv()
                quarter_copy(part, direction, 1).start()
        for part in range(PARTS):
            keep(part).wait()
            for direction in WAYS:
                quarter_copy(part, direction, 1).wait_recv()
            for direction in WAYS:
                chunk_copy(part, direction, 0).start()
            for direction in WAYS:
                owner_copy(part, direction, 0, 0).start()
            cross(part, 0, 0).start()
        for part in range(PARTS):
            for direction in WAYS:
                chunk_copy(part, direction, 0).wait_recv()
                chunk_copy(part, direction, 1).start()
            for order in (1, 2):
                for direction in WAYS:
                    owner_copy(part, direction, 0, order).start()
                cross(part, 0, order).start()
        for part in range(PARTS):
            for direction in WAYS:
                chunk_copy(part, direction, 1).wait_recv()
            for direction in WAYS:
                owner_copy(part, direction, 0, 3).start()
            cross(part, 0, 3).start()
        for order in range(CHUNKS):
            for part in range(PARTS):
                for direction in WAYS:
                    owner_copy(part, direction, 0, order).wait_recv()
                    owner_copy(part, direction, 1, order).start()
                    cross(part, 3 - 2 * direction, order).start()
        for order in range(CHUNKS):
            for part in range(PARTS):
                for direction in WAYS:
                    owner_copy(part, direction, 1, order).wait_recv()
                cross(part, 2, order).start()

    for piece in range(PIECES):
        for part in range(PARTS):
            for direction in WAYS:
                near(piece, part, direction, 0).wait_send()
                hop(piece, part, direction, 0).wait_send()
                forward(piece, part, direction).wait_send()
    spare.wait()

    def drain(view, sem):
        pltpu.make_async_copy(view, view, sem).wait()

    for part in range(PARTS):
        drain(gath.at[core, part, 0, 0, pl.ds(0, 3)], g_send.at[0, part])
        drain(gath.at[core, part, 0, pl.ds(0, 3)], g_send.at[1, part])
        drain(gath.at[core, part, pl.ds(0, 3)], g_send.at[2, part])
    drain(gath.at[core], cross_send)
    drain(gath.at[1 - core], cross_recv)


def reduce_grads(x_loc, g_loc, weights, n_dev):
    rows, width = x_loc.shape
    bm = width // 6
    bn = 2 * bm
    dma = pltpu.SemaphoreType.DMA
    any_spec = pl.BlockSpec(memory_space=pl.ANY)
    f32, bf16 = jnp.float32, jnp.bfloat16
    n_stage = 2
    piece_rows = BLOCKS * (bm // 4)
    main = piece_rows * 7 // 64 * 8
    outs = pl.pallas_call(
        functools.partial(reduce_kernel, rows, bm, 1.0 / n_dev),
        name="reduce_grads",
        out_shape=[
            jax.ShapeDtypeStruct((2, PARTS, RING, CHUNKS, RING, main, bn), f32),
            jax.ShapeDtypeStruct((PARTS, piece_rows - main, bn), f32),
            jax.ShapeDtypeStruct((PARTS, 2, rows // 2, width), bf16),
            jax.ShapeDtypeStruct((2, PARTS, 2, rows // 2, 4 * bm), bf16),
            jax.ShapeDtypeStruct((4, rows, 24 * bm), bf16),
            jax.ShapeDtypeStruct((2, rows, width), bf16),
            jax.ShapeDtypeStruct((rows, 24 * bm), bf16),
        ],
        in_specs=[any_spec] * 6,
        out_specs=[any_spec] * 7,
        scratch_shapes=[
            pltpu.VMEM((2 * PARTS, RING * rows, 4 * bm), bf16),
            pltpu.VMEM((PARTS, RING * rows, width), bf16),
            pltpu.VMEM((n_stage, bm, bn), f32),
            pltpu.VMEM((PARTS, 2, RING - 1, BLOCKS, bm // 8, bn), f32),
            pltpu.VMEM((PARTS, piece_rows, bn), f32),
            pltpu.SemaphoreType.REGULAR, dma((4,)), dma((2, 2)), dma((4,)),
            dma((PIECES, PARTS)),
            dma((PIECES, PARTS, 2)), dma((PIECES, PARTS, 2)),
            dma((PIECES, PARTS, 2)), dma((PIECES, PARTS, 2)),
            dma((PIECES, PARTS, 2)), dma((PIECES, PARTS, 2)),
            dma((n_stage,)), dma((PARTS, CHUNKS, BLOCKS)),
            dma((PARTS, 2, BLOCKS)), dma((PARTS, 2, RING - 1, BLOCKS)),
            dma((PARTS, 2, BLOCKS)), dma((PARTS, 2, RING - 1, BLOCKS)),
            dma((PARTS + 1,)), dma((3, PARTS)),
            dma((PARTS, 2, 2)), dma((PARTS, 2, 2)), dma((PARTS, 2, 2, CHUNKS)),
            dma, dma,
        ],
        compiler_params=pltpu.CompilerParams(collective_id=0, has_side_effects=True, vmem_limit_bytes=67043328),
        cost_estimate=pl.CostEstimate(flops=40 * rows * 24 * bm * width, bytes_accessed=200_000_000, transcendentals=0),
    )(x_loc, g_loc, *weights)
    return outs[0], outs[1]


def place_kernel(n_turns, depth, load_view, spots, *refs):
    gathered, dsts = refs[0], refs[-7:-3]
    slots, in_sem, out_sem = refs[-3:]
    ahead = depth // 2

    def load(turn):
        slot = lax.rem(turn, depth)
        return pltpu.make_async_copy(load_view(gathered, turn), slots.at[slot], in_sem.at[slot])

    def drain(turn):
        slot = lax.rem(turn, depth)
        return pltpu.make_async_copy(slots.at[slot], load_view(gathered, 0), out_sem.at[slot])

    def store(turn):
        slot = lax.rem(turn, depth)
        for owner, moves in spots(turn):
            for which in range(4):
                @pl.when(owner == which)
                def _():
                    for view, rows, cols in moves(which):
                        pltpu.make_async_copy(view(slots.at[slot]), dsts[which].at[rows, cols], out_sem.at[slot]).start()

    def prime(turn, carry):
        load(turn).start()
        return carry

    def body(turn, carry):
        @pl.when(turn + ahead < n_turns)
        def _():
            @pl.when(turn + ahead >= depth)
            def _():
                drain(turn + ahead - depth).wait()

            load(turn + ahead).start()

        load(turn).wait()
        store(turn)
        return carry

    def finish(turn, carry):
        drain(turn).wait()
        return carry

    lax.fori_loop(0, ahead, prime, 0)
    lax.fori_loop(0, n_turns, body, 0)
    lax.fori_loop(n_turns - depth, n_turns, finish, 0)


def spot(bm, which, part, core, chunk, quarter, block, row, n):
    bn = 2 * bm
    if which % 2 == 1:
        start = (8 * part + 4 * core + chunk) * bm
        col = block * bn
    else:
        index = 3 * chunk + block
        start = lax.div(index, 2) * bm
        col = (4 * part + 2 * core + lax.rem(index, 2)) * bn
    start = start + quarter * (bm // 4) + row
    return pl.ds(pl.multiple_of(start, 8), n), pl.ds(pl.multiple_of(col, bn), bn)


def ranges(bm, begin, end):
    quarter = bm // 4
    for block in range(BLOCKS):
        low, high = max(begin, block * quarter), min(end, (block + 1) * quarter)
        if low < high:
            yield low, block, low - block * quarter, high - low


def place_main(gathered, shapes):
    main, bn = gathered.shape[5:]
    bm = bn // 2
    depth = 12

    def unpack(turn):
        chunk = lax.rem(turn, CHUNKS)
        owner = lax.rem(lax.div(turn, CHUNKS), RING)
        part = lax.rem(lax.div(turn, CHUNKS * RING), PARTS)
        return lax.div(turn, CHUNKS * RING * PARTS), part, owner, chunk

    def load_view(ref, turn):
        return ref.at[unpack(turn)]

    def spots(turn):
        core, part, owner, chunk = unpack(turn)

        def moves(which):
            for quarter in range(RING):
                for begin, block, row, n in ranges(bm, 0, main):
                    yield (lambda ref, q=quarter, b=begin, n=n: ref.at[q, pl.ds(b, n)], *spot(bm, which, part, core, chunk, quarter, block, row, n))

        return [(owner, moves)]

    return place(gathered, shapes, 2 * PARTS * RING * CHUNKS, depth, load_view, spots, (RING, main, bn))


def place_rest(gathered, mesh_shape, shapes, earlier):
    n_dev, _, n_rows, bn = gathered.shape
    bm = bn // 2
    n_z, n_y, n_xc = mesh_shape
    begin_row = BLOCKS * (bm // 4) - n_rows
    group = 8
    depth = 8

    def load_view(ref, turn):
        return ref.at[pl.ds(turn * group, group)]

    def spots(turn):
        found = []
        for k in range(group):
            dev = turn * group + k
            xc, y, z = lax.rem(dev, n_xc), lax.rem(lax.div(dev, n_xc), n_y), lax.div(dev, n_xc * n_y)
            x, core = lax.div(xc, 2), lax.rem(xc, 2)
            for part in range(PARTS):
                owner, chunk, quarter = ((x, y, z), (y, z, x), (z, x, y))[part]

                def moves(which, k=k, part=part, core=core, chunk=chunk, quarter=quarter):
                    for begin, block, row, n in ranges(bm, begin_row, begin_row + n_rows):
                        yield (lambda ref, b=begin - begin_row, n=n: ref.at[k, part, pl.ds(b, n)], *spot(bm, which, part, core, chunk, quarter, block, row, n))

                found.append((owner, moves))
        return found

    return place(gathered, shapes, n_dev // group, depth, load_view, spots, (group, PARTS, n_rows, bn), earlier)


def place(gathered, shapes, n_turns, depth, load_view, spots, slot_shape, earlier=()):
    return pl.pallas_call(
        functools.partial(place_kernel, n_turns, depth, load_view, spots),
        name="place_grads",
        out_shape=[jax.ShapeDtypeStruct(s, jnp.float32) for s in shapes],
        in_specs=[pl.BlockSpec(memory_space=pl.ANY)] * (1 + len(earlier)),
        out_specs=[pl.BlockSpec(memory_space=pl.ANY)] * 4,
        scratch_shapes=[pltpu.VMEM((depth, *slot_shape), jnp.float32), pltpu.SemaphoreType.DMA((depth,)), pltpu.SemaphoreType.DMA((depth,))],
        input_output_aliases={1 + k: k for k in range(len(earlier))},
        cost_estimate=pl.CostEstimate(flops=8 * gathered.size, bytes_accessed=8 * gathered.size, transcendentals=0),
    )(gathered, *earlier)


def solution(mesh):
    n_dev = math.prod(mesh.shape.values())
    axes = ("z", "y", "xc")
    batch_spec = P(axes, None)
    whole_spec = P(None, None)

    def device_step(x_loc, g_loc, w_one, w_two, w_three, w_four):
        main, rest = reduce_grads(x_loc, g_loc, (w_one, w_two, w_three, w_four), n_dev)
        all_rest = lax.all_gather(rest, axes, axis=0)
        shapes = (w_one.shape, w_two.shape, w_three.shape, w_four.shape)
        mesh_shape = tuple(mesh.shape[name] for name in axes)
        return tuple(place_rest(all_rest, mesh_shape, shapes, place_main(main, shapes)))

    return jax.shard_map(
        device_step,
        mesh=mesh,
        in_specs=(batch_spec, batch_spec, whole_spec, whole_spec, whole_spec, whole_spec),
        out_specs=(whole_spec, whole_spec, whole_spec, whole_spec),
        check_vma=False,
    )
```

```python
import functools
import math
import jax
import jax.numpy as jnp
from jax import lax
from jax.experimental import pallas as pl
from jax.experimental.pallas import tpu as pltpu
from jax.sharding import PartitionSpec as P

GELU_SCALE = math.sqrt(2.0 / math.pi)
GELU_CUBIC = 0.044715
MESH = pl.DeviceIdType.MESH
RING = 4
PARTS = 3
CHUNKS = 4
BLOCKS = 3
LEAD = 3
LAG = 3
WAYS = (0, 1)
PIECES = 3


def gelu_value(pre_act):
    return 0.5 * pre_act * (1.0 + jnp.tanh(GELU_SCALE * (pre_act + GELU_CUBIC * pre_act * pre_act * pre_act)))


def gelu_grad(pre_act):
    tanh_val = jnp.tanh(GELU_SCALE * (pre_act + GELU_CUBIC * pre_act * pre_act * pre_act))
    return 0.5 * (1.0 + tanh_val) + 0.5 * pre_act * (1.0 - tanh_val * tanh_val) * GELU_SCALE * (1.0 + 3.0 * GELU_CUBIC * pre_act * pre_act)


def pick(index, values):
    chosen = values[-1]
    for k in range(len(values) - 2, -1, -1):
        chosen = jnp.where(index == k, values[k], chosen)
    return chosen


def reduce_kernel(rows, bm, scale, *refs):
    bn = 2 * bm
    x_in, g_in, w_one, w_two, w_three, w_four = refs[0:6]
    gath, rest, relay_wid, relay_hid, hid_out, wid_out, a_one = refs[6:13]
    hid = tuple(hid_out.at[which] for which in range(4))
    wid = (x_in, wid_out.at[0], wid_out.at[1], g_in)
    hid_v, wid_v, stage, ring2, result = refs[13:18]
    (free_sem, act_sem, weight_sem, tile_sem, own_sem, near_send, near_recv, hop_send, hop_recv, fwd_send, fwd_recv,
     stage_send, stage_recv, r1_send, r1_recv, r2_send, r2_recv,
     local_sem, g_send, g1_recv, g2_recv, g3_recv, cross_send, cross_recv) = refs[18:]
    n_stage = stage.shape[0]
    half_rows = rows // 2

    z, y, xc = lax.axis_index("z"), lax.axis_index("y"), lax.axis_index("xc")
    x, core = lax.div(xc, 2), lax.rem(xc, 2)
    coord = (x, y, z)
    first, second = (y, z, x), (z, x, y)
    partner = (z, y, x * 2 + (1 - core))

    def shifted(axis, direction):
        to = lax.rem(coord[axis] + (1 if direction == 0 else RING - 1), RING)
        return ((z, y, to * 2 + core), (z, to, xc), (to, y, xc))[axis]

    def tell_neighbours(sem):
        for axis in range(3):
            for direction in WAYS:
                pl.semaphore_signal(sem, inc=1, device_id=shifted(axis, direction), device_id_type=MESH)
        pl.semaphore_signal(sem, inc=1, device_id=partner, device_id_type=MESH)

    barrier = pltpu.get_barrier_semaphore()
    tell_neighbours(barrier)

    def source(piece, part, which, row, n):
        if piece == 0:
            return wid[which].at[pl.ds(row, n)]
        side = 1 - core if piece == 1 else core
        return hid[which].at[pl.ds(row, n), pl.ds(pl.multiple_of((8 * part + 4 * side) * bm, 4 * bm), 4 * bm)]

    def landing(piece, part, slot, row, n):
        if piece == 0:
            return wid_v.at[part, pl.ds(slot * rows + row, n)]
        return hid_v.at[(piece - 1) * PARTS + part, pl.ds(slot * rows + row, n)]

    def relay(piece, part, direction):
        if piece == 0:
            return relay_wid.at[part, direction]
        return relay_hid.at[piece - 1, part, direction]

    def own(piece, part, which):
        return pltpu.make_async_copy(source(piece, part, which, 0, rows), landing(piece, part, 0, 0, rows), own_sem.at[piece, part])

    def near(piece, part, direction, which):
        return pltpu.make_async_remote_copy(
            src_ref=source(piece, part, which, 0, rows), dst_ref=landing(piece, part, 1 + 2 * direction, 0, rows),
            send_sem=near_send.at[piece, part, direction], recv_sem=near_recv.at[piece, part, direction],
            device_id=shifted(part, direction), device_id_type=MESH)

    def hop(piece, part, direction, which):
        return pltpu.make_async_remote_copy(
            src_ref=source(piece, part, which, direction * half_rows, half_rows), dst_ref=relay(piece, part, direction),
            send_sem=hop_send.at[piece, part, direction], recv_sem=hop_recv.at[piece, part, direction],
            device_id=shifted(part, direction), device_id_type=MESH)

    def forward(piece, part, direction):
        return pltpu.make_async_remote_copy(
            src_ref=relay(piece, part, direction), dst_ref=landing(piece, part, 2, direction * half_rows, half_rows),
            send_sem=fwd_send.at[piece, part, direction], recv_sem=fwd_recv.at[piece, part, direction],
            device_id=shifted(part, direction), device_id_type=MESH)

    def start_for(copy, owner, ready):
        for which in ready:
            @pl.when(owner == which)
            def _():
                copy(which).start()

    def send_out(piece, ready=(0, 1, 2, 3)):
        for part in range(PARTS):
            for direction in WAYS:
                start_for(functools.partial(hop, piece, part, direction), lax.rem(coord[part] + 2, RING), ready)
        for part in range(PARTS):
            for direction in WAYS:
                start_for(functools.partial(near, piece, part, direction), lax.rem(coord[part] + (1 if direction == 0 else 3), RING), ready)

    def start_own(piece):
        for part in range(PARTS):
            start_for(functools.partial(own, piece, part), coord[part], (0, 1, 2, 3))

    def pass_on(piece, ready=None):
        for part in range(PARTS):
            for direction in WAYS:
                def relay_one():
                    hop(piece, part, direction, 0).wait_recv()
                    forward(piece, part, direction).start()

                if ready is None:
                    relay_one()
                    continue
                owner = lax.rem(coord[part] + (1 if direction == 0 else 3), RING)
                for which in ready:
                    pl.when(owner == which)(relay_one)

    def arrived(piece, part):
        own(piece, part, 0).wait()
        for direction in WAYS:
            near(piece, part, direction, 0).wait_recv()
            forward(piece, part, direction).wait_recv()

    tiles, lead = 12, weight_sem.shape[1] - 1

    def hidden(tile):
        return pl.ds(pl.multiple_of(tile * bn, bn), bn)

    def rounded(value):
        return value.astype(jnp.bfloat16)

    def widened(value):
        return value.astype(jnp.float32)

    def mm(left, right, transposed=False):
        return lax.dot_general(left, right, (((1,), (1 if transposed else 0,)), ((), ())), preferred_element_type=jnp.float32)

    def products(columns_v, rows_v, acts, out_tiles, total):
        def weight_copy(kind, weight, tile):
            slot = lax.rem(tile, lead + 1)
            if kind == 0:
                return pltpu.make_async_copy(weight.at[:, hidden(tile)], columns_v.at[slot], weight_sem.at[kind, slot])
            return pltpu.make_async_copy(weight.at[hidden(tile)], rows_v.at[slot], weight_sem.at[kind, slot])

        def tile_copy(index, ref, tile, out=True):
            ends = (out_tiles.at[index], ref.at[:, hidden(tile)])
            return pltpu.make_async_copy(*(ends if out else ends[::-1]), tile_sem.at[index])

        def close_total(base, index, ref, sem):
            acts[index] = rounded(total[...] + widened(acts[base]))
            copy = pltpu.make_async_copy(acts.at[index], ref, act_sem.at[sem])
            copy.start()
            copy.wait()

        def sweep(weights, following, step, outs):
            def turn(tile, carry):
                for kind, weight in weights:
                    @pl.when(tile < tiles - lead)
                    def _():
                        weight_copy(kind, weight, tile + lead).start()

                for kind, weight in following:
                    @pl.when(tile >= tiles - lead)
                    def _():
                        weight_copy(kind, weight, tile + lead - tiles).start()

                for kind, weight in weights:
                    weight_copy(kind, weight, tile).wait()
                slot = lax.rem(tile, 2)

                @pl.when(tile >= 2)
                def _():
                    for k, ref in enumerate(outs):
                        tile_copy(2 * k + slot, ref, tile).wait()

                step(tile, slot, lax.rem(tile, lead + 1))
                for k, ref in enumerate(outs):
                    tile_copy(2 * k + slot, ref, tile).start()
                return carry

            lax.fori_loop(0, tiles, turn, 0)
            for slot in WAYS:
                for k, ref in enumerate(outs):
                    tile_copy(2 * k + slot, ref, slot).wait()

        for tile in range(lead):
            weight_copy(0, w_one, tile).start()
            weight_copy(1, w_two, tile).start()
        loads = [pltpu.make_async_copy(ref, acts.at[k], act_sem.at[k]) for k, ref in enumerate((x_in, g_in))]
        for copy in loads:
            copy.start()
        total[...] = jnp.zeros(total.shape, jnp.float32)
        pl.semaphore_wait(barrier, 7)
        send_out(0, (0, 3))
        for copy in loads:
            copy.wait()

        def first_forward(tile, slot, load):
            pre = rounded(mm(acts[0], columns_v[load]))
            out_tiles[slot] = pre
            act = rounded(gelu_value(widened(pre)))
            out_tiles[2 + slot] = act
            total[...] = total[...] + mm(act, rows_v[load])

        with jax.named_scope("first_forward"):
            sweep(((0, w_one), (1, w_two)), ((0, w_three), (1, w_four)), first_forward, (a_one, hid[1]))
            close_total(0, 2, wid[2], 2)
        total[...] = jnp.zeros(total.shape, jnp.float32)
        send_out(0, (2,))
        send_out(1, (1,))
        send_out(2, (1,))
        pass_on(0, (0, 3))

        def second_block(tile, slot, load):
            pre = widened(rounded(mm(acts[2], columns_v[load])))
            back = mm(acts[1], rows_v[load], True)
            tanh_val = jnp.tanh(GELU_SCALE * (pre + GELU_CUBIC * pre * pre * pre))
            out_tiles[slot] = rounded(0.5 * pre * (1.0 + tanh_val))
            slope = 0.5 * (1.0 + tanh_val) + 0.5 * pre * (1.0 - tanh_val * tanh_val) * GELU_SCALE * (1.0 + 3.0 * GELU_CUBIC * pre * pre)
            grad = rounded(back * slope)
            out_tiles[2 + slot] = grad
            total[...] = total[...] + mm(grad, columns_v[load], True)

        with jax.named_scope("second_block"):
            sweep(((0, w_three), (1, w_four)), ((1, w_two),), second_block, (hid[3], hid[2]))
            close_total(1, 0, wid[1], 3)
        send_out(0, (1,))
        send_out(1, (2, 3))
        send_out(2, (2, 3))
        pass_on(0, (2,))
        pass_on(1, (1,))
        pass_on(2, (1,))

        def reload(tile):
            return tile_copy(2 + lax.rem(tile, 2), a_one, tile, out=False)

        reload(0).start()

        def first_backward(tile, slot, load):
            @pl.when(tile < tiles - 1)
            def _():
                reload(tile + 1).start()

            reload(tile).wait()
            back = mm(acts[0], rows_v[load], True)
            out_tiles[slot] = rounded(back * gelu_grad(widened(out_tiles[2 + slot])))

        with jax.named_scope("first_backward"):
            sweep(((1, w_two),), (), first_backward, (hid[0],))

    width = wid_v.shape[-1]
    pl.run_scoped(
        products, pltpu.VMEM((lead + 1, width, bn), jnp.bfloat16), pltpu.VMEM((lead + 1, bn, width), jnp.bfloat16),
        pltpu.VMEM((3, rows, width), jnp.bfloat16), pltpu.VMEM((4, rows, bn), jnp.bfloat16), pltpu.VMEM((rows, width), jnp.float32))

    def sums(acc, ring1):
        def product(side, part, chunk, block, store):
            odd = lax.rem(pick(part, coord), 2)
            dims = (((0,), (0,)), ((), ()))

            @pl.when(odd == 1)
            def _():
                left = hid_v[side * PARTS + part, :, pl.ds(pl.multiple_of(chunk * bm, bm), bm)]
                right = wid_v[part, :, pl.ds(pl.multiple_of(block * bn, bn), bn)]
                store(lax.dot_general(left, right, dims, preferred_element_type=jnp.float32))

            @pl.when(odd == 0)
            def _():
                index = 3 * chunk + block
                left = wid_v[part, :, pl.ds(pl.multiple_of(lax.div(index, 2) * bm, bm), bm)]
                right = hid_v[side * PARTS + part, :, pl.ds(pl.multiple_of(lax.rem(index, 2) * bn, bn), bn)]
                store(lax.dot_general(left, right, dims, preferred_element_type=jnp.float32))

        def hand_over(part, chunk, block, slot):
            return pltpu.make_async_remote_copy(
                src_ref=stage.at[slot], dst_ref=acc.at[part, chunk, block], send_sem=stage_send.at[slot],
                recv_sem=stage_recv.at[part, chunk, block], device_id=partner, device_id_type=MESH)

        tell_neighbours(free_sem)
        send_out(1, (0,))
        send_out(2, (0,))
        pass_on(0, (1,))
        pass_on(1, (2, 3))
        pass_on(2, (2, 3))
        pass_on(1, (0,))
        pass_on(2, (0,))
        for piece in range(PIECES):
            start_own(piece)
        pl.semaphore_wait(free_sem, 7)
        with jax.named_scope("await"):
            for piece in range(PIECES):
                for part in range(PARTS):
                    arrived(piece, part)

        top, low = bm // 2, bm // 8

        def ring1_copy(part, direction, step, block):
            chunk = lax.rem(first[part] + (RING - 1 - step if direction == 0 else 1 + step), RING)
            return pltpu.make_async_remote_copy(
                src_ref=acc.at[part, chunk, block, pl.ds(direction * top, top)], dst_ref=ring1.at[part, direction, step, block],
                send_sem=r1_send.at[part, direction, block], recv_sem=r1_recv.at[part, direction, step, block],
                device_id=shifted((part + 1) % 3, direction), device_id_type=MESH)

        def place_of(count):
            order, rest = lax.div(count, PARTS * BLOCKS), lax.rem(count, PARTS * BLOCKS)
            part, block = lax.rem(rest, PARTS), lax.div(rest, PARTS)
            return order, part, lax.rem(pick(part, first) + pick(order, (3, 1, 2, 0)), RING), block

        blocks = CHUNKS * PARTS * BLOCKS

        def both_halves(count, carry):
            @pl.when(count < blocks)
            def _():
                _, part, chunk, block = place_of(count)
                slot = lax.rem(count, n_stage)

                @pl.when(count >= n_stage)
                def _():
                    hand_over(0, 0, 0, slot).wait_send()

                def store(value):
                    stage[slot] = value

                product(0, part, chunk, block, store)
                hand_over(part, chunk, block, slot).start()

            @pl.when(count >= LAG)
            def _():
                order, part, chunk, block = place_of(count - LAG)
                hand_over(part, chunk, block, 0).wait_recv()

                def store(value):
                    acc[part, chunk, block] = acc[part, chunk, block] + value

                product(1, part, chunk, block, store)
                for direction in WAYS:
                    for which in range(PARTS):
                        @pl.when((order == direction) & (part == which))
                        def _():
                            ring1_copy(which, direction, 0, block).start()

            return carry

        with jax.named_scope("halves"):
            lax.fori_loop(0, blocks + LAG, both_halves, 0)

        def ring2_share(part, direction, block, place):
            row = pl.multiple_of(2 * low * place + direction * low, low)
            return acc.at[part, first[part], block, pl.ds(row, low)]

        def ring2_copy(part, direction, step, block):
            place = lax.rem(second[part] + (RING - 1 - step if direction == 0 else 1 + step), RING)
            return pltpu.make_async_remote_copy(
                src_ref=ring2_share(part, direction, block, place), dst_ref=ring2.at[part, direction, step, block],
                send_sem=r2_send.at[part, direction, block], recv_sem=r2_recv.at[part, direction, step, block],
                device_id=shifted((part + 2) % 3, direction), device_id_type=MESH)

        with jax.named_scope("ring1"):
            for step in range(RING - 1):
                for block in range(BLOCKS):
                    for part in range(PARTS):
                        for direction in WAYS:
                            ring1_copy(part, direction, step, block).wait_recv()
                            chunk = lax.rem(first[part] + (RING - 2 - step if direction == 0 else 2 + step), RING)
                            share = acc.at[part, chunk, block, pl.ds(direction * top, top)]
                            share[...] = share[...] + ring1[part, direction, step, block]
                            ring1_copy(part, direction, step, block).wait_send()
                            if step < RING - 2:
                                ring1_copy(part, direction, step + 1, block).start()
                        if step == RING - 2:
                            for direction in WAYS:
                                ring2_copy(part, direction, 0, block).start()

        with jax.named_scope("ring2"):
            for step in range(RING - 1):
                for block in range(BLOCKS):
                    for part in range(PARTS):
                        for direction in WAYS:
                            ring2_copy(part, direction, step, block).wait_recv()
                            place = lax.rem(second[part] + (RING - 2 - step if direction == 0 else 2 + step), RING)
                            share = ring2_share(part, direction, block, place)
                            value = share[...] + ring2[part, direction, step, block]
                            ring2_copy(part, direction, step, block).wait_send()
                            if step < RING - 2:
                                share[...] = value
                                ring2_copy(part, direction, step + 1, block).start()
                            else:
                                result[part, pl.ds(2 * low * block + direction * low, low)] = value * scale

        for slot in range(n_stage):
            hand_over(0, 0, 0, slot).wait_send()

    pl.run_scoped(
        sums, pltpu.VMEM((PARTS, CHUNKS, BLOCKS, bm, bn), jnp.float32),
        pltpu.VMEM((PARTS, 2, RING - 1, BLOCKS, bm // 2, bn), jnp.float32))

    main, piece_rows = gath.shape[5], result.shape[1]
    cut = main // 16 * 8

    def after(place, by):
        return lax.rem(place + by, RING)

    def at(part, owner, chunk, quarter=None):
        view = gath.at[core, part, owner, chunk]
        return view if quarter is None else view.at[quarter]

    def send(src, dst, sem, recv, axis, direction):
        return pltpu.make_async_remote_copy(
            src_ref=src, dst_ref=dst, send_sem=sem, recv_sem=recv, device_id=shifted(axis, direction), device_id_type=MESH)

    def quarter_copy(part, direction, leg):
        sem, recv = g_send.at[0, part], g1_recv.at[part, direction, leg]
        axis = (part + 2) % 3
        if leg == 0:
            src, dst = result.at[part, pl.ds(0, main)], at(part, coord[part], first[part], second[part])
            return send(src, dst, sem, recv, axis, direction)
        view = at(part, coord[part], first[part], after(second[part], 3 - 2 * direction))
        view = view.at[pl.ds(0, cut)] if direction == 0 else view.at[pl.ds(cut, main - cut)]
        return send(view, view, sem, recv, axis, direction)

    def chunk_copy(part, direction, leg):
        sem, recv = g_send.at[1, part], g2_recv.at[part, direction, leg]
        axis = (part + 1) % 3
        view = at(part, coord[part], first[part])
        if leg == 1:
            view = at(part, coord[part], after(first[part], 3 - 2 * direction)).at[pl.ds(2 * direction, 2)]
        return send(view, view, sem, recv, axis, direction)

    def owner_copy(part, direction, leg, order):
        sem, recv = g_send.at[2, part], g3_recv.at[part, direction, leg, order]
        chunk = after(first[part], (0, 3, 1, 2)[order])
        view = at(part, coord[part], chunk)
        if leg == 1:
            view = at(part, after(coord[part], 3 - 2 * direction), chunk).at[pl.ds(2 * direction, 2)]
        return send(view, view, sem, recv, part, direction)

    def cross(part, owner_by, order):
        view = at(part, after(coord[part], owner_by), after(first[part], (0, 3, 1, 2)[order]))
        return pltpu.make_async_remote_copy(
            src_ref=view, dst_ref=view, send_sem=cross_send, recv_sem=cross_recv, device_id=partner, device_id_type=MESH)

    def keep(part):
        return pltpu.make_async_copy(
            result.at[part, pl.ds(0, main)], at(part, coord[part], first[part], second[part]), local_sem.at[part])

    spare = pltpu.make_async_copy(result.at[:, pl.ds(main, piece_rows - main)], rest, local_sem.at[PARTS])
    with jax.named_scope("gather"):
        for part in range(PARTS):
            for direction in WAYS:
                quarter_copy(part, direction, 0).start()
            keep(part).start()
        spare.start()
        for part in range(PARTS):
            for direction in WAYS:
                quarter_copy(part, direction, 0).wait_recv()
                quarter_copy(part, direction, 1).start()
        for part in range(PARTS):
            keep(part).wait()
            for direction in WAYS:
                quarter_copy(part, direction, 1).wait_recv()
            for direction in WAYS:
                chunk_copy(part, direction, 0).start()
            for direction in WAYS:
                owner_copy(part, direction, 0, 0).start()
            cross(part, 0, 0).start()
        for part in range(PARTS):
            for direction in WAYS:
                chunk_copy(part, direction, 0).wait_recv()
                chunk_copy(part, direction, 1).start()
            for order in (1, 2):
                for direction in WAYS:
                    owner_copy(part, direction, 0, order).start()
                cross(part, 0, order).start()
        for part in range(PARTS):
            for direction in WAYS:
                chunk_copy(part, direction, 1).wait_recv()
            for direction in WAYS:
                owner_copy(part, direction, 0, 3).start()
            cross(part, 0, 3).start()
        for order in range(CHUNKS):
            for part in range(PARTS):
                for direction in WAYS:
                    owner_copy(part, direction, 0, order).wait_recv()
                    owner_copy(part, direction, 1, order).start()
                    cross(part, 3 - 2 * direction, order).start()
        for order in range(CHUNKS):
            for part in range(PARTS):
                for direction in WAYS:
                    owner_copy(part, direction, 1, order).wait_recv()
                cross(part, 2, order).start()

    for piece in range(PIECES):
        for part in range(PARTS):
            for direction in WAYS:
                near(piece, part, direction, 0).wait_send()
                hop(piece, part, direction, 0).wait_send()
                forward(piece, part, direction).wait_send()
    spare.wait()

    def drain(view, sem):
        pltpu.make_async_copy(view, view, sem).wait()

    for part in range(PARTS):
        drain(gath.at[core, part, 0, 0, pl.ds(0, 3)], g_send.at[0, part])
        drain(gath.at[core, part, 0, pl.ds(0, 3)], g_send.at[1, part])
        drain(gath.at[core, part, pl.ds(0, 3)], g_send.at[2, part])
    drain(gath.at[core], cross_send)
    drain(gath.at[1 - core], cross_recv)


def reduce_grads(x_loc, g_loc, weights, n_dev):
    rows, width = x_loc.shape
    bm = width // 6
    bn = 2 * bm
    dma = pltpu.SemaphoreType.DMA
    any_spec = pl.BlockSpec(memory_space=pl.ANY)
    f32, bf16 = jnp.float32, jnp.bfloat16
    n_stage = 4
    piece_rows = BLOCKS * (bm // 4)
    main = piece_rows * 7 // 64 * 8
    outs = pl.pallas_call(
        functools.partial(reduce_kernel, rows, bm, 1.0 / n_dev),
        name="reduce_grads",
        out_shape=[
            jax.ShapeDtypeStruct((2, PARTS, RING, CHUNKS, RING, main, bn), f32),
            jax.ShapeDtypeStruct((PARTS, piece_rows - main, bn), f32),
            jax.ShapeDtypeStruct((PARTS, 2, rows // 2, width), bf16),
            jax.ShapeDtypeStruct((2, PARTS, 2, rows // 2, 4 * bm), bf16),
            jax.ShapeDtypeStruct((4, rows, 24 * bm), bf16),
            jax.ShapeDtypeStruct((2, rows, width), bf16),
            jax.ShapeDtypeStruct((rows, 24 * bm), bf16),
        ],
        in_specs=[any_spec] * 6,
        out_specs=[any_spec] * 7,
        scratch_shapes=[
            pltpu.VMEM((2 * PARTS, RING * rows, 4 * bm), bf16),
            pltpu.VMEM((PARTS, RING * rows, width), bf16),
            pltpu.VMEM((n_stage, bm, bn), f32),
            pltpu.VMEM((PARTS, 2, RING - 1, BLOCKS, bm // 8, bn), f32),
            pltpu.VMEM((PARTS, piece_rows, bn), f32),
            pltpu.SemaphoreType.REGULAR, dma((4,)), dma((2, LEAD + 1)), dma((4,)),
            dma((PIECES, PARTS)),
            dma((PIECES, PARTS, 2)), dma((PIECES, PARTS, 2)),
            dma((PIECES, PARTS, 2)), dma((PIECES, PARTS, 2)),
            dma((PIECES, PARTS, 2)), dma((PIECES, PARTS, 2)),
            dma((n_stage,)), dma((PARTS, CHUNKS, BLOCKS)),
            dma((PARTS, 2, BLOCKS)), dma((PARTS, 2, RING - 1, BLOCKS)),
            dma((PARTS, 2, BLOCKS)), dma((PARTS, 2, RING - 1, BLOCKS)),
            dma((PARTS + 1,)), dma((3, PARTS)),
            dma((PARTS, 2, 2)), dma((PARTS, 2, 2)), dma((PARTS, 2, 2, CHUNKS)),
            dma, dma,
        ],
        compiler_params=pltpu.CompilerParams(collective_id=0, has_side_effects=True, vmem_limit_bytes=67043328),
        cost_estimate=pl.CostEstimate(flops=40 * rows * 24 * bm * width, bytes_accessed=200_000_000, transcendentals=0),
    )(x_loc, g_loc, *weights)
    return outs[0], outs[1]


def place_kernel(n_turns, depth, load_view, spots, *refs):
    gathered, dsts = refs[0], refs[-7:-3]
    slots, in_sem, out_sem = refs[-3:]
    ahead = depth // 2

    def load(turn):
        slot = lax.rem(turn, depth)
        return pltpu.make_async_copy(load_view(gathered, turn), slots.at[slot], in_sem.at[slot])

    def drain(turn):
        slot = lax.rem(turn, depth)
        return pltpu.make_async_copy(slots.at[slot], load_view(gathered, 0), out_sem.at[slot])

    def store(turn):
        slot = lax.rem(turn, depth)
        for owner, moves in spots(turn):
            for which in range(4):
                @pl.when(owner == which)
                def _():
                    for view, rows, cols in moves(which):
                        pltpu.make_async_copy(view(slots.at[slot]), dsts[which].at[rows, cols], out_sem.at[slot]).start()

    def prime(turn, carry):
        load(turn).start()
        return carry

    def body(turn, carry):
        @pl.when(turn + ahead < n_turns)
        def _():
            @pl.when(turn + ahead >= depth)
            def _():
                drain(turn + ahead - depth).wait()

            load(turn + ahead).start()

        load(turn).wait()
        store(turn)
        return carry

    def finish(turn, carry):
        drain(turn).wait()
        return carry

    lax.fori_loop(0, ahead, prime, 0)
    lax.fori_loop(0, n_turns, body, 0)
    lax.fori_loop(n_turns - depth, n_turns, finish, 0)


def spot(bm, which, part, core, chunk, quarter, block, row, n):
    bn = 2 * bm
    if which % 2 == 1:
        start = (8 * part + 4 * core + chunk) * bm
        col = block * bn
    else:
        index = 3 * chunk + block
        start = lax.div(index, 2) * bm
        col = (4 * part + 2 * core + lax.rem(index, 2)) * bn
    start = start + quarter * (bm // 4) + row
    return pl.ds(pl.multiple_of(start, 8), n), pl.ds(pl.multiple_of(col, bn), bn)


def ranges(bm, begin, end):
    quarter = bm // 4
    for block in range(BLOCKS):
        low, high = max(begin, block * quarter), min(end, (block + 1) * quarter)
        if low < high:
            yield low, block, low - block * quarter, high - low


def place_main(gathered, shapes):
    main, bn = gathered.shape[5:]
    bm = bn // 2
    depth = 12

    def unpack(turn):
        chunk = lax.rem(turn, CHUNKS)
        owner = lax.rem(lax.div(turn, CHUNKS), RING)
        part = lax.rem(lax.div(turn, CHUNKS * RING), PARTS)
        return lax.div(turn, CHUNKS * RING * PARTS), part, owner, chunk

    def load_view(ref, turn):
        return ref.at[unpack(turn)]

    def spots(turn):
        core, part, owner, chunk = unpack(turn)

        def moves(which):
            for quarter in range(RING):
                for begin, block, row, n in ranges(bm, 0, main):
                    yield (lambda ref, q=quarter, b=begin, n=n: ref.at[q, pl.ds(b, n)], *spot(bm, which, part, core, chunk, quarter, block, row, n))

        return [(owner, moves)]

    return place(gathered, shapes, 2 * PARTS * RING * CHUNKS, depth, load_view, spots, (RING, main, bn))


def place_rest(gathered, mesh_shape, shapes, earlier):
    n_dev, _, n_rows, bn = gathered.shape
    bm = bn // 2
    n_z, n_y, n_xc = mesh_shape
    begin_row = BLOCKS * (bm // 4) - n_rows
    group = 8
    depth = 8

    def load_view(ref, turn):
        return ref.at[pl.ds(turn * group, group)]

    def spots(turn):
        found = []
        for k in range(group):
            dev = turn * group + k
            xc, y, z = lax.rem(dev, n_xc), lax.rem(lax.div(dev, n_xc), n_y), lax.div(dev, n_xc * n_y)
            x, core = lax.div(xc, 2), lax.rem(xc, 2)
            for part in range(PARTS):
                owner, chunk, quarter = ((x, y, z), (y, z, x), (z, x, y))[part]

                def moves(which, k=k, part=part, core=core, chunk=chunk, quarter=quarter):
                    for begin, block, row, n in ranges(bm, begin_row, begin_row + n_rows):
                        yield (lambda ref, b=begin - begin_row, n=n: ref.at[k, part, pl.ds(b, n)], *spot(bm, which, part, core, chunk, quarter, block, row, n))

                found.append((owner, moves))
        return found

    return place(gathered, shapes, n_dev // group, depth, load_view, spots, (group, PARTS, n_rows, bn), earlier)


def place(gathered, shapes, n_turns, depth, load_view, spots, slot_shape, earlier=()):
    return pl.pallas_call(
        functools.partial(place_kernel, n_turns, depth, load_view, spots),
        name="place_grads",
        out_shape=[jax.ShapeDtypeStruct(s, jnp.float32) for s in shapes],
        in_specs=[pl.BlockSpec(memory_space=pl.ANY)] * (1 + len(earlier)),
        out_specs=[pl.BlockSpec(memory_space=pl.ANY)] * 4,
        scratch_shapes=[pltpu.VMEM((depth, *slot_shape), jnp.float32), pltpu.SemaphoreType.DMA((depth,)), pltpu.SemaphoreType.DMA((depth,))],
        input_output_aliases={1 + k: k for k in range(len(earlier))},
        cost_estimate=pl.CostEstimate(flops=8 * gathered.size, bytes_accessed=8 * gathered.size, transcendentals=0),
    )(gathered, *earlier)


def solution(mesh):
    n_dev = math.prod(mesh.shape.values())
    axes = ("z", "y", "xc")
    batch_spec = P(axes, None)
    whole_spec = P(None, None)

    def device_step(x_loc, g_loc, w_one, w_two, w_three, w_four):
        main, rest = reduce_grads(x_loc, g_loc, (w_one, w_two, w_three, w_four), n_dev)
        all_rest = lax.all_gather(rest, axes, axis=0)
        shapes = (w_one.shape, w_two.shape, w_three.shape, w_four.shape)
        mesh_shape = tuple(mesh.shape[name] for name in axes)
        return tuple(place_rest(all_rest, mesh_shape, shapes, place_main(main, shapes)))

    return jax.shard_map(
        device_step,
        mesh=mesh,
        in_specs=(batch_spec, batch_spec, whole_spec, whole_spec, whole_spec, whole_spec),
        out_specs=(whole_spec, whole_spec, whole_spec, whole_spec),
        check_vma=False,
    )
```

```python
import functools
import math
import jax
import jax.numpy as jnp
from jax import lax
from jax.experimental import pallas as pl
from jax.experimental.pallas import tpu as pltpu
from jax.sharding import PartitionSpec as P

GELU_SCALE = math.sqrt(2.0 / math.pi)
GELU_CUBIC = 0.044715
MESH = pl.DeviceIdType.MESH
RING = 4
PARTS = 3
CHUNKS = 4
BLOCKS = 3
LEAD = 3
LAG = 12
WAYS = (0, 1)
PIECES = 3


def gelu_value(pre_act):
    return 0.5 * pre_act * (1.0 + jnp.tanh(GELU_SCALE * (pre_act + GELU_CUBIC * pre_act * pre_act * pre_act)))


def gelu_grad(pre_act):
    tanh_val = jnp.tanh(GELU_SCALE * (pre_act + GELU_CUBIC * pre_act * pre_act * pre_act))
    return 0.5 * (1.0 + tanh_val) + 0.5 * pre_act * (1.0 - tanh_val * tanh_val) * GELU_SCALE * (1.0 + 3.0 * GELU_CUBIC * pre_act * pre_act)


def pick(index, values):
    chosen = values[-1]
    for k in range(len(values) - 2, -1, -1):
        chosen = jnp.where(index == k, values[k], chosen)
    return chosen


def reduce_kernel(rows, bm, scale, *refs):
    bn = 2 * bm
    x_in, g_in, w_one, w_two, w_three, w_four = refs[0:6]
    gath, rest, relay_wid, relay_hid, hid_out, wid_out, a_one = refs[6:13]
    hid = tuple(hid_out.at[which] for which in range(4))
    wid = (x_in, wid_out.at[0], wid_out.at[1], g_in)
    hid_v, wid_v, stage, ring2, result = refs[13:18]
    (free_sem, act_sem, weight_sem, tile_sem, own_sem, near_send, near_recv, hop_send, hop_recv, fwd_send, fwd_recv,
     stage_send, stage_recv, r1_send, r1_recv, r2_send, r2_recv,
     local_sem, g_send, g1_recv, g2_recv, g3_recv, cross_send, cross_recv) = refs[18:]
    n_stage = stage.shape[0]
    half_rows = rows // 2

    z, y, xc = lax.axis_index("z"), lax.axis_index("y"), lax.axis_index("xc")
    x, core = lax.div(xc, 2), lax.rem(xc, 2)
    coord = (x, y, z)
    first, second = (y, z, x), (z, x, y)
    partner = (z, y, x * 2 + (1 - core))

    def shifted(axis, direction):
        to = lax.rem(coord[axis] + (1 if direction == 0 else RING - 1), RING)
        return ((z, y, to * 2 + core), (z, to, xc), (to, y, xc))[axis]

    def tell_neighbours(sem):
        for axis in range(3):
            for direction in WAYS:
                pl.semaphore_signal(sem, inc=1, device_id=shifted(axis, direction), device_id_type=MESH)
        pl.semaphore_signal(sem, inc=1, device_id=partner, device_id_type=MESH)

    barrier = pltpu.get_barrier_semaphore()
    tell_neighbours(barrier)

    def source(piece, part, which, row, n):
        if piece == 0:
            return wid[which].at[pl.ds(row, n)]
        side = 1 - core if piece == 1 else core
        return hid[which].at[pl.ds(row, n), pl.ds(pl.multiple_of((8 * part + 4 * side) * bm, 4 * bm), 4 * bm)]

    def landing(piece, part, slot, row, n):
        if piece == 0:
            return wid_v.at[part, pl.ds(slot * rows + row, n)]
        return hid_v.at[(piece - 1) * PARTS + part, pl.ds(slot * rows + row, n)]

    def relay(piece, part, direction):
        if piece == 0:
            return relay_wid.at[part, direction]
        return relay_hid.at[piece - 1, part, direction]

    def own(piece, part, which):
        return pltpu.make_async_copy(source(piece, part, which, 0, rows), landing(piece, part, 0, 0, rows), own_sem.at[piece, part])

    def near(piece, part, direction, which):
        return pltpu.make_async_remote_copy(
            src_ref=source(piece, part, which, 0, rows), dst_ref=landing(piece, part, 1 + 2 * direction, 0, rows),
            send_sem=near_send.at[piece, part, direction], recv_sem=near_recv.at[piece, part, direction],
            device_id=shifted(part, direction), device_id_type=MESH)

    def hop(piece, part, direction, which):
        return pltpu.make_async_remote_copy(
            src_ref=source(piece, part, which, direction * half_rows, half_rows), dst_ref=relay(piece, part, direction),
            send_sem=hop_send.at[piece, part, direction], recv_sem=hop_recv.at[piece, part, direction],
            device_id=shifted(part, direction), device_id_type=MESH)

    def forward(piece, part, direction):
        return pltpu.make_async_remote_copy(
            src_ref=relay(piece, part, direction), dst_ref=landing(piece, part, 2, direction * half_rows, half_rows),
            send_sem=fwd_send.at[piece, part, direction], recv_sem=fwd_recv.at[piece, part, direction],
            device_id=shifted(part, direction), device_id_type=MESH)

    def start_for(copy, owner, ready):
        for which in ready:
            @pl.when(owner == which)
            def _():
                copy(which).start()

    def send_out(piece, ready=(0, 1, 2, 3)):
        for part in range(PARTS):
            for direction in WAYS:
                start_for(functools.partial(hop, piece, part, direction), lax.rem(coord[part] + 2, RING), ready)
        for part in range(PARTS):
            for direction in WAYS:
                start_for(functools.partial(near, piece, part, direction), lax.rem(coord[part] + (1 if direction == 0 else 3), RING), ready)

    def start_own(piece):
        for part in range(PARTS):
            start_for(functools.partial(own, piece, part), coord[part], (0, 1, 2, 3))

    def pass_on(piece, ready=None):
        for part in range(PARTS):
            for direction in WAYS:
                def relay_one():
                    hop(piece, part, direction, 0).wait_recv()
                    forward(piece, part, direction).start()

                if ready is None:
                    relay_one()
                    continue
                owner = lax.rem(coord[part] + (1 if direction == 0 else 3), RING)
                for which in ready:
                    pl.when(owner == which)(relay_one)

    def arrived(piece, part):
        own(piece, part, 0).wait()
        for direction in WAYS:
            near(piece, part, direction, 0).wait_recv()
            forward(piece, part, direction).wait_recv()

    tiles, lead = 12, weight_sem.shape[1] - 1

    def hidden(tile):
        return pl.ds(pl.multiple_of(tile * bn, bn), bn)

    def rounded(value):
        return value.astype(jnp.bfloat16)

    def widened(value):
        return value.astype(jnp.float32)

    def mm(left, right, transposed=False):
        return lax.dot_general(left, right, (((1,), (1 if transposed else 0,)), ((), ())), preferred_element_type=jnp.float32)

    def products(columns_v, rows_v, acts, out_tiles, total):
        def weight_copy(kind, weight, tile):
            slot = lax.rem(tile, lead + 1)
            if kind == 0:
                return pltpu.make_async_copy(weight.at[:, hidden(tile)], columns_v.at[slot], weight_sem.at[kind, slot])
            return pltpu.make_async_copy(weight.at[hidden(tile)], rows_v.at[slot], weight_sem.at[kind, slot])

        def tile_copy(index, ref, tile, out=True):
            ends = (out_tiles.at[index], ref.at[:, hidden(tile)])
            return pltpu.make_async_copy(*(ends if out else ends[::-1]), tile_sem.at[index])

        def close_total(base, index, ref, sem):
            acts[index] = rounded(total[...] + widened(acts[base]))
            copy = pltpu.make_async_copy(acts.at[index], ref, act_sem.at[sem])
            copy.start()
            copy.wait()

        def sweep(weights, following, step, outs):
            def turn(tile, carry):
                for kind, weight in weights:
                    @pl.when(tile < tiles - lead)
                    def _():
                        weight_copy(kind, weight, tile + lead).start()

                for kind, weight in following:
                    @pl.when(tile >= tiles - lead)
                    def _():
                        weight_copy(kind, weight, tile + lead - tiles).start()

                for kind, weight in weights:
                    weight_copy(kind, weight, tile).wait()
                slot = lax.rem(tile, 2)

                @pl.when(tile >= 2)
                def _():
                    for k, ref in enumerate(outs):
                        tile_copy(2 * k + slot, ref, tile).wait()

                step(tile, slot, lax.rem(tile, lead + 1))
                for k, ref in enumerate(outs):
                    tile_copy(2 * k + slot, ref, tile).start()
                return carry

            lax.fori_loop(0, tiles, turn, 0)
            for slot in WAYS:
                for k, ref in enumerate(outs):
                    tile_copy(2 * k + slot, ref, slot).wait()

        for tile in range(lead):
            weight_copy(0, w_one, tile).start()
            weight_copy(1, w_two, tile).start()
        loads = [pltpu.make_async_copy(ref, acts.at[k], act_sem.at[k]) for k, ref in enumerate((x_in, g_in))]
        for copy in loads:
            copy.start()
        total[...] = jnp.zeros(total.shape, jnp.float32)
        pl.semaphore_wait(barrier, 7)
        send_out(0, (0, 3))
        for copy in loads:
            copy.wait()

        def first_forward(tile, slot, load):
            pre = rounded(mm(acts[0], columns_v[load]))
            out_tiles[slot] = pre
            act = rounded(gelu_value(widened(pre)))
            out_tiles[2 + slot] = act
            total[...] = total[...] + mm(act, rows_v[load])

        with jax.named_scope("first_forward"):
            sweep(((0, w_one), (1, w_two)), ((0, w_three), (1, w_four)), first_forward, (a_one, hid[1]))
            close_total(0, 2, wid[2], 2)
        total[...] = jnp.zeros(total.shape, jnp.float32)
        send_out(0, (2,))
        send_out(1, (1,))
        send_out(2, (1,))
        pass_on(0, (0, 3))

        def second_block(tile, slot, load):
            pre = widened(rounded(mm(acts[2], columns_v[load])))
            back = mm(acts[1], rows_v[load], True)
            tanh_val = jnp.tanh(GELU_SCALE * (pre + GELU_CUBIC * pre * pre * pre))
            out_tiles[slot] = rounded(0.5 * pre * (1.0 + tanh_val))
            slope = 0.5 * (1.0 + tanh_val) + 0.5 * pre * (1.0 - tanh_val * tanh_val) * GELU_SCALE * (1.0 + 3.0 * GELU_CUBIC * pre * pre)
            grad = rounded(back * slope)
            out_tiles[2 + slot] = grad
            total[...] = total[...] + mm(grad, columns_v[load], True)

        with jax.named_scope("second_block"):
            sweep(((0, w_three), (1, w_four)), ((1, w_two),), second_block, (hid[3], hid[2]))
            close_total(1, 0, wid[1], 3)
        send_out(0, (1,))
        send_out(1, (2, 3))
        send_out(2, (2, 3))
        pass_on(0, (2,))
        pass_on(1, (1,))
        pass_on(2, (1,))

        def reload(tile):
            return tile_copy(2 + lax.rem(tile, 2), a_one, tile, out=False)

        reload(0).start()

        def first_backward(tile, slot, load):
            @pl.when(tile < tiles - 1)
            def _():
                reload(tile + 1).start()

            reload(tile).wait()
            back = mm(acts[0], rows_v[load], True)
            out_tiles[slot] = rounded(back * gelu_grad(widened(out_tiles[2 + slot])))

        with jax.named_scope("first_backward"):
            sweep(((1, w_two),), (), first_backward, (hid[0],))

    width = wid_v.shape[-1]
    pl.run_scoped(
        products, pltpu.VMEM((lead + 1, width, bn), jnp.bfloat16), pltpu.VMEM((lead + 1, bn, width), jnp.bfloat16),
        pltpu.VMEM((3, rows, width), jnp.bfloat16), pltpu.VMEM((4, rows, bn), jnp.bfloat16), pltpu.VMEM((rows, width), jnp.float32))

    def sums(acc, ring1):
        def product(side, part, chunk, block, store):
            odd = lax.rem(pick(part, coord), 2)
            dims = (((0,), (0,)), ((), ()))

            @pl.when(odd == 1)
            def _():
                left = hid_v[side * PARTS + part, :, pl.ds(pl.multiple_of(chunk * bm, bm), bm)]
                right = wid_v[part, :, pl.ds(pl.multiple_of(block * bn, bn), bn)]
                store(lax.dot_general(left, right, dims, preferred_element_type=jnp.float32))

            @pl.when(odd == 0)
            def _():
                index = 3 * chunk + block
                left = wid_v[part, :, pl.ds(pl.multiple_of(lax.div(index, 2) * bm, bm), bm)]
                right = hid_v[side * PARTS + part, :, pl.ds(pl.multiple_of(lax.rem(index, 2) * bn, bn), bn)]
                store(lax.dot_general(left, right, dims, preferred_element_type=jnp.float32))

        def hand_over(part, chunk, block, slot):
            return pltpu.make_async_remote_copy(
                src_ref=stage.at[slot], dst_ref=acc.at[part, chunk, block], send_sem=stage_send.at[slot],
                recv_sem=stage_recv.at[part, chunk, block], device_id=partner, device_id_type=MESH)

        tell_neighbours(free_sem)
        with jax.named_scope("send_last"):
            send_out(1, (0,))
            pass_on(0, (1,))
            pass_on(1, (2, 3))
            pass_on(2, (2, 3))
            pass_on(1, (0,))
            send_out(2, (0,))
            for piece in range(PIECES):
                start_own(piece)
        with jax.named_scope("await_other"):
            pl.semaphore_wait(free_sem, 7)
            for piece in range(PIECES - 1):
                for part in range(PARTS):
                    arrived(piece, part)

        top, low = bm // 2, bm // 8

        def ring1_copy(part, direction, step, block):
            chunk = lax.rem(first[part] + (RING - 1 - step if direction == 0 else 1 + step), RING)
            return pltpu.make_async_remote_copy(
                src_ref=acc.at[part, chunk, block, pl.ds(direction * top, top)], dst_ref=ring1.at[part, direction, step, block],
                send_sem=r1_send.at[part, direction, block], recv_sem=r1_recv.at[part, direction, step, block],
                device_id=shifted((part + 1) % 3, direction), device_id_type=MESH)

        def place_of(count):
            order, rest = lax.div(count, PARTS * BLOCKS), lax.rem(count, PARTS * BLOCKS)
            part, block = lax.rem(rest, PARTS), lax.div(rest, PARTS)
            return order, part, lax.rem(pick(part, first) + pick(order, (3, 1, 2, 0)), RING), block

        blocks = CHUNKS * PARTS * BLOCKS

        def both_halves(count, carry):
            @pl.when(count < blocks)
            def _():
                _, part, chunk, block = place_of(count)
                slot = lax.rem(count, n_stage)

                @pl.when(count >= n_stage)
                def _():
                    hand_over(0, 0, 0, slot).wait_send()

                def store(value):
                    stage[slot] = value

                product(0, part, chunk, block, store)
                hand_over(part, chunk, block, slot).start()

            @pl.when(count >= LAG)
            def _():
                order, part, chunk, block = place_of(count - LAG)
                hand_over(part, chunk, block, 0).wait_recv()

                def store(value):
                    acc[part, chunk, block] = acc[part, chunk, block] + value

                product(1, part, chunk, block, store)
                for direction in WAYS:
                    for which in range(PARTS):
                        @pl.when((order == direction) & (part == which))
                        def _():
                            ring1_copy(which, direction, 0, block).start()

            return carry

        def ring1_step(step):
            for block in range(BLOCKS):
                for part in range(PARTS):
                    for direction in WAYS:
                        ring1_copy(part, direction, step, block).wait_recv()
                        chunk = lax.rem(first[part] + (RING - 2 - step if direction == 0 else 2 + step), RING)
                        share = acc.at[part, chunk, block, pl.ds(direction * top, top)]
                        share[...] = share[...] + ring1[part, direction, step, block]
                        ring1_copy(part, direction, step, block).wait_send()
                        if step < RING - 2:
                            ring1_copy(part, direction, step + 1, block).start()
                    if step == RING - 2:
                        for direction in WAYS:
                            ring2_copy(part, direction, 0, block).start()

        with jax.named_scope("other_half"):
            lax.fori_loop(0, LAG, both_halves, 0)
        with jax.named_scope("await_own"):
            pass_on(2, (0,))
            for part in range(PARTS):
                arrived(2, part)
        last = blocks - PARTS * BLOCKS
        with jax.named_scope("halves"):
            lax.fori_loop(LAG, last + LAG, both_halves, 0)
        def ring2_share(part, direction, block, place):
            row = pl.multiple_of(2 * low * place + direction * low, low)
            return acc.at[part, first[part], block, pl.ds(row, low)]

        def ring2_copy(part, direction, step, block):
            place = lax.rem(second[part] + (RING - 1 - step if direction == 0 else 1 + step), RING)
            return pltpu.make_async_remote_copy(
                src_ref=ring2_share(part, direction, block, place), dst_ref=ring2.at[part, direction, step, block],
                send_sem=r2_send.at[part, direction, block], recv_sem=r2_recv.at[part, direction, step, block],
                device_id=shifted((part + 2) % 3, direction), device_id_type=MESH)

        with jax.named_scope("ring1#step=0"):
            ring1_step(0)
        with jax.named_scope("last_chunk"):
            lax.fori_loop(last + LAG, blocks + LAG, both_halves, 0)
        for step in range(1, RING - 1):
            with jax.named_scope(f"ring1#step={step}"):
                ring1_step(step)

        with jax.named_scope("ring2"):
            for step in range(RING - 1):
                for block in range(BLOCKS):
                    for part in range(PARTS):
                        for direction in WAYS:
                            ring2_copy(part, direction, step, block).wait_recv()
                            place = lax.rem(second[part] + (RING - 2 - step if direction == 0 else 2 + step), RING)
                            share = ring2_share(part, direction, block, place)
                            value = share[...] + ring2[part, direction, step, block]
                            ring2_copy(part, direction, step, block).wait_send()
                            if step < RING - 2:
                                share[...] = value
                                ring2_copy(part, direction, step + 1, block).start()
                            else:
                                result[part, pl.ds(2 * low * block + direction * low, low)] = value * scale

        for slot in range(n_stage):
            hand_over(0, 0, 0, slot).wait_send()

    pl.run_scoped(
        sums, pltpu.VMEM((PARTS, CHUNKS, BLOCKS, bm, bn), jnp.float32),
        pltpu.VMEM((PARTS, 2, RING - 1, BLOCKS, bm // 2, bn), jnp.float32))

    main, piece_rows = gath.shape[5], result.shape[1]
    cut = main // 16 * 8

    def after(place, by):
        return lax.rem(place + by, RING)

    def at(part, owner, chunk, quarter=None):
        view = gath.at[core, part, owner, chunk]
        return view if quarter is None else view.at[quarter]

    def send(src, dst, sem, recv, axis, direction):
        return pltpu.make_async_remote_copy(
            src_ref=src, dst_ref=dst, send_sem=sem, recv_sem=recv, device_id=shifted(axis, direction), device_id_type=MESH)

    def quarter_copy(part, direction, leg):
        sem, recv = g_send.at[0, part], g1_recv.at[part, direction, leg]
        axis = (part + 2) % 3
        if leg == 0:
            src, dst = result.at[part, pl.ds(0, main)], at(part, coord[part], first[part], second[part])
            return send(src, dst, sem, recv, axis, direction)
        view = at(part, coord[part], first[part], after(second[part], 3 - 2 * direction))
        view = view.at[pl.ds(0, cut)] if direction == 0 else view.at[pl.ds(cut, main - cut)]
        return send(view, view, sem, recv, axis, direction)

    def chunk_copy(part, direction, leg):
        sem, recv = g_send.at[1, part], g2_recv.at[part, direction, leg]
        axis = (part + 1) % 3
        view = at(part, coord[part], first[part])
        if leg == 1:
            view = at(part, coord[part], after(first[part], 3 - 2 * direction)).at[pl.ds(2 * direction, 2)]
        return send(view, view, sem, recv, axis, direction)

    def owner_copy(part, direction, leg, order):
        sem, recv = g_send.at[2, part], g3_recv.at[part, direction, leg, order]
        chunk = after(first[part], (0, 3, 1, 2)[order])
        view = at(part, coord[part], chunk)
        if leg == 1:
            view = at(part, after(coord[part], 3 - 2 * direction), chunk).at[pl.ds(2 * direction, 2)]
        return send(view, view, sem, recv, part, direction)

    def cross(part, owner_by, order):
        view = at(part, after(coord[part], owner_by), after(first[part], (0, 3, 1, 2)[order]))
        return pltpu.make_async_remote_copy(
            src_ref=view, dst_ref=view, send_sem=cross_send, recv_sem=cross_recv, device_id=partner, device_id_type=MESH)

    def keep(part):
        return pltpu.make_async_copy(
            result.at[part, pl.ds(0, main)], at(part, coord[part], first[part], second[part]), local_sem.at[part])

    spare = pltpu.make_async_copy(result.at[:, pl.ds(main, piece_rows - main)], rest, local_sem.at[PARTS])
    with jax.named_scope("gather"):
        for part in range(PARTS):
            for direction in WAYS:
                quarter_copy(part, direction, 0).start()
            keep(part).start()
        spare.start()
        for part in range(PARTS):
            for direction in WAYS:
                quarter_copy(part, direction, 0).wait_recv()
                quarter_copy(part, direction, 1).start()
        for part in range(PARTS):
            keep(part).wait()
            for direction in WAYS:
                quarter_copy(part, direction, 1).wait_recv()
            for direction in WAYS:
                chunk_copy(part, direction, 0).start()
            for direction in WAYS:
                owner_copy(part, direction, 0, 0).start()
            cross(part, 0, 0).start()
        for part in range(PARTS):
            for direction in WAYS:
                chunk_copy(part, direction, 0).wait_recv()
                chunk_copy(part, direction, 1).start()
            for order in (1, 2):
                for direction in WAYS:
                    owner_copy(part, direction, 0, order).start()
                cross(part, 0, order).start()
        for part in range(PARTS):
            for direction in WAYS:
                chunk_copy(part, direction, 1).wait_recv()
            for direction in WAYS:
                owner_copy(part, direction, 0, 3).start()
            cross(part, 0, 3).start()
        for order in range(CHUNKS):
            for part in range(PARTS):
                for direction in WAYS:
                    owner_copy(part, direction, 0, order).wait_recv()
                    owner_copy(part, direction, 1, order).start()
                    cross(part, 3 - 2 * direction, order).start()
        for order in range(CHUNKS):
            for part in range(PARTS):
                for direction in WAYS:
                    owner_copy(part, direction, 1, order).wait_recv()
                cross(part, 2, order).start()

    for piece in range(PIECES):
        for part in range(PARTS):
            for direction in WAYS:
                near(piece, part, direction, 0).wait_send()
                hop(piece, part, direction, 0).wait_send()
                forward(piece, part, direction).wait_send()
    spare.wait()

    def drain(view, sem):
        pltpu.make_async_copy(view, view, sem).wait()

    for part in range(PARTS):
        drain(gath.at[core, part, 0, 0, pl.ds(0, 3)], g_send.at[0, part])
        drain(gath.at[core, part, 0, pl.ds(0, 3)], g_send.at[1, part])
        drain(gath.at[core, part, pl.ds(0, 3)], g_send.at[2, part])
    drain(gath.at[core], cross_send)
    drain(gath.at[1 - core], cross_recv)


def reduce_grads(x_loc, g_loc, weights, n_dev):
    rows, width = x_loc.shape
    bm = width // 6
    bn = 2 * bm
    dma = pltpu.SemaphoreType.DMA
    any_spec = pl.BlockSpec(memory_space=pl.ANY)
    f32, bf16 = jnp.float32, jnp.bfloat16
    n_stage = 4
    piece_rows = BLOCKS * (bm // 4)
    main = piece_rows * 7 // 64 * 8
    outs = pl.pallas_call(
        functools.partial(reduce_kernel, rows, bm, 1.0 / n_dev),
        name="reduce_grads",
        out_shape=[
            jax.ShapeDtypeStruct((2, PARTS, RING, CHUNKS, RING, main, bn), f32),
            jax.ShapeDtypeStruct((PARTS, piece_rows - main, bn), f32),
            jax.ShapeDtypeStruct((PARTS, 2, rows // 2, width), bf16),
            jax.ShapeDtypeStruct((2, PARTS, 2, rows // 2, 4 * bm), bf16),
            jax.ShapeDtypeStruct((4, rows, 24 * bm), bf16),
            jax.ShapeDtypeStruct((2, rows, width), bf16),
            jax.ShapeDtypeStruct((rows, 24 * bm), bf16),
        ],
        in_specs=[any_spec] * 6,
        out_specs=[any_spec] * 7,
        scratch_shapes=[
            pltpu.VMEM((2 * PARTS, RING * rows, 4 * bm), bf16),
            pltpu.VMEM((PARTS, RING * rows, width), bf16),
            pltpu.VMEM((n_stage, bm, bn), f32),
            pltpu.VMEM((PARTS, 2, RING - 1, BLOCKS, bm // 8, bn), f32),
            pltpu.VMEM((PARTS, piece_rows, bn), f32),
            pltpu.SemaphoreType.REGULAR, dma((4,)), dma((2, LEAD + 1)), dma((4,)),
            dma((PIECES, PARTS)),
            dma((PIECES, PARTS, 2)), dma((PIECES, PARTS, 2)),
            dma((PIECES, PARTS, 2)), dma((PIECES, PARTS, 2)),
            dma((PIECES, PARTS, 2)), dma((PIECES, PARTS, 2)),
            dma((n_stage,)), dma((PARTS, CHUNKS, BLOCKS)),
            dma((PARTS, 2, BLOCKS)), dma((PARTS, 2, RING - 1, BLOCKS)),
            dma((PARTS, 2, BLOCKS)), dma((PARTS, 2, RING - 1, BLOCKS)),
            dma((PARTS + 1,)), dma((3, PARTS)),
            dma((PARTS, 2, 2)), dma((PARTS, 2, 2)), dma((PARTS, 2, 2, CHUNKS)),
            dma, dma,
        ],
        compiler_params=pltpu.CompilerParams(collective_id=0, has_side_effects=True, vmem_limit_bytes=67043328),
        cost_estimate=pl.CostEstimate(flops=40 * rows * 24 * bm * width, bytes_accessed=200_000_000, transcendentals=0),
    )(x_loc, g_loc, *weights)
    return outs[0], outs[1]


def place_kernel(n_turns, depth, load_view, spots, *refs):
    gathered, dsts = refs[0], refs[-7:-3]
    slots, in_sem, out_sem = refs[-3:]
    ahead = depth // 2

    def load(turn):
        slot = lax.rem(turn, depth)
        return pltpu.make_async_copy(load_view(gathered, turn), slots.at[slot], in_sem.at[slot])

    def drain(turn):
        slot = lax.rem(turn, depth)
        return pltpu.make_async_copy(slots.at[slot], load_view(gathered, 0), out_sem.at[slot])

    def store(turn):
        slot = lax.rem(turn, depth)
        for owner, moves in spots(turn):
            for which in range(4):
                @pl.when(owner == which)
                def _():
                    for view, rows, cols in moves(which):
                        pltpu.make_async_copy(view(slots.at[slot]), dsts[which].at[rows, cols], out_sem.at[slot]).start()

    def prime(turn, carry):
        load(turn).start()
        return carry

    def body(turn, carry):
        @pl.when(turn + ahead < n_turns)
        def _():
            @pl.when(turn + ahead >= depth)
            def _():
                drain(turn + ahead - depth).wait()

            load(turn + ahead).start()

        load(turn).wait()
        store(turn)
        return carry

    def finish(turn, carry):
        drain(turn).wait()
        return carry

    lax.fori_loop(0, ahead, prime, 0)
    lax.fori_loop(0, n_turns, body, 0)
    lax.fori_loop(n_turns - depth, n_turns, finish, 0)


def spot(bm, which, part, core, chunk, quarter, block, row, n):
    bn = 2 * bm
    if which % 2 == 1:
        start = (8 * part + 4 * core + chunk) * bm
        col = block * bn
    else:
        index = 3 * chunk + block
        start = lax.div(index, 2) * bm
        col = (4 * part + 2 * core + lax.rem(index, 2)) * bn
    start = start + quarter * (bm // 4) + row
    return pl.ds(pl.multiple_of(start, 8), n), pl.ds(pl.multiple_of(col, bn), bn)


def ranges(bm, begin, end):
    quarter = bm // 4
    for block in range(BLOCKS):
        low, high = max(begin, block * quarter), min(end, (block + 1) * quarter)
        if low < high:
            yield low, block, low - block * quarter, high - low


def place_main(gathered, shapes):
    main, bn = gathered.shape[5:]
    bm = bn // 2
    depth = 12

    def unpack(turn):
        chunk = lax.rem(turn, CHUNKS)
        owner = lax.rem(lax.div(turn, CHUNKS), RING)
        part = lax.rem(lax.div(turn, CHUNKS * RING), PARTS)
        return lax.div(turn, CHUNKS * RING * PARTS), part, owner, chunk

    def load_view(ref, turn):
        return ref.at[unpack(turn)]

    def spots(turn):
        core, part, owner, chunk = unpack(turn)

        def moves(which):
            for quarter in range(RING):
                for begin, block, row, n in ranges(bm, 0, main):
                    yield (lambda ref, q=quarter, b=begin, n=n: ref.at[q, pl.ds(b, n)], *spot(bm, which, part, core, chunk, quarter, block, row, n))

        return [(owner, moves)]

    return place(gathered, shapes, 2 * PARTS * RING * CHUNKS, depth, load_view, spots, (RING, main, bn))


def place_rest(gathered, mesh_shape, shapes, earlier):
    n_dev, _, n_rows, bn = gathered.shape
    bm = bn // 2
    n_z, n_y, n_xc = mesh_shape
    begin_row = BLOCKS * (bm // 4) - n_rows
    group = 8
    depth = 8

    def load_view(ref, turn):
        return ref.at[pl.ds(turn * group, group)]

    def spots(turn):
        found = []
        for k in range(group):
            dev = turn * group + k
            xc, y, z = lax.rem(dev, n_xc), lax.rem(lax.div(dev, n_xc), n_y), lax.div(dev, n_xc * n_y)
            x, core = lax.div(xc, 2), lax.rem(xc, 2)
            for part in range(PARTS):
                owner, chunk, quarter = ((x, y, z), (y, z, x), (z, x, y))[part]

                def moves(which, k=k, part=part, core=core, chunk=chunk, quarter=quarter):
                    for begin, block, row, n in ranges(bm, begin_row, begin_row + n_rows):
                        yield (lambda ref, b=begin - begin_row, n=n: ref.at[k, part, pl.ds(b, n)], *spot(bm, which, part, core, chunk, quarter, block, row, n))

                found.append((owner, moves))
        return found

    return place(gathered, shapes, n_dev // group, depth, load_view, spots, (group, PARTS, n_rows, bn), earlier)


def place(gathered, shapes, n_turns, depth, load_view, spots, slot_shape, earlier=()):
    return pl.pallas_call(
        functools.partial(place_kernel, n_turns, depth, load_view, spots),
        name="place_grads",
        out_shape=[jax.ShapeDtypeStruct(s, jnp.float32) for s in shapes],
        in_specs=[pl.BlockSpec(memory_space=pl.ANY)] * (1 + len(earlier)),
        out_specs=[pl.BlockSpec(memory_space=pl.ANY)] * 4,
        scratch_shapes=[pltpu.VMEM((depth, *slot_shape), jnp.float32), pltpu.SemaphoreType.DMA((depth,)), pltpu.SemaphoreType.DMA((depth,))],
        input_output_aliases={1 + k: k for k in range(len(earlier))},
        cost_estimate=pl.CostEstimate(flops=8 * gathered.size, bytes_accessed=8 * gathered.size, transcendentals=0),
    )(gathered, *earlier)


def solution(mesh):
    n_dev = math.prod(mesh.shape.values())
    axes = ("z", "y", "xc")
    batch_spec = P(axes, None)
    whole_spec = P(None, None)

    def device_step(x_loc, g_loc, w_one, w_two, w_three, w_four):
        main, rest = reduce_grads(x_loc, g_loc, (w_one, w_two, w_three, w_four), n_dev)
        all_rest = lax.all_gather(rest, axes, axis=0)
        shapes = (w_one.shape, w_two.shape, w_three.shape, w_four.shape)
        mesh_shape = tuple(mesh.shape[name] for name in axes)
        return tuple(place_rest(all_rest, mesh_shape, shapes, place_main(main, shapes)))

    return jax.shard_map(
        device_step,
        mesh=mesh,
        in_specs=(batch_spec, batch_spec, whole_spec, whole_spec, whole_spec, whole_spec),
        out_specs=(whole_spec, whole_spec, whole_spec, whole_spec),
        check_vma=False,
    )
```

```python
import functools
import math
import jax
import jax.numpy as jnp
from jax import lax
from jax.experimental import pallas as pl
from jax.experimental.pallas import tpu as pltpu
from jax.sharding import PartitionSpec as P

GELU_SCALE = math.sqrt(2.0 / math.pi)
GELU_CUBIC = 0.044715
MESH = pl.DeviceIdType.MESH
RING = 4
PARTS = 3
CHUNKS = 4
BLOCKS = 3
LEAD = 3
LAG = 12
WAYS = (0, 1)
PIECES = 3


def gelu_value(pre_act):
    return 0.5 * pre_act * (1.0 + jnp.tanh(GELU_SCALE * (pre_act + GELU_CUBIC * pre_act * pre_act * pre_act)))


def gelu_grad(pre_act):
    tanh_val = jnp.tanh(GELU_SCALE * (pre_act + GELU_CUBIC * pre_act * pre_act * pre_act))
    return 0.5 * (1.0 + tanh_val) + 0.5 * pre_act * (1.0 - tanh_val * tanh_val) * GELU_SCALE * (1.0 + 3.0 * GELU_CUBIC * pre_act * pre_act)


def pick(index, values):
    chosen = values[-1]
    for k in range(len(values) - 2, -1, -1):
        chosen = jnp.where(index == k, values[k], chosen)
    return chosen


def reduce_kernel(rows, bm, scale, *refs):
    bn = 2 * bm
    x_in, g_in, w_one, w_two, w_three, w_four = refs[0:6]
    gath, rest, relay_wid, relay_hid, hid_out, wid_out = refs[6:12]
    hid = tuple(hid_out.at[which] for which in range(4))
    wid = (x_in, wid_out.at[0], wid_out.at[1], g_in)
    hid_v, wid_v, stage, ring2, result = refs[12:17]
    (free_sem, act_sem, weight_sem, tile_sem, own_sem, near_send, near_recv, hop_send, hop_recv, fwd_send, fwd_recv,
     stage_send, stage_recv, r1_send, r1_recv, r2_send, r2_recv,
     local_sem, g_send, g1_recv, g2_recv, g3_recv, cross_send, cross_recv) = refs[17:]
    n_stage = stage.shape[0]
    half_rows = rows // 2

    z, y, xc = lax.axis_index("z"), lax.axis_index("y"), lax.axis_index("xc")
    x, core = lax.div(xc, 2), lax.rem(xc, 2)
    coord = (x, y, z)
    first, second = (y, z, x), (z, x, y)
    partner = (z, y, x * 2 + (1 - core))

    def shifted(axis, direction):
        to = lax.rem(coord[axis] + (1 if direction == 0 else RING - 1), RING)
        return ((z, y, to * 2 + core), (z, to, xc), (to, y, xc))[axis]

    def tell_neighbours(sem):
        for axis in range(3):
            for direction in WAYS:
                pl.semaphore_signal(sem, inc=1, device_id=shifted(axis, direction), device_id_type=MESH)
        pl.semaphore_signal(sem, inc=1, device_id=partner, device_id_type=MESH)

    barrier = pltpu.get_barrier_semaphore()
    tell_neighbours(barrier)

    def source(piece, part, which, row, n):
        if piece == 0:
            return wid[which].at[pl.ds(row, n)]
        side = 1 - core if piece == 1 else core
        return hid[which].at[pl.ds(row, n), pl.ds(pl.multiple_of((8 * part + 4 * side) * bm, 4 * bm), 4 * bm)]

    def landing(piece, part, slot, row, n):
        if piece == 0:
            return wid_v.at[part, pl.ds(slot * rows + row, n)]
        return hid_v.at[(piece - 1) * PARTS + part, pl.ds(slot * rows + row, n)]

    def relay(piece, part, direction):
        if piece == 0:
            return relay_wid.at[part, direction]
        return relay_hid.at[piece - 1, part, direction]

    def own(piece, part, which):
        return pltpu.make_async_copy(source(piece, part, which, 0, rows), landing(piece, part, 0, 0, rows), own_sem.at[piece, part])

    def near(piece, part, direction, which):
        return pltpu.make_async_remote_copy(
            src_ref=source(piece, part, which, 0, rows), dst_ref=landing(piece, part, 1 + 2 * direction, 0, rows),
            send_sem=near_send.at[piece, part, direction], recv_sem=near_recv.at[piece, part, direction],
            device_id=shifted(part, direction), device_id_type=MESH)

    def hop(piece, part, direction, which):
        return pltpu.make_async_remote_copy(
            src_ref=source(piece, part, which, direction * half_rows, half_rows), dst_ref=relay(piece, part, direction),
            send_sem=hop_send.at[piece, part, direction], recv_sem=hop_recv.at[piece, part, direction],
            device_id=shifted(part, direction), device_id_type=MESH)

    def forward(piece, part, direction):
        return pltpu.make_async_remote_copy(
            src_ref=relay(piece, part, direction), dst_ref=landing(piece, part, 2, direction * half_rows, half_rows),
            send_sem=fwd_send.at[piece, part, direction], recv_sem=fwd_recv.at[piece, part, direction],
            device_id=shifted(part, direction), device_id_type=MESH)

    def start_for(copy, owner, ready):
        for which in ready:
            @pl.when(owner == which)
            def _():
                copy(which).start()

    def start_hops(piece, ready):
        for part in range(PARTS):
            for direction in WAYS:
                start_for(functools.partial(hop, piece, part, direction), lax.rem(coord[part] + 2, RING), ready)

    def start_nears(piece, ready):
        for part in range(PARTS):
            for direction in WAYS:
                start_for(functools.partial(near, piece, part, direction), lax.rem(coord[part] + (1 if direction == 0 else 3), RING), ready)

    def start_own(piece):
        for part in range(PARTS):
            start_for(functools.partial(own, piece, part), coord[part], (0, 1, 2, 3))

    def pass_on(piece, ready=None):
        for part in range(PARTS):
            for direction in WAYS:
                def relay_one():
                    hop(piece, part, direction, 0).wait_recv()
                    forward(piece, part, direction).start()

                if ready is None:
                    relay_one()
                    continue
                owner = lax.rem(coord[part] + (1 if direction == 0 else 3), RING)
                for which in ready:
                    pl.when(owner == which)(relay_one)

    def arrived(piece, part):
        own(piece, part, 0).wait()
        for direction in WAYS:
            near(piece, part, direction, 0).wait_recv()
            forward(piece, part, direction).wait_recv()

    tiles, lead = 12, weight_sem.shape[1] - 1

    def hidden(turn):
        side = jnp.where(turn < tiles // 2, 1 - core, core)
        rest = lax.rem(turn, tiles // 2)
        tile = 4 * lax.div(rest, 2) + 2 * side + lax.rem(rest, 2)
        return pl.ds(pl.multiple_of(tile * bn, bn), bn)

    def rounded(value):
        return value.astype(jnp.bfloat16)

    def widened(value):
        return value.astype(jnp.float32)

    def mm(left, right, transposed=False):
        return lax.dot_general(left, right, (((1,), (1 if transposed else 0,)), ((), ())), preferred_element_type=jnp.float32)

    def products(columns_v, rows_v, acts, out_tiles, total, a_one):
        def weight_copy(kind, weight, tile):
            slot = lax.rem(tile, lead + 1)
            if kind == 0:
                return pltpu.make_async_copy(weight.at[:, hidden(tile)], columns_v.at[slot], weight_sem.at[kind, slot])
            return pltpu.make_async_copy(weight.at[hidden(tile)], rows_v.at[slot], weight_sem.at[kind, slot])

        def tile_copy(index, ref, tile):
            return pltpu.make_async_copy(out_tiles.at[index], ref.at[:, hidden(tile)], tile_sem.at[index])

        def close_total(base, index, ref, sem):
            acts[index] = rounded(total[...] + widened(acts[base]))
            copy = pltpu.make_async_copy(acts.at[index], ref, act_sem.at[sem])
            copy.start()
            copy.wait()

        def sweep(weights, following, step, outs, midway):
            def turn(tile, carry):
                for kind, weight in weights:
                    @pl.when(tile < tiles - lead)
                    def _():
                        weight_copy(kind, weight, tile + lead).start()

                for kind, weight in following:
                    @pl.when(tile >= tiles - lead)
                    def _():
                        weight_copy(kind, weight, tile + lead - tiles).start()

                for kind, weight in weights:
                    weight_copy(kind, weight, tile).wait()
                slot = lax.rem(tile, 2)

                @pl.when(tile >= 2)
                def _():
                    for k, ref in enumerate(outs):
                        tile_copy(2 * k + slot, ref, tile).wait()

                step(tile, slot, lax.rem(tile, lead + 1))
                for k, ref in enumerate(outs):
                    tile_copy(2 * k + slot, ref, tile).start()
                return carry

            most = 2 * tiles // 3
            lax.fori_loop(0, most, turn, 0)
            midway()
            lax.fori_loop(most, tiles, turn, 0)
            for slot in WAYS:
                for k, ref in enumerate(outs):
                    tile_copy(2 * k + slot, ref, slot).wait()

        for tile in range(lead):
            weight_copy(0, w_one, tile).start()
            weight_copy(1, w_two, tile).start()
        loads = [pltpu.make_async_copy(ref, acts.at[k], act_sem.at[k]) for k, ref in enumerate((x_in, g_in))]
        for copy in loads:
            copy.start()
        total[...] = jnp.zeros(total.shape, jnp.float32)
        pl.semaphore_wait(barrier, 7)
        start_hops(0, (0, 3))
        start_nears(0, (0, 3))
        for copy in loads:
            copy.wait()

        def first_forward(tile, slot, load):
            pre = rounded(mm(acts[0], columns_v[load]))
            a_one[tile] = pre
            act = rounded(gelu_value(widened(pre)))
            out_tiles[slot] = act
            total[...] = total[...] + mm(act, rows_v[load])

        def midway_one():
            start_hops(1, (1,))
            start_nears(1, (1,))

        with jax.named_scope("first_forward"):
            sweep(((0, w_one), (1, w_two)), ((0, w_three), (1, w_four)), first_forward, (hid[1],), midway_one)
            start_hops(2, (1,))
            close_total(0, 2, wid[2], 2)
        total[...] = jnp.zeros(total.shape, jnp.float32)
        start_hops(0, (2,))
        start_nears(0, (2,))
        start_nears(2, (1,))
        pass_on(0, (0, 3))

        def second_block(tile, slot, load):
            pre = widened(rounded(mm(acts[2], columns_v[load])))
            back = mm(acts[1], rows_v[load], True)
            tanh_val = jnp.tanh(GELU_SCALE * (pre + GELU_CUBIC * pre * pre * pre))
            out_tiles[slot] = rounded(0.5 * pre * (1.0 + tanh_val))
            slope = 0.5 * (1.0 + tanh_val) + 0.5 * pre * (1.0 - tanh_val * tanh_val) * GELU_SCALE * (1.0 + 3.0 * GELU_CUBIC * pre * pre)
            grad = rounded(back * slope)
            out_tiles[2 + slot] = grad
            total[...] = total[...] + mm(grad, columns_v[load], True)

        def midway_two():
            start_hops(1, (2, 3))
            start_nears(1, (2, 3))

        with jax.named_scope("second_block"):
            sweep(((0, w_three), (1, w_four)), ((1, w_two),), second_block, (hid[3], hid[2]), midway_two)
            start_hops(2, (2, 3))
            close_total(1, 0, wid[1], 3)
        start_hops(0, (1,))
        start_nears(0, (1,))
        start_nears(2, (2, 3))

        def first_backward(tile, slot, load):
            back = mm(acts[0], rows_v[load], True)
            out_tiles[slot] = rounded(back * gelu_grad(widened(a_one[tile])))

        def midway_three():
            start_hops(1, (0,))
            start_nears(1, (0,))
            pass_on(1, (1,))
            pass_on(2, (1,))
            pass_on(0, (2,))

        with jax.named_scope("first_backward"):
            sweep(((1, w_two),), (), first_backward, (hid[0],), midway_three)
        start_hops(2, (0,))
        start_nears(2, (0,))

    width = wid_v.shape[-1]
    pl.run_scoped(
        products, pltpu.VMEM((lead + 1, width, bn), jnp.bfloat16), pltpu.VMEM((lead + 1, bn, width), jnp.bfloat16),
        pltpu.VMEM((3, rows, width), jnp.bfloat16), pltpu.VMEM((4, rows, bn), jnp.bfloat16), pltpu.VMEM((rows, width), jnp.float32),
        pltpu.VMEM((tiles, rows, bn), jnp.bfloat16))

    def sums(acc, ring1):
        def product(side, part, chunk, block, store):
            odd = lax.rem(pick(part, coord), 2)
            dims = (((0,), (0,)), ((), ()))

            @pl.when(odd == 1)
            def _():
                left = hid_v[side * PARTS + part, :, pl.ds(pl.multiple_of(chunk * bm, bm), bm)]
                right = wid_v[part, :, pl.ds(pl.multiple_of(block * bn, bn), bn)]
                store(lax.dot_general(left, right, dims, preferred_element_type=jnp.float32))

            @pl.when(odd == 0)
            def _():
                index = 3 * chunk + block
                left = wid_v[part, :, pl.ds(pl.multiple_of(lax.div(index, 2) * bm, bm), bm)]
                right = hid_v[side * PARTS + part, :, pl.ds(pl.multiple_of(lax.rem(index, 2) * bn, bn), bn)]
                store(lax.dot_general(left, right, dims, preferred_element_type=jnp.float32))

        def hand_over(part, chunk, block, slot):
            return pltpu.make_async_remote_copy(
                src_ref=stage.at[slot], dst_ref=acc.at[part, chunk, block], send_sem=stage_send.at[slot],
                recv_sem=stage_recv.at[part, chunk, block], device_id=partner, device_id_type=MESH)

        tell_neighbours(free_sem)
        with jax.named_scope("send_last"):
            pass_on(0, (1,))
            pass_on(1, (2, 3))
            pass_on(2, (2, 3))
            pass_on(1, (0,))
            for piece in range(PIECES):
                start_own(piece)
        with jax.named_scope("await_other"):
            pl.semaphore_wait(free_sem, 7)
            for piece in range(PIECES - 1):
                for part in range(PARTS):
                    arrived(piece, part)

        top, low = bm // 2, bm // 8

        def ring1_copy(part, direction, step, block):
            chunk = lax.rem(first[part] + (RING - 1 - step if direction == 0 else 1 + step), RING)
            return pltpu.make_async_remote_copy(
                src_ref=acc.at[part, chunk, block, pl.ds(direction * top, top)], dst_ref=ring1.at[part, direction, step, block],
                send_sem=r1_send.at[part, direction, block], recv_sem=r1_recv.at[part, direction, step, block],
                device_id=shifted((part + 1) % 3, direction), device_id_type=MESH)

        def place_of(count):
            order, rest = lax.div(count, PARTS * BLOCKS), lax.rem(count, PARTS * BLOCKS)
            part, block = lax.rem(rest, PARTS), lax.div(rest, PARTS)
            return order, part, lax.rem(pick(part, first) + pick(order, (3, 1, 2, 0)), RING), block

        blocks = CHUNKS * PARTS * BLOCKS

        def both_halves(count, carry):
            @pl.when(count < blocks)
            def _():
                _, part, chunk, block = place_of(count)
                slot = lax.rem(count, n_stage)

                @pl.when(count >= n_stage)
                def _():
                    hand_over(0, 0, 0, slot).wait_send()

                def store(value):
                    stage[slot] = value

                product(0, part, chunk, block, store)
                hand_over(part, chunk, block, slot).start()

            @pl.when(count >= LAG)
            def _():
                order, part, chunk, block = place_of(count - LAG)
                hand_over(part, chunk, block, 0).wait_recv()

                def store(value):
                    acc[part, chunk, block] = acc[part, chunk, block] + value

                product(1, part, chunk, block, store)
                for direction in WAYS:
                    for which in range(PARTS):
                        @pl.when((order == direction) & (part == which))
                        def _():
                            ring1_copy(which, direction, 0, block).start()

            return carry

        def ring1_step(step):
            for block in range(BLOCKS):
                for part in range(PARTS):
                    for direction in WAYS:
                        ring1_copy(part, direction, step, block).wait_recv()
                        chunk = lax.rem(first[part] + (RING - 2 - step if direction == 0 else 2 + step), RING)
                        share = acc.at[part, chunk, block, pl.ds(direction * top, top)]
                        share[...] = share[...] + ring1[part, direction, step, block]
                        ring1_copy(part, direction, step, block).wait_send()
                        if step < RING - 2:
                            ring1_copy(part, direction, step + 1, block).start()
                    if step == RING - 2:
                        for direction in WAYS:
                            ring2_copy(part, direction, 0, block).start()

        with jax.named_scope("other_half"):
            lax.fori_loop(0, LAG, both_halves, 0)
        with jax.named_scope("await_own"):
            pass_on(2, (0,))
            for part in range(PARTS):
                arrived(2, part)
        last = blocks - PARTS * BLOCKS
        with jax.named_scope("halves"):
            lax.fori_loop(LAG, last + LAG, both_halves, 0)
        def ring2_share(part, direction, block, place):
            row = pl.multiple_of(2 * low * place + direction * low, low)
            return acc.at[part, first[part], block, pl.ds(row, low)]

        def ring2_copy(part, direction, step, block):
            place = lax.rem(second[part] + (RING - 1 - step if direction == 0 else 1 + step), RING)
            return pltpu.make_async_remote_copy(
                src_ref=ring2_share(part, direction, block, place), dst_ref=ring2.at[part, direction, step, block],
                send_sem=r2_send.at[part, direction, block], recv_sem=r2_recv.at[part, direction, step, block],
                device_id=shifted((part + 2) % 3, direction), device_id_type=MESH)

        with jax.named_scope("ring1#step=0"):
            ring1_step(0)
        with jax.named_scope("last_chunk"):
            lax.fori_loop(last + LAG, blocks + LAG, both_halves, 0)
        for step in range(1, RING - 1):
            with jax.named_scope(f"ring1#step={step}"):
                ring1_step(step)

        with jax.named_scope("ring2"):
            for step in range(RING - 1):
                for block in range(BLOCKS):
                    for part in range(PARTS):
                        for direction in WAYS:
                            ring2_copy(part, direction, step, block).wait_recv()
                            place = lax.rem(second[part] + (RING - 2 - step if direction == 0 else 2 + step), RING)
                            share = ring2_share(part, direction, block, place)
                            value = share[...] + ring2[part, direction, step, block]
                            ring2_copy(part, direction, step, block).wait_send()
                            if step < RING - 2:
                                share[...] = value
                                ring2_copy(part, direction, step + 1, block).start()
                            else:
                                result[part, pl.ds(2 * low * block + direction * low, low)] = value * scale

        for slot in range(n_stage):
            hand_over(0, 0, 0, slot).wait_send()

    pl.run_scoped(
        sums, pltpu.VMEM((PARTS, CHUNKS, BLOCKS, bm, bn), jnp.float32),
        pltpu.VMEM((PARTS, 2, RING - 1, BLOCKS, bm // 2, bn), jnp.float32))

    main, piece_rows = gath.shape[5], result.shape[1]
    cut = main // 16 * 8

    def after(place, by):
        return lax.rem(place + by, RING)

    def at(part, owner, chunk, quarter=None):
        view = gath.at[core, part, owner, chunk]
        return view if quarter is None else view.at[quarter]

    def send(src, dst, sem, recv, axis, direction):
        return pltpu.make_async_remote_copy(
            src_ref=src, dst_ref=dst, send_sem=sem, recv_sem=recv, device_id=shifted(axis, direction), device_id_type=MESH)

    def quarter_copy(part, direction, leg):
        sem, recv = g_send.at[0, part], g1_recv.at[part, direction, leg]
        axis = (part + 2) % 3
        if leg == 0:
            src, dst = result.at[part, pl.ds(0, main)], at(part, coord[part], first[part], second[part])
            return send(src, dst, sem, recv, axis, direction)
        view = at(part, coord[part], first[part], after(second[part], 3 - 2 * direction))
        view = view.at[pl.ds(0, cut)] if direction == 0 else view.at[pl.ds(cut, main - cut)]
        return send(view, view, sem, recv, axis, direction)

    def chunk_copy(part, direction, leg):
        sem, recv = g_send.at[1, part], g2_recv.at[part, direction, leg]
        axis = (part + 1) % 3
        view = at(part, coord[part], first[part])
        if leg == 1:
            view = at(part, coord[part], after(first[part], 3 - 2 * direction)).at[pl.ds(2 * direction, 2)]
        return send(view, view, sem, recv, axis, direction)

    def owner_copy(part, direction, leg, order):
        sem, recv = g_send.at[2, part], g3_recv.at[part, direction, leg, order]
        chunk = after(first[part], (0, 3, 1, 2)[order])
        view = at(part, coord[part], chunk)
        if leg == 1:
            view = at(part, after(coord[part], 3 - 2 * direction), chunk).at[pl.ds(2 * direction, 2)]
        return send(view, view, sem, recv, part, direction)

    def cross(part, owner_by, order):
        view = at(part, after(coord[part], owner_by), after(first[part], (0, 3, 1, 2)[order]))
        return pltpu.make_async_remote_copy(
            src_ref=view, dst_ref=view, send_sem=cross_send, recv_sem=cross_recv, device_id=partner, device_id_type=MESH)

    def keep(part):
        return pltpu.make_async_copy(
            result.at[part, pl.ds(0, main)], at(part, coord[part], first[part], second[part]), local_sem.at[part])

    spare = pltpu.make_async_copy(result.at[:, pl.ds(main, piece_rows - main)], rest, local_sem.at[PARTS])
    with jax.named_scope("gather"):
        for part in range(PARTS):
            for direction in WAYS:
                quarter_copy(part, direction, 0).start()
            keep(part).start()
        spare.start()
        for part in range(PARTS):
            for direction in WAYS:
                quarter_copy(part, direction, 0).wait_recv()
                quarter_copy(part, direction, 1).start()
        for part in range(PARTS):
            keep(part).wait()
            for direction in WAYS:
                quarter_copy(part, direction, 1).wait_recv()
            for direction in WAYS:
                chunk_copy(part, direction, 0).start()
            for direction in WAYS:
                owner_copy(part, direction, 0, 0).start()
            cross(part, 0, 0).start()
        for part in range(PARTS):
            for direction in WAYS:
                chunk_copy(part, direction, 0).wait_recv()
                chunk_copy(part, direction, 1).start()
            for order in (1, 2):
                for direction in WAYS:
                    owner_copy(part, direction, 0, order).start()
                cross(part, 0, order).start()
        for part in range(PARTS):
            for direction in WAYS:
                chunk_copy(part, direction, 1).wait_recv()
            for direction in WAYS:
                owner_copy(part, direction, 0, 3).start()
            cross(part, 0, 3).start()
        for order in range(CHUNKS):
            for part in range(PARTS):
                for direction in WAYS:
                    owner_copy(part, direction, 0, order).wait_recv()
                    owner_copy(part, direction, 1, order).start()
                    cross(part, 3 - 2 * direction, order).start()
        for order in range(CHUNKS):
            for part in range(PARTS):
                for direction in WAYS:
                    owner_copy(part, direction, 1, order).wait_recv()
                cross(part, 2, order).start()

    for piece in range(PIECES):
        for part in range(PARTS):
            for direction in WAYS:
                near(piece, part, direction, 0).wait_send()
                hop(piece, part, direction, 0).wait_send()
                forward(piece, part, direction).wait_send()
    spare.wait()

    def drain(view, sem):
        pltpu.make_async_copy(view, view, sem).wait()

    for part in range(PARTS):
        drain(gath.at[core, part, 0, 0, pl.ds(0, 3)], g_send.at[0, part])
        drain(gath.at[core, part, 0, pl.ds(0, 3)], g_send.at[1, part])
        drain(gath.at[core, part, pl.ds(0, 3)], g_send.at[2, part])
    drain(gath.at[core], cross_send)
    drain(gath.at[1 - core], cross_recv)


def reduce_grads(x_loc, g_loc, weights, n_dev):
    rows, width = x_loc.shape
    bm = width // 6
    bn = 2 * bm
    dma = pltpu.SemaphoreType.DMA
    any_spec = pl.BlockSpec(memory_space=pl.ANY)
    f32, bf16 = jnp.float32, jnp.bfloat16
    n_stage = 4
    piece_rows = BLOCKS * (bm // 4)
    main = piece_rows * 7 // 64 * 8
    outs = pl.pallas_call(
        functools.partial(reduce_kernel, rows, bm, 1.0 / n_dev),
        name="reduce_grads",
        out_shape=[
            jax.ShapeDtypeStruct((2, PARTS, RING, CHUNKS, RING, main, bn), f32),
            jax.ShapeDtypeStruct((PARTS, piece_rows - main, bn), f32),
            jax.ShapeDtypeStruct((PARTS, 2, rows // 2, width), bf16),
            jax.ShapeDtypeStruct((2, PARTS, 2, rows // 2, 4 * bm), bf16),
            jax.ShapeDtypeStruct((4, rows, 24 * bm), bf16),
            jax.ShapeDtypeStruct((2, rows, width), bf16),
        ],
        in_specs=[any_spec] * 6,
        out_specs=[any_spec] * 6,
        scratch_shapes=[
            pltpu.VMEM((2 * PARTS, RING * rows, 4 * bm), bf16),
            pltpu.VMEM((PARTS, RING * rows, width), bf16),
            pltpu.VMEM((n_stage, bm, bn), f32),
            pltpu.VMEM((PARTS, 2, RING - 1, BLOCKS, bm // 8, bn), f32),
            pltpu.VMEM((PARTS, piece_rows, bn), f32),
            pltpu.SemaphoreType.REGULAR, dma((4,)), dma((2, LEAD + 1)), dma((4,)),
            dma((PIECES, PARTS)),
            dma((PIECES, PARTS, 2)), dma((PIECES, PARTS, 2)),
            dma((PIECES, PARTS, 2)), dma((PIECES, PARTS, 2)),
            dma((PIECES, PARTS, 2)), dma((PIECES, PARTS, 2)),
            dma((n_stage,)), dma((PARTS, CHUNKS, BLOCKS)),
            dma((PARTS, 2, BLOCKS)), dma((PARTS, 2, RING - 1, BLOCKS)),
            dma((PARTS, 2, BLOCKS)), dma((PARTS, 2, RING - 1, BLOCKS)),
            dma((PARTS + 1,)), dma((3, PARTS)),
            dma((PARTS, 2, 2)), dma((PARTS, 2, 2)), dma((PARTS, 2, 2, CHUNKS)),
            dma, dma,
        ],
        compiler_params=pltpu.CompilerParams(collective_id=0, has_side_effects=True, vmem_limit_bytes=67043328),
        cost_estimate=pl.CostEstimate(flops=40 * rows * 24 * bm * width, bytes_accessed=200_000_000, transcendentals=0),
    )(x_loc, g_loc, *weights)
    return outs[0], outs[1]


def place_kernel(n_turns, depth, load_view, spots, *refs):
    gathered, dsts = refs[0], refs[-7:-3]
    slots, in_sem, out_sem = refs[-3:]
    ahead = depth // 2

    def load(turn):
        slot = lax.rem(turn, depth)
        return pltpu.make_async_copy(load_view(gathered, turn), slots.at[slot], in_sem.at[slot])

    def drain(turn):
        slot = lax.rem(turn, depth)
        return pltpu.make_async_copy(slots.at[slot], load_view(gathered, 0), out_sem.at[slot])

    def store(turn):
        slot = lax.rem(turn, depth)
        for owner, moves in spots(turn):
            for which in range(4):
                @pl.when(owner == which)
                def _():
                    for view, rows, cols in moves(which):
                        pltpu.make_async_copy(view(slots.at[slot]), dsts[which].at[rows, cols], out_sem.at[slot]).start()

    def prime(turn, carry):
        load(turn).start()
        return carry

    def body(turn, carry):
        @pl.when(turn + ahead < n_turns)
        def _():
            @pl.when(turn + ahead >= depth)
            def _():
                drain(turn + ahead - depth).wait()

            load(turn + ahead).start()

        load(turn).wait()
        store(turn)
        return carry

    def finish(turn, carry):
        drain(turn).wait()
        return carry

    lax.fori_loop(0, ahead, prime, 0)
    lax.fori_loop(0, n_turns, body, 0)
    lax.fori_loop(n_turns - depth, n_turns, finish, 0)


def spot(bm, which, part, core, chunk, quarter, block, row, n):
    bn = 2 * bm
    if which % 2 == 1:
        start = (8 * part + 4 * core + chunk) * bm
        col = block * bn
    else:
        index = 3 * chunk + block
        start = lax.div(index, 2) * bm
        col = (4 * part + 2 * core + lax.rem(index, 2)) * bn
    start = start + quarter * (bm // 4) + row
    return pl.ds(pl.multiple_of(start, 8), n), pl.ds(pl.multiple_of(col, bn), bn)


def ranges(bm, begin, end):
    quarter = bm // 4
    for block in range(BLOCKS):
        low, high = max(begin, block * quarter), min(end, (block + 1) * quarter)
        if low < high:
            yield low, block, low - block * quarter, high - low


def place_main(gathered, shapes):
    main, bn = gathered.shape[5:]
    bm = bn // 2
    depth = 12

    def unpack(turn):
        chunk = lax.rem(turn, CHUNKS)
        owner = lax.rem(lax.div(turn, CHUNKS), RING)
        part = lax.rem(lax.div(turn, CHUNKS * RING), PARTS)
        return lax.div(turn, CHUNKS * RING * PARTS), part, owner, chunk

    def load_view(ref, turn):
        return ref.at[unpack(turn)]

    def spots(turn):
        core, part, owner, chunk = unpack(turn)

        def moves(which):
            for quarter in range(RING):
                for begin, block, row, n in ranges(bm, 0, main):
                    yield (lambda ref, q=quarter, b=begin, n=n: ref.at[q, pl.ds(b, n)], *spot(bm, which, part, core, chunk, quarter, block, row, n))

        return [(owner, moves)]

    return place(gathered, shapes, 2 * PARTS * RING * CHUNKS, depth, load_view, spots, (RING, main, bn))


def place_rest(gathered, mesh_shape, shapes, earlier):
    n_dev, _, n_rows, bn = gathered.shape
    bm = bn // 2
    n_z, n_y, n_xc = mesh_shape
    begin_row = BLOCKS * (bm // 4) - n_rows
    group = 8
    depth = 8

    def load_view(ref, turn):
        return ref.at[pl.ds(turn * group, group)]

    def spots(turn):
        found = []
        for k in range(group):
            dev = turn * group + k
            xc, y, z = lax.rem(dev, n_xc), lax.rem(lax.div(dev, n_xc), n_y), lax.div(dev, n_xc * n_y)
            x, core = lax.div(xc, 2), lax.rem(xc, 2)
            for part in range(PARTS):
                owner, chunk, quarter = ((x, y, z), (y, z, x), (z, x, y))[part]

                def moves(which, k=k, part=part, core=core, chunk=chunk, quarter=quarter):
                    for begin, block, row, n in ranges(bm, begin_row, begin_row + n_rows):
                        yield (lambda ref, b=begin - begin_row, n=n: ref.at[k, part, pl.ds(b, n)], *spot(bm, which, part, core, chunk, quarter, block, row, n))

                found.append((owner, moves))
        return found

    return place(gathered, shapes, n_dev // group, depth, load_view, spots, (group, PARTS, n_rows, bn), earlier)


def place(gathered, shapes, n_turns, depth, load_view, spots, slot_shape, earlier=()):
    return pl.pallas_call(
        functools.partial(place_kernel, n_turns, depth, load_view, spots),
        name="place_grads",
        out_shape=[jax.ShapeDtypeStruct(s, jnp.float32) for s in shapes],
        in_specs=[pl.BlockSpec(memory_space=pl.ANY)] * (1 + len(earlier)),
        out_specs=[pl.BlockSpec(memory_space=pl.ANY)] * 4,
        scratch_shapes=[pltpu.VMEM((depth, *slot_shape), jnp.float32), pltpu.SemaphoreType.DMA((depth,)), pltpu.SemaphoreType.DMA((depth,))],
        input_output_aliases={1 + k: k for k in range(len(earlier))},
        cost_estimate=pl.CostEstimate(flops=8 * gathered.size, bytes_accessed=8 * gathered.size, transcendentals=0),
    )(gathered, *earlier)


def solution(mesh):
    n_dev = math.prod(mesh.shape.values())
    axes = ("z", "y", "xc")
    batch_spec = P(axes, None)
    whole_spec = P(None, None)

    def device_step(x_loc, g_loc, w_one, w_two, w_three, w_four):
        main, rest = reduce_grads(x_loc, g_loc, (w_one, w_two, w_three, w_four), n_dev)
        all_rest = lax.all_gather(rest, axes, axis=0)
        shapes = (w_one.shape, w_two.shape, w_three.shape, w_four.shape)
        mesh_shape = tuple(mesh.shape[name] for name in axes)
        return tuple(place_rest(all_rest, mesh_shape, shapes, place_main(main, shapes)))

    return jax.shard_map(
        device_step,
        mesh=mesh,
        in_specs=(batch_spec, batch_spec, whole_spec, whole_spec, whole_spec, whole_spec),
        out_specs=(whole_spec, whole_spec, whole_spec, whole_spec),
        check_vma=False,
    )
```

```python
import functools
import math
import jax
import jax.numpy as jnp
from jax import lax
from jax.experimental import pallas as pl
from jax.experimental.pallas import tpu as pltpu
from jax.sharding import PartitionSpec as P

GELU_SCALE = math.sqrt(2.0 / math.pi)
GELU_CUBIC = 0.044715
MESH = pl.DeviceIdType.MESH
RING = 4
PARTS = 3
CHUNKS = 4
BLOCKS = 3
LEAD = 3
LAG = 12
ORDER = (0, 3, 1, 2)
WAYS = (0, 1)
PIECES = 3


def gelu_parts(pre_act):
    tanh_val = jnp.tanh(GELU_SCALE * (pre_act + GELU_CUBIC * pre_act * pre_act * pre_act))
    value = 0.5 * pre_act * (1.0 + tanh_val)
    return value, 0.5 * (1.0 + tanh_val) + 0.5 * pre_act * (1.0 - tanh_val * tanh_val) * GELU_SCALE * (1.0 + 3.0 * GELU_CUBIC * pre_act * pre_act)


def split(index, n):
    return lax.rem(index, n), lax.div(index, n)


def pick(index, values):
    chosen = values[-1]
    for k in range(len(values) - 2, -1, -1):
        chosen = jnp.where(index == k, values[k], chosen)
    return chosen


def reduce_kernel(rows, bm, scale, *refs):
    bn = 2 * bm
    n_pass = 2 * PARTS
    x_in, g_in, w_one, w_two, w_three, w_four, gath, relay_wid, relay_hid, hid_out, wid_out, *refs = refs
    passing, refs = refs[:n_pass], refs[n_pass:]
    hid = tuple(hid_out.at[which] for which in range(RING))
    wid = (x_in, wid_out.at[0], wid_out.at[1], g_in)
    (hid_v, wid_v, stage, ring2, result, free_sem, act_sem, weight_sem, tile_sem, own_sem,
     near_send, near_recv, hop_send, hop_recv, fwd_send, fwd_recv, stage_send, stage_recv, r1_send, r1_recv, r2_send, r2_recv,
     local_sem, pass_in, pass_out, g_send, g1_recv, g2_recv, g3_recv, cross_send, cross_recv) = refs
    n_stage = stage.shape[0]
    half_rows = rows // 2

    z, y, xc = lax.axis_index("z"), lax.axis_index("y"), lax.axis_index("xc")
    x, core = lax.div(xc, 2), lax.rem(xc, 2)
    coord = (x, y, z)
    first, second = (y, z, x), (z, x, y)
    partner = (z, y, x * 2 + (1 - core))

    def shifted(axis, direction):
        to = lax.rem(coord[axis] + (1 if direction == 0 else RING - 1), RING)
        return ((z, y, to * 2 + core), (z, to, xc), (to, y, xc))[axis]

    def tell_neighbours(sem):
        for axis in range(3):
            for direction in WAYS:
                pl.semaphore_signal(sem, inc=1, device_id=shifted(axis, direction), device_id_type=MESH)
        pl.semaphore_signal(sem, inc=1, device_id=partner, device_id_type=MESH)

    barrier = pltpu.get_barrier_semaphore()
    tell_neighbours(barrier)

    def source(piece, part, which, row, n):
        if piece == 0:
            return wid[which].at[pl.ds(row, n)]
        side = 1 - core if piece == 1 else core
        return hid[which].at[pl.ds(row, n), pl.ds(pl.multiple_of((8 * part + 4 * side) * bm, 4 * bm), 4 * bm)]

    def landing(piece, part, slot, row, n):
        if piece == 0:
            return wid_v.at[part, pl.ds(slot * rows + row, n)]
        return hid_v.at[(piece - 1) * PARTS + part, pl.ds(slot * rows + row, n)]

    def relay(piece, part, direction):
        if piece == 0:
            return relay_wid.at[part, direction]
        return relay_hid.at[piece - 1, part, direction]

    def own(piece, part, which=0):
        return pltpu.make_async_copy(source(piece, part, which, 0, rows), landing(piece, part, 0, 0, rows), own_sem.at[piece, part])

    def near(piece, part, direction, which=0):
        return pltpu.make_async_remote_copy(
            src_ref=source(piece, part, which, 0, rows), dst_ref=landing(piece, part, 1 + 2 * direction, 0, rows),
            send_sem=near_send.at[piece, part, direction], recv_sem=near_recv.at[piece, part, direction],
            device_id=shifted(part, direction), device_id_type=MESH)

    def hop(piece, part, direction, which=0):
        return pltpu.make_async_remote_copy(
            src_ref=source(piece, part, which, direction * half_rows, half_rows), dst_ref=relay(piece, part, direction),
            send_sem=hop_send.at[piece, part, direction], recv_sem=hop_recv.at[piece, part, direction],
            device_id=shifted(part, direction), device_id_type=MESH)

    def forward(piece, part, direction):
        return pltpu.make_async_remote_copy(
            src_ref=relay(piece, part, direction), dst_ref=landing(piece, part, 2, direction * half_rows, half_rows),
            send_sem=fwd_send.at[piece, part, direction], recv_sem=fwd_recv.at[piece, part, direction],
            device_id=shifted(part, direction), device_id_type=MESH)

    def beyond(part, direction):
        return lax.rem(coord[part] + (1 if direction == 0 else RING - 1), RING)

    def round_by(direction, steps):
        return RING - steps if direction == 0 else steps

    def start_for(copy, owner, ready):
        for which in ready:
            @pl.when(owner == which)
            def _():
                copy(which).start()

    def start_hops(piece, ready):
        for part in range(PARTS):
            for direction in WAYS:
                start_for(functools.partial(hop, piece, part, direction), lax.rem(coord[part] + 2, RING), ready)

    def start_nears(piece, ready):
        for part in range(PARTS):
            for direction in WAYS:
                start_for(functools.partial(near, piece, part, direction), beyond(part, direction), ready)

    def start_own(piece):
        for part in range(PARTS):
            start_for(functools.partial(own, piece, part), coord[part], (0, 1, 2, 3))

    def pass_on(piece, ready=None):
        for part in range(PARTS):
            for direction in WAYS:
                def relay_one():
                    hop(piece, part, direction).wait_recv()
                    forward(piece, part, direction).start()

                if ready is None:
                    relay_one()
                    continue
                owner = beyond(part, direction)
                for which in ready:
                    pl.when(owner == which)(relay_one)

    def arrived(piece, part):
        own(piece, part).wait()
        for direction in WAYS:
            near(piece, part, direction).wait_recv()
            forward(piece, part, direction).wait_recv()

    tiles, lead = 12, weight_sem.shape[1] - 1

    def hidden(turn):
        side = jnp.where(turn < tiles // 2, 1 - core, core)
        rest = lax.rem(turn, tiles // 2)
        tile = 4 * lax.div(rest, 2) + 2 * side + lax.rem(rest, 2)
        return pl.ds(pl.multiple_of(tile * bn, bn), bn)

    def rounded(value):
        return value.astype(jnp.bfloat16)

    def widened(value):
        return value.astype(jnp.float32)

    def mm(left, right, transposed=False):
        return lax.dot_general(left, right, (((1,), (1 if transposed else 0,)), ((), ())), preferred_element_type=jnp.float32)

    def products(columns_v, rows_v, acts, out_tiles, total, a_one):
        def weight_copy(kind, weight, tile):
            slot = lax.rem(tile, lead + 1)
            if kind == 0:
                return pltpu.make_async_copy(weight.at[:, hidden(tile)], columns_v.at[slot], weight_sem.at[kind, slot])
            return pltpu.make_async_copy(weight.at[hidden(tile)], rows_v.at[slot], weight_sem.at[kind, slot])

        def tile_copy(index, ref, tile):
            return pltpu.make_async_copy(out_tiles.at[index], ref.at[:, hidden(tile)], tile_sem.at[index])

        def close_total(base, index, ref, sem):
            acts[index] = rounded(total[...] + widened(acts[base]))
            copy = pltpu.make_async_copy(acts.at[index], ref, act_sem.at[sem])
            copy.start()
            copy.wait()

        def sweep(weights, following, step, outs, midway):
            def turn(tile, carry):
                for kind, weight in weights:
                    @pl.when(tile < tiles - lead)
                    def _():
                        weight_copy(kind, weight, tile + lead).start()

                for kind, weight in following:
                    @pl.when(tile >= tiles - lead)
                    def _():
                        weight_copy(kind, weight, tile + lead - tiles).start()

                for kind, weight in weights:
                    weight_copy(kind, weight, tile).wait()
                slot = lax.rem(tile, 2)

                @pl.when(tile >= 2)
                def _():
                    for k, ref in enumerate(outs):
                        tile_copy(2 * k + slot, ref, tile).wait()

                step(tile, slot, lax.rem(tile, lead + 1))
                for k, ref in enumerate(outs):
                    tile_copy(2 * k + slot, ref, tile).start()
                return carry

            most = 2 * tiles // 3
            lax.fori_loop(0, most, turn, 0)
            midway()
            lax.fori_loop(most, tiles, turn, 0)
            for slot in WAYS:
                for k, ref in enumerate(outs):
                    tile_copy(2 * k + slot, ref, slot).wait()

        for tile in range(lead):
            weight_copy(0, w_one, tile).start()
            weight_copy(1, w_two, tile).start()
        loads = [pltpu.make_async_copy(ref, acts.at[k], act_sem.at[k]) for k, ref in enumerate((x_in, g_in))]
        for copy in loads:
            copy.start()
        total[...] = jnp.zeros(total.shape, jnp.float32)
        pl.semaphore_wait(barrier, 7)
        start_hops(0, (0, 3))
        start_nears(0, (0, 3))
        for copy in loads:
            copy.wait()

        def first_forward(tile, slot, load):
            pre = rounded(mm(acts[0], columns_v[load]))
            a_one[tile] = pre
            act = rounded(gelu_parts(widened(pre))[0])
            out_tiles[slot] = act
            total[...] = total[...] + mm(act, rows_v[load])

        def midway_one():
            start_hops(1, (1,))
            start_nears(1, (1,))

        with jax.named_scope("first_forward"):
            sweep(((0, w_one), (1, w_two)), ((0, w_three), (1, w_four)), first_forward, (hid[1],), midway_one)
            start_hops(2, (1,))
            close_total(0, 2, wid[2], 2)
        total[...] = jnp.zeros(total.shape, jnp.float32)
        start_hops(0, (2,))
        start_nears(0, (2,))
        start_nears(2, (1,))
        pass_on(0, (0, 3))

        def second_block(tile, slot, load):
            pre = widened(rounded(mm(acts[2], columns_v[load])))
            back = mm(acts[1], rows_v[load], True)
            act, slope = gelu_parts(pre)
            out_tiles[slot] = rounded(act)
            grad = rounded(back * slope)
            out_tiles[2 + slot] = grad
            total[...] = total[...] + mm(grad, columns_v[load], True)

        def midway_two():
            start_hops(1, (2, 3))
            start_nears(1, (2, 3))

        with jax.named_scope("second_block"):
            sweep(((0, w_three), (1, w_four)), ((1, w_two),), second_block, (hid[3], hid[2]), midway_two)
            start_hops(2, (2, 3))
            close_total(1, 0, wid[1], 3)
        start_hops(0, (1,))
        start_nears(0, (1,))
        start_nears(2, (2, 3))

        def first_backward(tile, slot, load):
            back = mm(acts[0], rows_v[load], True)
            out_tiles[slot] = rounded(back * gelu_parts(widened(a_one[tile]))[1])

        def midway_three():
            start_hops(1, (0,))
            start_nears(1, (0,))
            pass_on(1, (1,))
            pass_on(2, (1,))
            pass_on(0, (2,))

        with jax.named_scope("first_backward"):
            sweep(((1, w_two),), (), first_backward, (hid[0],), midway_three)
        start_hops(2, (0,))
        start_nears(2, (0,))

    width = wid_v.shape[-1]
    pl.run_scoped(
        products, pltpu.VMEM((lead + 1, width, bn), jnp.bfloat16), pltpu.VMEM((lead + 1, bn, width), jnp.bfloat16),
        pltpu.VMEM((3, rows, width), jnp.bfloat16), pltpu.VMEM((4, rows, bn), jnp.bfloat16), pltpu.VMEM((rows, width), jnp.float32),
        pltpu.VMEM((tiles, rows, bn), jnp.bfloat16))

    def sums(acc, ring1):
        def product(side, part, chunk, block, store):
            odd = lax.rem(pick(part, coord), 2)
            dims = (((0,), (0,)), ((), ()))

            @pl.when(odd == 1)
            def _():
                left = hid_v[side * PARTS + part, :, pl.ds(pl.multiple_of(chunk * bm, bm), bm)]
                right = wid_v[part, :, pl.ds(pl.multiple_of(block * bn, bn), bn)]
                store(lax.dot_general(left, right, dims, preferred_element_type=jnp.float32))

            @pl.when(odd == 0)
            def _():
                index = 3 * chunk + block
                left = wid_v[part, :, pl.ds(pl.multiple_of(lax.div(index, 2) * bm, bm), bm)]
                right = hid_v[side * PARTS + part, :, pl.ds(pl.multiple_of(lax.rem(index, 2) * bn, bn), bn)]
                store(lax.dot_general(left, right, dims, preferred_element_type=jnp.float32))

        def hand_over(part=0, chunk=0, block=0, slot=0):
            return pltpu.make_async_remote_copy(
                src_ref=stage.at[slot], dst_ref=acc.at[part, chunk, block], send_sem=stage_send.at[slot],
                recv_sem=stage_recv.at[part, chunk, block], device_id=partner, device_id_type=MESH)

        tell_neighbours(free_sem)
        with jax.named_scope("send_last"):
            pass_on(0, (1,))
            pass_on(1, (2, 3))
            pass_on(2, (2, 3))
            pass_on(1, (0,))
            for piece in range(PIECES):
                start_own(piece)
        with jax.named_scope("await_other"):
            pl.semaphore_wait(free_sem, 7)
            for piece in range(PIECES - 1):
                for part in range(PARTS):
                    arrived(piece, part)

        top, low = bm // 2, bm // 8

        def ring1_copy(part, direction, step, block):
            chunk = lax.rem(first[part] + round_by(direction, 1 + step), RING)
            return pltpu.make_async_remote_copy(
                src_ref=acc.at[part, chunk, block, pl.ds(direction * top, top)], dst_ref=ring1.at[part, direction, step, block],
                send_sem=r1_send.at[part, direction, block], recv_sem=r1_recv.at[part, direction, step, block],
                device_id=shifted((part + 1) % 3, direction), device_id_type=MESH)

        def place_of(count):
            order, rest = lax.div(count, PARTS * BLOCKS), lax.rem(count, PARTS * BLOCKS)
            part, block = lax.rem(rest, PARTS), lax.div(rest, PARTS)
            return order, part, lax.rem(pick(part, first) + pick(order, (3, 1, 2, 0)), RING), block

        blocks = CHUNKS * PARTS * BLOCKS

        def both_halves(count, carry):
            @pl.when(count < blocks)
            def _():
                _, part, chunk, block = place_of(count)
                slot = lax.rem(count, n_stage)

                @pl.when(count >= n_stage)
                def _():
                    hand_over(slot=slot).wait_send()

                def store(value):
                    stage[slot] = value

                product(0, part, chunk, block, store)
                hand_over(part, chunk, block, slot).start()

            @pl.when(count >= LAG)
            def _():
                order, part, chunk, block = place_of(count - LAG)
                hand_over(part, chunk, block).wait_recv()

                def store(value):
                    acc[part, chunk, block] = acc[part, chunk, block] + value

                product(1, part, chunk, block, store)
                for direction in WAYS:
                    for which in range(PARTS):
                        @pl.when((order == direction) & (part == which))
                        def _():
                            ring1_copy(which, direction, 0, block).start()

            return carry

        def ring1_step(step):
            for block in range(BLOCKS):
                for part in range(PARTS):
                    for direction in WAYS:
                        ring1_copy(part, direction, step, block).wait_recv()
                        chunk = lax.rem(first[part] + round_by(direction, 2 + step), RING)
                        share = acc.at[part, chunk, block, pl.ds(direction * top, top)]
                        share[...] = share[...] + ring1[part, direction, step, block]
                        ring1_copy(part, direction, step, block).wait_send()
                        if step < RING - 2:
                            ring1_copy(part, direction, step + 1, block).start()
                    if step == RING - 2:
                        for direction in WAYS:
                            ring2_copy(part, direction, 0, block).start()

        with jax.named_scope("other_half"):
            lax.fori_loop(0, LAG, both_halves, 0)
        with jax.named_scope("await_own"):
            pass_on(2, (0,))
            for part in range(PARTS):
                arrived(2, part)
        last = blocks - PARTS * BLOCKS
        with jax.named_scope("halves"):
            lax.fori_loop(LAG, last + LAG, both_halves, 0)
        def ring2_share(part, direction, block, place):
            row = pl.multiple_of(2 * low * place + direction * low, low)
            return acc.at[part, first[part], block, pl.ds(row, low)]

        def ring2_copy(part, direction, step, block):
            place = lax.rem(second[part] + round_by(direction, 1 + step), RING)
            return pltpu.make_async_remote_copy(
                src_ref=ring2_share(part, direction, block, place), dst_ref=ring2.at[part, direction, step, block],
                send_sem=r2_send.at[part, direction, block], recv_sem=r2_recv.at[part, direction, step, block],
                device_id=shifted((part + 2) % 3, direction), device_id_type=MESH)

        with jax.named_scope("ring1#step=0"):
            ring1_step(0)
        with jax.named_scope("last_chunk"):
            lax.fori_loop(last + LAG, blocks + LAG, both_halves, 0)
        for step in range(1, RING - 1):
            with jax.named_scope(f"ring1#step={step}"):
                ring1_step(step)

        with jax.named_scope("ring2"):
            for step in range(RING - 1):
                for block in range(BLOCKS):
                    for part in range(PARTS):
                        for direction in WAYS:
                            ring2_copy(part, direction, step, block).wait_recv()
                            place = lax.rem(second[part] + round_by(direction, 2 + step), RING)
                            share = ring2_share(part, direction, block, place)
                            value = share[...] + ring2[part, direction, step, block]
                            ring2_copy(part, direction, step, block).wait_send()
                            if step < RING - 2:
                                share[...] = value
                                ring2_copy(part, direction, step + 1, block).start()
                            else:
                                result[part, pl.ds(2 * low * block + direction * low, low)] = value * scale

        for slot in range(n_stage):
            hand_over(slot=slot).wait_send()

    pl.run_scoped(
        sums, pltpu.VMEM((PARTS, CHUNKS, BLOCKS, bm, bn), jnp.float32),
        pltpu.VMEM((PARTS, 2, RING - 1, BLOCKS, bm // 2, bn), jnp.float32))

    piece_rows = result.shape[1]
    cut = piece_rows // 16 * 8

    def after(place, by):
        return lax.rem(place + by, RING)

    def at(part, owner, chunk, quarter=None):
        view = gath.at[core, part, owner, chunk]
        return view if quarter is None else view.at[quarter]

    def send(src, dst, sem, recv, axis, direction):
        return pltpu.make_async_remote_copy(
            src_ref=src, dst_ref=dst, send_sem=sem, recv_sem=recv, device_id=shifted(axis, direction), device_id_type=MESH)

    def quarter_copy(part, direction, leg):
        sem, recv = g_send.at[0, part], g1_recv.at[part, direction, leg]
        axis = (part + 2) % 3
        if leg == 0:
            src, dst = result.at[part], at(part, coord[part], first[part], second[part])
            return send(src, dst, sem, recv, axis, direction)
        view = at(part, coord[part], first[part], after(second[part], 3 - 2 * direction))
        view = view.at[pl.ds(0, cut)] if direction == 0 else view.at[pl.ds(cut, piece_rows - cut)]
        return send(view, view, sem, recv, axis, direction)

    def chunk_copy(part, direction, leg):
        sem, recv = g_send.at[1, part], g2_recv.at[part, direction, leg]
        axis = (part + 1) % 3
        view = at(part, coord[part], first[part])
        if leg == 1:
            view = at(part, coord[part], after(first[part], 3 - 2 * direction)).at[pl.ds(2 * direction, 2)]
        return send(view, view, sem, recv, axis, direction)

    def owner_copy(part, direction, leg, order):
        sem, recv = g_send.at[2 + leg, part], g3_recv.at[part, direction, leg, order]
        chunk = after(first[part], ORDER[order])
        view = at(part, coord[part], chunk)
        if leg == 1:
            view = at(part, beyond(part, 1 - direction), chunk, 2 * direction)
        return send(view, view, sem, recv, part, direction)

    def cross(part, owner_by, order, quarter=None):
        view = at(part, after(coord[part], owner_by), after(first[part], ORDER[order]), quarter)
        kind = 0 if quarter is None else 1
        return pltpu.make_async_remote_copy(
            src_ref=view, dst_ref=view, send_sem=cross_send.at[kind], recv_sem=cross_recv.at[kind], device_id=partner, device_id_type=MESH)

    def keep(part):
        return pltpu.make_async_copy(result.at[part], at(part, coord[part], first[part], second[part]), local_sem.at[part])

    turns = [(order, part, direction) for order in range(CHUNKS) for part in range(PARTS) for direction in WAYS]

    def passing_in(turn):
        order, part, direction = turns[turn]
        view = at(part, beyond(part, 1 - direction), after(first[part], ORDER[order]), 1 + 2 * direction)
        slot = turn % n_stage
        return pltpu.make_async_copy(view, stage.at[slot, pl.ds(0, piece_rows)], pass_in.at[slot])

    def passing_out(turn):
        order, part, direction = turns[turn]
        slot = turn % n_stage
        return pltpu.make_async_copy(
            stage.at[slot, pl.ds(0, piece_rows)], passing[direction * PARTS + part].at[after(first[part], ORDER[order])], pass_out.at[slot])

    with jax.named_scope("gather"):
        for part in range(PARTS):
            for direction in WAYS:
                quarter_copy(part, direction, 0).start()
            keep(part).start()
        for part in range(PARTS):
            for direction in WAYS:
                quarter_copy(part, direction, 0).wait_recv()
                quarter_copy(part, direction, 1).start()
        for part in range(PARTS):
            keep(part).wait()
            for direction in WAYS:
                quarter_copy(part, direction, 1).wait_recv()
            for direction in WAYS:
                chunk_copy(part, direction, 0).start()
            for direction in WAYS:
                owner_copy(part, direction, 0, 0).start()
            cross(part, 0, 0).start()
        for part in range(PARTS):
            for direction in WAYS:
                chunk_copy(part, direction, 0).wait_recv()
                chunk_copy(part, direction, 1).start()
            for order in (1, 2):
                for direction in WAYS:
                    owner_copy(part, direction, 0, order).start()
                cross(part, 0, order).start()
        for part in range(PARTS):
            for direction in WAYS:
                chunk_copy(part, direction, 1).wait_recv()
            for direction in WAYS:
                owner_copy(part, direction, 0, 3).start()
            cross(part, 0, 3).start()
        for turn, (order, part, direction) in enumerate(turns):
            owner_copy(part, direction, 0, order).wait_recv()
            owner_copy(part, direction, 1, order).start()
            cross(part, 3 - 2 * direction, order).start()
            if turn >= n_stage:
                passing_out(turn - n_stage).wait()
            passing_in(turn).start()
            if turn > 0:
                passing_in(turn - 1).wait()
                passing_out(turn - 1).start()
        passing_in(len(turns) - 1).wait()
        passing_out(len(turns) - 1).start()
        for turn in range(len(turns) - n_stage, len(turns)):
            passing_out(turn).wait()
        for order, part, direction in turns:
            owner_copy(part, direction, 1, order).wait_recv()
            cross(part, 2, order, 2 * direction).start()

    for piece in range(PIECES):
        for part in range(PARTS):
            for direction in WAYS:
                near(piece, part, direction).wait_send()
                hop(piece, part, direction).wait_send()
                forward(piece, part, direction).wait_send()

    def drain(view, sem):
        pltpu.make_async_copy(view, view, sem).wait()

    for part in range(PARTS):
        drain(gath.at[core, part, 0, 0, pl.ds(0, 3)], g_send.at[0, part])
        drain(gath.at[core, part, 0, pl.ds(0, 3)], g_send.at[1, part])
        drain(gath.at[core, part, pl.ds(0, 2)], g_send.at[2, part])
        drain(gath.at[core, part, 0, :, pl.ds(0, 2)], g_send.at[3, part])
    for who, sem in ((core, cross_send), (1 - core, cross_recv)):
        drain(gath.at[who, :, pl.ds(0, 3)], sem.at[0])
        drain(gath.at[who, :, 0, :, pl.ds(0, 2)], sem.at[1])


def reduce_grads(x_loc, g_loc, weights, n_dev):
    rows, width = x_loc.shape
    bm = width // 6
    bn = 2 * bm
    dma = pltpu.SemaphoreType.DMA
    any_spec = pl.BlockSpec(memory_space=pl.ANY)
    f32, bf16 = jnp.float32, jnp.bfloat16
    n_stage = 4
    piece_rows = BLOCKS * (bm // 4)
    outs = pl.pallas_call(
        functools.partial(reduce_kernel, rows, bm, 1.0 / n_dev),
        name="reduce_grads",
        out_shape=[
            jax.ShapeDtypeStruct((2, PARTS, RING, CHUNKS, RING, piece_rows, bn), f32),
            jax.ShapeDtypeStruct((PARTS, 2, rows // 2, width), bf16),
            jax.ShapeDtypeStruct((2, PARTS, 2, rows // 2, 4 * bm), bf16),
            jax.ShapeDtypeStruct((4, rows, 24 * bm), bf16),
            jax.ShapeDtypeStruct((2, rows, width), bf16),
            *[jax.ShapeDtypeStruct((CHUNKS, piece_rows, bn), f32)] * (2 * PARTS),
        ],
        in_specs=[any_spec] * 6,
        out_specs=[any_spec] * (5 + 2 * PARTS),
        scratch_shapes=[
            pltpu.VMEM((2 * PARTS, RING * rows, 4 * bm), bf16),
            pltpu.VMEM((PARTS, RING * rows, width), bf16),
            pltpu.VMEM((n_stage, bm, bn), f32),
            pltpu.VMEM((PARTS, 2, RING - 1, BLOCKS, bm // 8, bn), f32),
            pltpu.VMEM((PARTS, piece_rows, bn), f32),
            pltpu.SemaphoreType.REGULAR, dma((4,)), dma((2, LEAD + 1)), dma((4,)),
            dma((PIECES, PARTS)),
            *[dma((PIECES, PARTS, 2))] * 6,
            dma((n_stage,)), dma((PARTS, CHUNKS, BLOCKS)),
            dma((PARTS, 2, BLOCKS)), dma((PARTS, 2, RING - 1, BLOCKS)),
            dma((PARTS, 2, BLOCKS)), dma((PARTS, 2, RING - 1, BLOCKS)),
            dma((PARTS,)), dma((n_stage,)), dma((n_stage,)), dma((4, PARTS)),
            dma((PARTS, 2, 2)), dma((PARTS, 2, 2)), dma((PARTS, 2, 2, CHUNKS)),
            dma((2,)), dma((2,)),
        ],
        compiler_params=pltpu.CompilerParams(collective_id=0, has_side_effects=True, vmem_limit_bytes=67043328),
        cost_estimate=pl.CostEstimate(flops=40 * rows * 24 * bm * width, bytes_accessed=200_000_000, transcendentals=0),
    )(x_loc, g_loc, *weights)
    return outs[0], outs[5:]


def place_kernel(begin, end, depth, start_load, like, spots, n_src, *refs):
    srcs, dsts = refs[:n_src], refs[-7:-3]
    slots, in_sem, out_sem = refs[-3:]
    ahead = depth // 2

    def load(turn):
        slot = lax.rem(turn, depth)
        start_load(srcs, turn, slots.at[slot], in_sem.at[slot])

    def settle(turn, sem):
        slot = lax.rem(turn, depth)
        pltpu.make_async_copy(like(srcs), slots.at[slot], sem.at[slot]).wait()

    def store(turn):
        slot = lax.rem(turn, depth)
        owner, part, core, pieces = spots(turn)
        bn = slots.shape[-1]
        quarter_rows = bn // 8
        for which in range(RING):
            @pl.when(owner == which)
            def _():
                for k, (chunk, quarter) in enumerate(pieces):
                    for block in range(BLOCKS):
                        rows, cols = spot(bn // 2, which, part, core, chunk, quarter, block)
                        pltpu.make_async_copy(
                            slots.at[slot, k, pl.ds(block * quarter_rows, quarter_rows)], dsts[which].at[rows, cols], out_sem.at[slot]).start()

    def prime(turn, carry):
        load(turn)
        return carry

    def body(turn, carry):
        @pl.when(turn + ahead < end)
        def _():
            @pl.when(turn + ahead >= begin + depth)
            def _():
                settle(turn + ahead - depth, out_sem)

            load(turn + ahead)

        settle(turn, in_sem)
        store(turn)
        return carry

    def finish(turn, carry):
        settle(turn, out_sem)
        return carry

    lax.fori_loop(begin, begin + ahead, prime, 0)
    lax.fori_loop(begin, end, body, 0)
    lax.fori_loop(end - depth, end, finish, 0)


def spot(bm, which, part, core, chunk, quarter, block):
    bn = 2 * bm
    if which % 2:
        start = (8 * part + 4 * core + chunk) * bm
        col = block * bn
    else:
        index = 3 * chunk + block
        start = lax.div(index, 2) * bm
        col = (4 * part + 2 * core + lax.rem(index, 2)) * bn
    rows = bm // 4
    return pl.ds(pl.multiple_of(start + quarter * rows, rows), rows), pl.ds(pl.multiple_of(col, bn), bn)


def where_am_i():
    z, y, xc = lax.axis_index("z"), lax.axis_index("y"), lax.axis_index("xc")
    return (lax.div(xc, 2), y, z), lax.rem(xc, 2)


def place_kept(gathered, shapes, begin, end, earlier=()):
    whole = 2 * PARTS * 3 * CHUNKS * 2

    def unpack(turn):
        coords, _ = where_am_i()
        half, rest = split(turn, 2)
        chunk, rest = split(rest, CHUNKS)
        by, rest = split(rest, 3)
        part, core = split(rest, PARTS)
        far = turn - whole
        chunk = jnp.where(far < 0, chunk, lax.rem(far, CHUNKS))
        part = jnp.where(far < 0, part, lax.rem(lax.div(far, CHUNKS), PARTS))
        core = jnp.where(far < 0, core, lax.div(far, CHUNKS * PARTS))
        owner = lax.rem(pick(part, coords) + jnp.where(far < 0, by + jnp.where(by == 2, 1, 0), 2), RING)
        return far, core, part, owner, chunk, half

    def start_load(srcs, turn, slot, sem):
        far, core, part, owner, chunk, half = unpack(turn)
        chunk_view = srcs[0].at[core, part, owner, chunk]

        @pl.when(far < 0)
        def _():
            pltpu.make_async_copy(chunk_view.at[pl.ds(2 * half, 2)], slot, sem).start()

        @pl.when(far >= 0)
        def _():
            for k in WAYS:
                pltpu.make_async_copy(chunk_view.at[2 * k], slot.at[k], sem).start()

    def spots(turn):
        far, core, part, owner, chunk, half = unpack(turn)
        return owner, part, core, [(chunk, jnp.where(far < 0, 2 * half + k, 2 * k)) for k in WAYS]

    return place((gathered,), shapes, begin, end, start_load, lambda srcs: srcs[0].at[0, 0, 0, 0, pl.ds(0, 2)], spots, earlier)


def place_passed(arrays, shapes, earlier):
    def start_load(srcs, turn, slot, sem):
        for k, src in enumerate(srcs):
            @pl.when(lax.div(turn, 2) == k)
            def _():
                pltpu.make_async_copy(src.at[pl.ds(2 * lax.rem(turn, 2), 2)], slot, sem).start()

    def spots(turn):
        coords, core = where_am_i()
        pair, rest = split(turn, 2)
        part, rest = split(rest, PARTS)
        way, other = split(rest, 2)
        owner = lax.rem(pick(part, coords) + 2, RING)
        return owner, part, jnp.where(other == 0, core, 1 - core), [(2 * pair + k, 1 + 2 * way) for k in WAYS]

    return place(arrays, shapes, 0, 2 * len(arrays), start_load, lambda srcs: srcs[0].at[pl.ds(0, 2)], spots, earlier)


def place(srcs, shapes, begin, end, start_load, like, spots, earlier):
    depth = 16
    piece_rows, bn = srcs[0].shape[-2:]
    moved = (end - begin) * 2 * piece_rows * bn
    return pl.pallas_call(
        functools.partial(place_kernel, begin, end, depth, start_load, like, spots, len(srcs)),
        name="place_grads",
        out_shape=[jax.ShapeDtypeStruct(s, jnp.float32) for s in shapes],
        in_specs=[pl.BlockSpec(memory_space=pl.ANY)] * (len(srcs) + len(earlier)),
        out_specs=[pl.BlockSpec(memory_space=pl.ANY)] * 4,
        scratch_shapes=[pltpu.VMEM((depth, 2, piece_rows, bn), jnp.float32), pltpu.SemaphoreType.DMA((depth,)), pltpu.SemaphoreType.DMA((depth,))],
        input_output_aliases={len(srcs) + k: k for k in range(len(earlier))},
        cost_estimate=pl.CostEstimate(flops=16 * moved, bytes_accessed=8 * moved, transcendentals=0),
    )(*srcs, *earlier)


def solution(mesh):
    n_dev = math.prod(mesh.shape.values())
    axes = ("z", "y", "xc")
    batch_spec = P(axes, None)
    whole_spec = P(None, None)

    def device_step(x_loc, g_loc, w_one, w_two, w_three, w_four):
        gathered, passing = reduce_grads(x_loc, g_loc, (w_one, w_two, w_three, w_four), n_dev)
        shapes = (w_one.shape, w_two.shape, w_three.shape, w_four.shape)
        rings = [("xc", mesh.shape["xc"], 2), ("y", RING, 1), ("z", RING, 1)]
        arrived = []
        for way in WAYS:
            for part, (name, size, stride) in enumerate(rings):
                step = stride if way == 0 else size - stride
                arrived.append(lax.ppermute(passing[way * PARTS + part], name, [(k, (k + step) % size) for k in range(size)]))
        turns = 2 * PARTS * (3 * 2 + 1) * CHUNKS
        grads = place_kept(gathered, shapes, 0, turns // 2)
        *grads, arrived = lax.optimization_barrier((*grads, arrived))
        swapped = [lax.ppermute(a, "xc", [(k, k ^ 1) for k in range(mesh.shape["xc"])]) for a in arrived]
        grads = place_kept(gathered, shapes, turns // 2, turns, grads)
        return tuple(place_passed((*arrived, *swapped), shapes, grads))

    return jax.shard_map(
        device_step,
        mesh=mesh,
        in_specs=(batch_spec, batch_spec, whole_spec, whole_spec, whole_spec, whole_spec),
        out_specs=(whole_spec, whole_spec, whole_spec, whole_spec),
        check_vma=False,
    )
```

```python
import functools
import math
import jax
import jax.numpy as jnp
from jax import lax
from jax.experimental import pallas as pl
from jax.experimental.pallas import tpu as pltpu
from jax.sharding import PartitionSpec as P

GELU_SCALE = math.sqrt(2.0 / math.pi)
GELU_CUBIC = 0.044715
MESH = pl.DeviceIdType.MESH
RING = 4
PARTS = 3
CHUNKS = 4
BLOCKS = 3
LEAD = 3
LAG = 18
ORDER = (0, 3, 1, 2)
WAYS = (0, 1)
PIECES = 3


def gelu_parts(pre_act):
    tanh_val = jnp.tanh(GELU_SCALE * (pre_act + GELU_CUBIC * pre_act * pre_act * pre_act))
    value = 0.5 * pre_act * (1.0 + tanh_val)
    return value, 0.5 * (1.0 + tanh_val) + 0.5 * pre_act * (1.0 - tanh_val * tanh_val) * GELU_SCALE * (1.0 + 3.0 * GELU_CUBIC * pre_act * pre_act)


def split(index, n):
    return lax.rem(index, n), lax.div(index, n)


def pick(index, values):
    chosen = values[-1]
    for k in range(len(values) - 2, -1, -1):
        chosen = jnp.where(index == k, values[k], chosen)
    return chosen


def reduce_kernel(rows, bm, scale, *refs):
    bn = 2 * bm
    n_pass = 4 * PARTS
    x_in, g_in, w_one, w_two, w_three, w_four, gath, relay_wid, relay_hid, hid_out, wid_out, *refs = refs
    passing, refs = refs[:n_pass], refs[n_pass:]
    hid = tuple(hid_out.at[which] for which in range(RING))
    wid = (x_in, wid_out.at[0], wid_out.at[1], g_in)
    (hid_v, wid_v, stage, ring2, result, free_sem, act_sem, weight_sem, tile_sem, own_sem,
     near_send, near_recv, hop_send, hop_recv, fwd_send, fwd_recv, stage_send, stage_recv, r1_send, r1_recv, r2_send, r2_recv,
     local_sem, pass_in, pass_out, g_send, g1_recv, g2_recv, g3_recv, cross_send, cross_recv) = refs
    n_stage = stage.shape[0]
    half_rows = rows // 2

    z, y, xc = lax.axis_index("z"), lax.axis_index("y"), lax.axis_index("xc")
    x, core = lax.div(xc, 2), lax.rem(xc, 2)
    coord = (x, y, z)
    first, second = (y, z, x), (z, x, y)
    partner = (z, y, x * 2 + (1 - core))

    def shifted(axis, direction):
        to = lax.rem(coord[axis] + (1 if direction == 0 else RING - 1), RING)
        return ((z, y, to * 2 + core), (z, to, xc), (to, y, xc))[axis]

    def tell_neighbours(sem):
        for axis in range(3):
            for direction in WAYS:
                pl.semaphore_signal(sem, inc=1, device_id=shifted(axis, direction), device_id_type=MESH)
        pl.semaphore_signal(sem, inc=1, device_id=partner, device_id_type=MESH)

    barrier = pltpu.get_barrier_semaphore()
    tell_neighbours(barrier)

    def source(piece, part, which, row, n):
        if piece == 0:
            return wid[which].at[pl.ds(row, n)]
        side = 1 - core if piece == 1 else core
        return hid[which].at[pl.ds(row, n), pl.ds(pl.multiple_of((8 * part + 4 * side) * bm, 4 * bm), 4 * bm)]

    def landing(piece, part, slot, row, n):
        if piece == 0:
            return wid_v.at[part, pl.ds(slot * rows + row, n)]
        return hid_v.at[(piece - 1) * PARTS + part, pl.ds(slot * rows + row, n)]

    def relay(piece, part, direction):
        if piece == 0:
            return relay_wid.at[part, direction]
        return relay_hid.at[piece - 1, part, direction]

    def own(piece, part, which=0):
        return pltpu.make_async_copy(source(piece, part, which, 0, rows), landing(piece, part, 0, 0, rows), own_sem.at[piece, part])

    def near(piece, part, direction, which=0):
        return pltpu.make_async_remote_copy(
            src_ref=source(piece, part, which, 0, rows), dst_ref=landing(piece, part, 1 + 2 * direction, 0, rows),
            send_sem=near_send.at[piece, part, direction], recv_sem=near_recv.at[piece, part, direction],
            device_id=shifted(part, direction), device_id_type=MESH)

    def hop(piece, part, direction, which=0):
        return pltpu.make_async_remote_copy(
            src_ref=source(piece, part, which, direction * half_rows, half_rows), dst_ref=relay(piece, part, direction),
            send_sem=hop_send.at[piece, part, direction], recv_sem=hop_recv.at[piece, part, direction],
            device_id=shifted(part, direction), device_id_type=MESH)

    def forward(piece, part, direction):
        return pltpu.make_async_remote_copy(
            src_ref=relay(piece, part, direction), dst_ref=landing(piece, part, 2, direction * half_rows, half_rows),
            send_sem=fwd_send.at[piece, part, direction], recv_sem=fwd_recv.at[piece, part, direction],
            device_id=shifted(part, direction), device_id_type=MESH)

    def beyond(part, direction):
        return lax.rem(coord[part] + (1 if direction == 0 else RING - 1), RING)

    def round_by(direction, steps):
        return RING - steps if direction == 0 else steps

    def start_for(copy, owner, ready):
        for which in ready:
            @pl.when(owner == which)
            def _():
                copy(which).start()

    def start_hops(piece, ready):
        for part in range(PARTS):
            for direction in WAYS:
                start_for(functools.partial(hop, piece, part, direction), lax.rem(coord[part] + 2, RING), ready)

    def start_nears(piece, ready):
        for part in range(PARTS):
            for direction in WAYS:
                start_for(functools.partial(near, piece, part, direction), beyond(part, direction), ready)

    def start_own(piece):
        for part in range(PARTS):
            start_for(functools.partial(own, piece, part), coord[part], (0, 1, 2, 3))

    def pass_on(piece, ready=None):
        for part in range(PARTS):
            for direction in WAYS:
                def relay_one():
                    hop(piece, part, direction).wait_recv()
                    forward(piece, part, direction).start()

                if ready is None:
                    relay_one()
                    continue
                owner = beyond(part, direction)
                for which in ready:
                    pl.when(owner == which)(relay_one)

    def arrived(piece, part):
        own(piece, part).wait()
        for direction in WAYS:
            near(piece, part, direction).wait_recv()
            forward(piece, part, direction).wait_recv()

    tiles, lead = 12, weight_sem.shape[1] - 1

    def hidden(turn):
        side = jnp.where(turn < tiles // 2, 1 - core, core)
        rest = lax.rem(turn, tiles // 2)
        tile = 4 * lax.div(rest, 2) + 2 * side + lax.rem(rest, 2)
        return pl.ds(pl.multiple_of(tile * bn, bn), bn)

    def rounded(value):
        return value.astype(jnp.bfloat16)

    def widened(value):
        return value.astype(jnp.float32)

    def mm(left, right, transposed=False):
        return lax.dot_general(left, right, (((1,), (1 if transposed else 0,)), ((), ())), preferred_element_type=jnp.float32)

    def products(columns_v, rows_v, acts, out_tiles, total, a_one):
        def weight_copy(kind, weight, tile):
            slot = lax.rem(tile, lead + 1)
            if kind == 0:
                return pltpu.make_async_copy(weight.at[:, hidden(tile)], columns_v.at[slot], weight_sem.at[kind, slot])
            return pltpu.make_async_copy(weight.at[hidden(tile)], rows_v.at[slot], weight_sem.at[kind, slot])

        def tile_copy(index, ref, tile):
            return pltpu.make_async_copy(out_tiles.at[index], ref.at[:, hidden(tile)], tile_sem.at[index])

        def close_total(base, index, ref, sem):
            acts[index] = rounded(total[...] + widened(acts[base]))
            copy = pltpu.make_async_copy(acts.at[index], ref, act_sem.at[sem])
            copy.start()
            copy.wait()

        def sweep(weights, following, step, outs, midway):
            def turn(tile, carry):
                for kind, weight in weights:
                    @pl.when(tile < tiles - lead)
                    def _():
                        weight_copy(kind, weight, tile + lead).start()

                for kind, weight in following:
                    @pl.when(tile >= tiles - lead)
                    def _():
                        weight_copy(kind, weight, tile + lead - tiles).start()

                for kind, weight in weights:
                    weight_copy(kind, weight, tile).wait()
                slot = lax.rem(tile, 2)

                @pl.when(tile >= 2)
                def _():
                    for k, ref in enumerate(outs):
                        tile_copy(2 * k + slot, ref, tile).wait()

                step(tile, slot, lax.rem(tile, lead + 1))
                for k, ref in enumerate(outs):
                    tile_copy(2 * k + slot, ref, tile).start()
                return carry

            most = 2 * tiles // 3
            lax.fori_loop(0, most, turn, 0)
            midway()
            lax.fori_loop(most, tiles, turn, 0)
            for slot in WAYS:
                for k, ref in enumerate(outs):
                    tile_copy(2 * k + slot, ref, slot).wait()

        for tile in range(lead):
            weight_copy(0, w_one, tile).start()
            weight_copy(1, w_two, tile).start()
        loads = [pltpu.make_async_copy(ref, acts.at[k], act_sem.at[k]) for k, ref in enumerate((x_in, g_in))]
        for copy in loads:
            copy.start()
        total[...] = jnp.zeros(total.shape, jnp.float32)
        pl.semaphore_wait(barrier, 7)
        start_hops(0, (0, 3))
        start_nears(0, (0, 3))
        for copy in loads:
            copy.wait()

        def first_forward(tile, slot, load):
            pre = rounded(mm(acts[0], columns_v[load]))
            a_one[tile] = pre
            act = rounded(gelu_parts(widened(pre))[0])
            out_tiles[slot] = act
            total[...] = total[...] + mm(act, rows_v[load])

        def midway_one():
            start_hops(1, (1,))
            start_nears(1, (1,))

        with jax.named_scope("first_forward"):
            sweep(((0, w_one), (1, w_two)), ((0, w_three), (1, w_four)), first_forward, (hid[1],), midway_one)
            start_hops(2, (1,))
            close_total(0, 2, wid[2], 2)
        total[...] = jnp.zeros(total.shape, jnp.float32)
        start_hops(0, (2,))
        start_nears(0, (2,))
        start_nears(2, (1,))
        pass_on(0, (0, 3))

        def second_block(tile, slot, load):
            pre = widened(rounded(mm(acts[2], columns_v[load])))
            back = mm(acts[1], rows_v[load], True)
            act, slope = gelu_parts(pre)
            out_tiles[slot] = rounded(act)
            grad = rounded(back * slope)
            out_tiles[2 + slot] = grad
            total[...] = total[...] + mm(grad, columns_v[load], True)

        def midway_two():
            start_hops(1, (2, 3))
            start_nears(1, (2, 3))

        with jax.named_scope("second_block"):
            sweep(((0, w_three), (1, w_four)), ((1, w_two),), second_block, (hid[3], hid[2]), midway_two)
            start_hops(2, (2, 3))
            close_total(1, 0, wid[1], 3)
        start_hops(0, (1,))
        start_nears(0, (1,))
        start_nears(2, (2, 3))

        def first_backward(tile, slot, load):
            back = mm(acts[0], rows_v[load], True)
            out_tiles[slot] = rounded(back * gelu_parts(widened(a_one[tile]))[1])

        def midway_three():
            start_hops(1, (0,))
            start_nears(1, (0,))
            pass_on(1, (1,))
            pass_on(2, (1,))
            pass_on(0, (2,))

        with jax.named_scope("first_backward"):
            sweep(((1, w_two),), (), first_backward, (hid[0],), midway_three)
        start_hops(2, (0,))
        start_nears(2, (0,))

    width = wid_v.shape[-1]
    pl.run_scoped(
        products, pltpu.VMEM((lead + 1, width, bn), jnp.bfloat16), pltpu.VMEM((lead + 1, bn, width), jnp.bfloat16),
        pltpu.VMEM((3, rows, width), jnp.bfloat16), pltpu.VMEM((4, rows, bn), jnp.bfloat16), pltpu.VMEM((rows, width), jnp.float32),
        pltpu.VMEM((tiles, rows, bn), jnp.bfloat16))

    def sums(acc, ring1):
        def product(side, part, chunk, block, store):
            odd = lax.rem(pick(part, coord), 2)
            dims = (((0,), (0,)), ((), ()))

            @pl.when(odd == 1)
            def _():
                left = hid_v[side * PARTS + part, :, pl.ds(pl.multiple_of(chunk * bm, bm), bm)]
                right = wid_v[part, :, pl.ds(pl.multiple_of(block * bn, bn), bn)]
                store(lax.dot_general(left, right, dims, preferred_element_type=jnp.float32))

            @pl.when(odd == 0)
            def _():
                index = 3 * chunk + block
                left = wid_v[part, :, pl.ds(pl.multiple_of(lax.div(index, 2) * bm, bm), bm)]
                right = hid_v[side * PARTS + part, :, pl.ds(pl.multiple_of(lax.rem(index, 2) * bn, bn), bn)]
                store(lax.dot_general(left, right, dims, preferred_element_type=jnp.float32))

        def hand_over(part=0, chunk=0, block=0, slot=0):
            return pltpu.make_async_remote_copy(
                src_ref=stage.at[slot], dst_ref=acc.at[part, chunk, block], send_sem=stage_send.at[slot],
                recv_sem=stage_recv.at[part, chunk, block], device_id=partner, device_id_type=MESH)

        tell_neighbours(free_sem)
        with jax.named_scope("send_last"):
            pass_on(0, (1,))
            pass_on(1, (2, 3))
            pass_on(2, (2, 3))
            pass_on(1, (0,))
            for piece in range(PIECES):
                start_own(piece)
        with jax.named_scope("await_other"):
            pl.semaphore_wait(free_sem, 7)
            for piece in range(PIECES - 1):
                for part in range(PARTS):
                    arrived(piece, part)

        top, low = bm // 2, bm // 8

        def ring1_copy(part, direction, step, block):
            chunk = lax.rem(first[part] + round_by(direction, 1 + step), RING)
            return pltpu.make_async_remote_copy(
                src_ref=acc.at[part, chunk, block, pl.ds(direction * top, top)], dst_ref=ring1.at[part, direction, step, block],
                send_sem=r1_send.at[part, direction, block], recv_sem=r1_recv.at[part, direction, step, block],
                device_id=shifted((part + 1) % 3, direction), device_id_type=MESH)

        def place_of(count):
            part, rest = split(count, PARTS)
            early = rest < 2 * BLOCKS
            order = jnp.where(early, lax.rem(rest, 2), lax.div(rest, BLOCKS))
            block = jnp.where(early, lax.div(rest, 2), lax.rem(rest, BLOCKS))
            return order, part, lax.rem(pick(part, first) + pick(order, (3, 1, 2, 0)), RING), block

        blocks = CHUNKS * PARTS * BLOCKS

        def both_halves(count, carry):
            @pl.when(count < blocks)
            def _():
                _, part, chunk, block = place_of(count)
                slot = lax.rem(count, n_stage)

                @pl.when(count >= n_stage)
                def _():
                    hand_over(slot=slot).wait_send()

                def store(value):
                    stage[slot] = value

                product(0, part, chunk, block, store)
                hand_over(part, chunk, block, slot).start()

            @pl.when(count >= LAG)
            def _():
                order, part, chunk, block = place_of(count - LAG)
                hand_over(part, chunk, block).wait_recv()

                def store(value):
                    acc[part, chunk, block] = acc[part, chunk, block] + value

                product(1, part, chunk, block, store)
                for direction in WAYS:
                    for which in range(PARTS):
                        @pl.when((order == direction) & (part == which))
                        def _():
                            ring1_copy(which, direction, 0, block).start()

            return carry

        def ring1_step(step):
            for block in range(BLOCKS):
                for part in range(PARTS):
                    for direction in WAYS:
                        ring1_copy(part, direction, step, block).wait_recv()
                        chunk = lax.rem(first[part] + round_by(direction, 2 + step), RING)
                        share = acc.at[part, chunk, block, pl.ds(direction * top, top)]
                        share[...] = share[...] + ring1[part, direction, step, block]
                        ring1_copy(part, direction, step, block).wait_send()
                        if step < RING - 2:
                            ring1_copy(part, direction, step + 1, block).start()
                    if step == RING - 2:
                        for direction in WAYS:
                            ring2_copy(part, direction, 0, block).start()

        with jax.named_scope("other_half"):
            lax.fori_loop(0, LAG, both_halves, 0)
        with jax.named_scope("await_own"):
            pass_on(2, (0,))
            for part in range(PARTS):
                arrived(2, part)
        last = blocks - PARTS * BLOCKS
        with jax.named_scope("halves"):
            lax.fori_loop(LAG, last + LAG, both_halves, 0)
        def ring2_share(part, direction, block, place):
            row = pl.multiple_of(2 * low * place + direction * low, low)
            return acc.at[part, first[part], block, pl.ds(row, low)]

        def ring2_copy(part, direction, step, block):
            place = lax.rem(second[part] + round_by(direction, 1 + step), RING)
            return pltpu.make_async_remote_copy(
                src_ref=ring2_share(part, direction, block, place), dst_ref=ring2.at[part, direction, step, block],
                send_sem=r2_send.at[part, direction, block], recv_sem=r2_recv.at[part, direction, step, block],
                device_id=shifted((part + 2) % 3, direction), device_id_type=MESH)

        with jax.named_scope("ring1#step=0"):
            ring1_step(0)
        with jax.named_scope("last_chunk"):
            lax.fori_loop(last + LAG, blocks + LAG, both_halves, 0)
        for step in range(1, RING - 1):
            with jax.named_scope(f"ring1#step={step}"):
                ring1_step(step)

        with jax.named_scope("ring2"):
            for step in range(RING - 1):
                for block in range(BLOCKS):
                    for part in range(PARTS):
                        for direction in WAYS:
                            ring2_copy(part, direction, step, block).wait_recv()
                            place = lax.rem(second[part] + round_by(direction, 2 + step), RING)
                            share = ring2_share(part, direction, block, place)
                            value = share[...] + ring2[part, direction, step, block]
                            ring2_copy(part, direction, step, block).wait_send()
                            if step < RING - 2:
                                share[...] = value
                                ring2_copy(part, direction, step + 1, block).start()
                            else:
                                result[part, pl.ds(2 * low * block + direction * low, low)] = value * scale

        for slot in range(n_stage):
            hand_over(slot=slot).wait_send()

    pl.run_scoped(
        sums, pltpu.VMEM((PARTS, CHUNKS, BLOCKS, bm, bn), jnp.float32),
        pltpu.VMEM((PARTS, 2, RING - 1, BLOCKS, bm // 2, bn), jnp.float32))

    piece_rows = result.shape[1]
    cut = piece_rows // 16 * 8

    def after(place, by):
        return lax.rem(place + by, RING)

    def at(part, owner, chunk, quarter=None):
        view = gath.at[core, part, owner, chunk]
        return view if quarter is None else view.at[quarter]

    def send(src, dst, sem, recv, axis, direction):
        return pltpu.make_async_remote_copy(
            src_ref=src, dst_ref=dst, send_sem=sem, recv_sem=recv, device_id=shifted(axis, direction), device_id_type=MESH)

    def quarter_copy(part, direction, leg):
        sem, recv = g_send.at[0, part], g1_recv.at[part, direction, leg]
        axis = (part + 2) % 3
        if leg == 0:
            src, dst = result.at[part], at(part, coord[part], first[part], second[part])
            return send(src, dst, sem, recv, axis, direction)
        view = at(part, coord[part], first[part], after(second[part], 3 - 2 * direction))
        view = view.at[pl.ds(0, cut)] if direction == 0 else view.at[pl.ds(cut, piece_rows - cut)]
        return send(view, view, sem, recv, axis, direction)

    def chunk_copy(part, direction, leg):
        sem, recv = g_send.at[1, part], g2_recv.at[part, direction, leg]
        axis = (part + 1) % 3
        view = at(part, coord[part], first[part])
        if leg == 1:
            view = at(part, coord[part], after(first[part], 3 - 2 * direction)).at[pl.ds(2 * direction, 2)]
        return send(view, view, sem, recv, axis, direction)

    def owner_copy(part, direction, order):
        view = at(part, coord[part], after(first[part], ORDER[order]))
        return send(view, view, g_send.at[2, part], g3_recv.at[part, direction, order], part, direction)

    def cross(part, owner, order):
        view = at(part, owner, after(first[part], ORDER[order]))
        return pltpu.make_async_remote_copy(
            src_ref=view, dst_ref=view, send_sem=cross_send, recv_sem=cross_recv, device_id=partner, device_id_type=MESH)

    def keep(part):
        return pltpu.make_async_copy(result.at[part], at(part, coord[part], first[part], second[part]), local_sem.at[part])

    turns = [(order, part, direction) for order in range(CHUNKS) for part in range(PARTS) for direction in WAYS]

    def passing_in(turn):
        order, part, direction = turns[turn]
        view = at(part, beyond(part, 1 - direction), after(first[part], ORDER[order]), pl.ds(2 * direction, 2))
        slot = turn % 2
        return pltpu.make_async_copy(view, stage.at[pl.ds(2 * slot, 2), pl.ds(0, piece_rows)], pass_in.at[slot])

    def passing_out(turn):
        order, part, direction = turns[turn]
        chunk = after(first[part], ORDER[order])
        return [pltpu.make_async_copy(
            stage.at[2 * (turn % 2) + k, pl.ds(0, piece_rows)],
            passing[(2 * k + direction) * PARTS + part].at[chunk], pass_out.at[turn % 2, k]) for k in WAYS]

    def pass_further(turn):
        passing_in(turn).wait()
        for copy in passing_out(turn):
            copy.start()

    def passed(turn):
        for copy in passing_out(turn):
            copy.wait()

    with jax.named_scope("gather"):
        for part in range(PARTS):
            for direction in WAYS:
                quarter_copy(part, direction, 0).start()
            keep(part).start()
        for part in range(PARTS):
            for direction in WAYS:
                quarter_copy(part, direction, 0).wait_recv()
                quarter_copy(part, direction, 1).start()
        for part in range(PARTS):
            keep(part).wait()
            for direction in WAYS:
                quarter_copy(part, direction, 1).wait_recv()
            for direction in WAYS:
                chunk_copy(part, direction, 0).start()
            for direction in WAYS:
                owner_copy(part, direction, 0).start()
            cross(part, coord[part], 0).start()
        for part in range(PARTS):
            for direction in WAYS:
                chunk_copy(part, direction, 0).wait_recv()
                chunk_copy(part, direction, 1).start()
            for order in (1, 2):
                for direction in WAYS:
                    owner_copy(part, direction, order).start()
                cross(part, coord[part], order).start()
        for part in range(PARTS):
            for direction in WAYS:
                chunk_copy(part, direction, 1).wait_recv()
            for direction in WAYS:
                owner_copy(part, direction, 3).start()
            cross(part, coord[part], 3).start()
        for turn, (order, part, direction) in enumerate(turns):
            owner_copy(part, direction, order).wait_recv()
            cross(part, beyond(part, 1 - direction), order).start()
            if turn > 1:
                passed(turn - 2)
            passing_in(turn).start()
            if turn > 0:
                pass_further(turn - 1)
        pass_further(len(turns) - 1)
        for turn in range(len(turns) - 2, len(turns)):
            passed(turn)

    for piece in range(PIECES):
        for part in range(PARTS):
            for direction in WAYS:
                near(piece, part, direction).wait_send()
                hop(piece, part, direction).wait_send()
                forward(piece, part, direction).wait_send()

    def drain(view, sem):
        pltpu.make_async_copy(view, view, sem).wait()

    for part in range(PARTS):
        drain(gath.at[core, part, 0, 0, pl.ds(0, 3)], g_send.at[0, part])
        drain(gath.at[core, part, 0, pl.ds(0, 3)], g_send.at[1, part])
        drain(gath.at[core, part, pl.ds(0, 2)], g_send.at[2, part])
    drain(gath.at[core, :, pl.ds(0, 3)], cross_send)
    drain(gath.at[1 - core, :, pl.ds(0, 3)], cross_recv)


def reduce_grads(x_loc, g_loc, weights, n_dev):
    rows, width = x_loc.shape
    bm = width // 6
    bn = 2 * bm
    dma = pltpu.SemaphoreType.DMA
    any_spec = pl.BlockSpec(memory_space=pl.ANY)
    f32, bf16 = jnp.float32, jnp.bfloat16
    n_stage = 4
    piece_rows = BLOCKS * (bm // 4)
    outs = pl.pallas_call(
        functools.partial(reduce_kernel, rows, bm, 1.0 / n_dev),
        name="reduce_grads",
        out_shape=[
            jax.ShapeDtypeStruct((2, PARTS, RING, CHUNKS, RING, piece_rows, bn), f32),
            jax.ShapeDtypeStruct((PARTS, 2, rows // 2, width), bf16),
            jax.ShapeDtypeStruct((2, PARTS, 2, rows // 2, 4 * bm), bf16),
            jax.ShapeDtypeStruct((4, rows, 24 * bm), bf16),
            jax.ShapeDtypeStruct((2, rows, width), bf16),
            *[jax.ShapeDtypeStruct((CHUNKS, piece_rows, bn), f32)] * (4 * PARTS),
        ],
        in_specs=[any_spec] * 6,
        out_specs=[any_spec] * (5 + 4 * PARTS),
        scratch_shapes=[
            pltpu.VMEM((2 * PARTS, RING * rows, 4 * bm), bf16),
            pltpu.VMEM((PARTS, RING * rows, width), bf16),
            pltpu.VMEM((n_stage, bm, bn), f32),
            pltpu.VMEM((PARTS, 2, RING - 1, BLOCKS, bm // 8, bn), f32),
            pltpu.VMEM((PARTS, piece_rows, bn), f32),
            pltpu.SemaphoreType.REGULAR, dma((4,)), dma((2, LEAD + 1)), dma((4,)),
            dma((PIECES, PARTS)),
            *[dma((PIECES, PARTS, 2))] * 6,
            dma((n_stage,)), dma((PARTS, CHUNKS, BLOCKS)),
            dma((PARTS, 2, BLOCKS)), dma((PARTS, 2, RING - 1, BLOCKS)),
            dma((PARTS, 2, BLOCKS)), dma((PARTS, 2, RING - 1, BLOCKS)),
            dma((PARTS,)), dma((2,)), dma((2, 2)), dma((3, PARTS)),
            dma((PARTS, 2, 2)), dma((PARTS, 2, 2)), dma((PARTS, 2, CHUNKS)),
            dma, dma,
        ],
        compiler_params=pltpu.CompilerParams(collective_id=0, has_side_effects=True, vmem_limit_bytes=67043328),
        cost_estimate=pl.CostEstimate(flops=40 * rows * 24 * bm * width, bytes_accessed=200_000_000, transcendentals=0),
    )(x_loc, g_loc, *weights)
    return outs[0], outs[5:]


def place_kernel(begin, end, depth, start_load, like, spots, n_src, *refs):
    srcs, dsts = refs[:n_src], refs[-7:-3]
    slots, in_sem, out_sem = refs[-3:]
    ahead = depth // 2

    def load(turn):
        slot = lax.rem(turn, depth)
        start_load(srcs, turn, slots.at[slot], in_sem.at[slot])

    def settle(turn, sem):
        slot = lax.rem(turn, depth)
        pltpu.make_async_copy(like(srcs), slots.at[slot], sem.at[slot]).wait()

    def store(turn):
        slot = lax.rem(turn, depth)
        owner, part, core, pieces = spots(turn)
        bn = slots.shape[-1]
        quarter_rows = bn // 8
        for which in range(RING):
            @pl.when(owner == which)
            def _():
                for k, (chunk, quarter) in enumerate(pieces):
                    for block in range(BLOCKS):
                        rows, cols = spot(bn // 2, which, part, core, chunk, quarter, block)
                        pltpu.make_async_copy(
                            slots.at[slot, k, pl.ds(block * quarter_rows, quarter_rows)], dsts[which].at[rows, cols], out_sem.at[slot]).start()

    def prime(turn, carry):
        load(turn)
        return carry

    def body(turn, carry):
        @pl.when(turn + ahead < end)
        def _():
            @pl.when(turn + ahead >= begin + depth)
            def _():
                settle(turn + ahead - depth, out_sem)

            load(turn + ahead)

        settle(turn, in_sem)
        store(turn)
        return carry

    def finish(turn, carry):
        settle(turn, out_sem)
        return carry

    lax.fori_loop(begin, begin + ahead, prime, 0)
    lax.fori_loop(begin, end, body, 0)
    lax.fori_loop(end - depth, end, finish, 0)


def spot(bm, which, part, core, chunk, quarter, block):
    bn = 2 * bm
    if which % 2:
        start = (8 * part + 4 * core + chunk) * bm
        col = block * bn
    else:
        index = 3 * chunk + block
        start = lax.div(index, 2) * bm
        col = (4 * part + 2 * core + lax.rem(index, 2)) * bn
    rows = bm // 4
    return pl.ds(pl.multiple_of(start + quarter * rows, rows), rows), pl.ds(pl.multiple_of(col, bn), bn)


def where_am_i():
    z, y, xc = lax.axis_index("z"), lax.axis_index("y"), lax.axis_index("xc")
    return (lax.div(xc, 2), y, z), lax.rem(xc, 2)


def place_kept(gathered, shapes, begin, end, earlier=()):
    def unpack(turn):
        coords, _ = where_am_i()
        half, rest = split(turn, 2)
        chunk, rest = split(rest, CHUNKS)
        by, rest = split(rest, 3)
        part, core = split(rest, PARTS)
        return core, part, lax.rem(pick(part, coords) + pick(by, (0, 1, 3)), RING), chunk, half

    def start_load(srcs, turn, slot, sem):
        core, part, owner, chunk, half = unpack(turn)
        pltpu.make_async_copy(srcs[0].at[core, part, owner, chunk, pl.ds(2 * half, 2)], slot, sem).start()

    def spots(turn):
        core, part, owner, chunk, half = unpack(turn)
        return owner, part, core, [(chunk, 2 * half + k) for k in WAYS]

    return place((gathered,), shapes, begin, end, start_load, lambda srcs: srcs[0].at[0, 0, 0, 0, pl.ds(0, 2)], spots, earlier)


def place_passed(arrays, group, shapes, earlier):
    def start_load(srcs, turn, slot, sem):
        for k, src in enumerate(srcs):
            @pl.when(lax.div(turn, 2) == k)
            def _():
                pltpu.make_async_copy(src.at[pl.ds(2 * lax.rem(turn, 2), 2)], slot, sem).start()

    def spots(turn):
        coords, core = where_am_i()
        pair, rest = split(turn, 2)
        part, rest = split(rest, PARTS)
        way, other = split(rest, 2)
        owner = lax.rem(pick(part, coords) + 2, RING)
        return owner, part, jnp.where(other == 0, core, 1 - core), [(2 * pair + k, group + 2 * way) for k in WAYS]

    return place(arrays, shapes, 0, 2 * len(arrays), start_load, lambda srcs: srcs[0].at[pl.ds(0, 2)], spots, earlier)


def place(srcs, shapes, begin, end, start_load, like, spots, earlier):
    depth = 16
    piece_rows, bn = srcs[0].shape[-2:]
    moved = (end - begin) * 2 * piece_rows * bn
    return pl.pallas_call(
        functools.partial(place_kernel, begin, end, depth, start_load, like, spots, len(srcs)),
        name="place_grads",
        out_shape=[jax.ShapeDtypeStruct(s, jnp.float32) for s in shapes],
        in_specs=[pl.BlockSpec(memory_space=pl.ANY)] * (len(srcs) + len(earlier)),
        out_specs=[pl.BlockSpec(memory_space=pl.ANY)] * 4,
        scratch_shapes=[pltpu.VMEM((depth, 2, piece_rows, bn), jnp.float32), pltpu.SemaphoreType.DMA((depth,)), pltpu.SemaphoreType.DMA((depth,))],
        input_output_aliases={len(srcs) + k: k for k in range(len(earlier))},
        cost_estimate=pl.CostEstimate(flops=16 * moved, bytes_accessed=8 * moved, transcendentals=0),
    )(*srcs, *earlier)


def solution(mesh):
    n_dev = math.prod(mesh.shape.values())
    axes = ("z", "y", "xc")
    batch_spec = P(axes, None)
    whole_spec = P(None, None)

    def device_step(x_loc, g_loc, w_one, w_two, w_three, w_four):
        gathered, passing = reduce_grads(x_loc, g_loc, (w_one, w_two, w_three, w_four), n_dev)
        shapes = (w_one.shape, w_two.shape, w_three.shape, w_four.shape)
        rings = [("xc", mesh.shape["xc"], 2), ("y", RING, 1), ("z", RING, 1)]
        arrived = []
        for group in WAYS:
            arrived.append([])
            for way in WAYS:
                for part, (name, size, stride) in enumerate(rings):
                    step = stride if way == 0 else size - stride
                    source = passing[(2 * group + way) * PARTS + part]
                    arrived[group].append(lax.ppermute(source, name, [(k, (k + step) % size) for k in range(size)]))
        turns = 2 * PARTS * 3 * CHUNKS * 2
        swapped = []
        grads = ()
        for group in WAYS:
            grads = place_kept(gathered, shapes, group * turns // 2, (1 + group) * turns // 2, grads)
            *grads, arrived[group] = lax.optimization_barrier((*grads, arrived[group]))
            swapped.append([lax.ppermute(a, "xc", [(k, k ^ 1) for k in range(mesh.shape["xc"])]) for a in arrived[group]])
        for group in WAYS:
            grads = place_passed((*arrived[group], *swapped[group]), group, shapes, grads)
        return tuple(grads)

    return jax.shard_map(
        device_step,
        mesh=mesh,
        in_specs=(batch_spec, batch_spec, whole_spec, whole_spec, whole_spec, whole_spec),
        out_specs=(whole_spec, whole_spec, whole_spec, whole_spec),
        check_vma=False,
    )
```

```python
import functools
import math
import jax
import jax.numpy as jnp
from jax import lax
from jax.experimental import pallas as pl
from jax.experimental.pallas import tpu as pltpu
from jax.sharding import PartitionSpec as P

GELU_SCALE = math.sqrt(2.0 / math.pi)
GELU_CUBIC = 0.044715
MESH = pl.DeviceIdType.MESH
RING = 4
PARTS = 3
CHUNKS = 4
BLOCKS = 3
LEAD = 3
LAG = 18
ORDER = (0, 3, 1, 2)
WAYS = (0, 1)
PIECES = 3


def gelu_parts(pre_act):
    tanh_val = jnp.tanh(GELU_SCALE * (pre_act + GELU_CUBIC * pre_act * pre_act * pre_act))
    value = 0.5 * pre_act * (1.0 + tanh_val)
    return value, 0.5 * (1.0 + tanh_val) + 0.5 * pre_act * (1.0 - tanh_val * tanh_val) * GELU_SCALE * (1.0 + 3.0 * GELU_CUBIC * pre_act * pre_act)


def split(index, n):
    return lax.rem(index, n), lax.div(index, n)


def pick(index, values):
    chosen = values[-1]
    for k in range(len(values) - 2, -1, -1):
        chosen = jnp.where(index == k, values[k], chosen)
    return chosen


def reduce_kernel(rows, bm, scale, *refs):
    bn = 2 * bm
    n_pass = 4 * PARTS
    x_in, g_in, w_one, w_two, w_three, w_four, gath, own_out, relay_wid, relay_hid, hid_out, wid_out, *refs = refs
    passing, refs = refs[:n_pass], refs[n_pass:]
    hid = tuple(hid_out.at[which] for which in range(RING))
    wid = (x_in, wid_out.at[0], wid_out.at[1], g_in)
    (hid_v, wid_v, stage, ring2, result, free_sem, act_sem, weight_sem, tile_sem, own_sem,
     near_send, near_recv, hop_send, hop_recv, fwd_send, fwd_recv, stage_send, stage_recv, r1_send, r1_recv, r2_send, r2_recv,
     local_sem, pass_in, pass_out, g_send, g1_recv, g2_recv, g3_recv, cross_send, cross_recv) = refs
    n_stage = stage.shape[0]
    half_rows = rows // 2

    z, y, xc = lax.axis_index("z"), lax.axis_index("y"), lax.axis_index("xc")
    x, core = lax.div(xc, 2), lax.rem(xc, 2)
    coord = (x, y, z)
    first, second = (y, z, x), (z, x, y)
    partner = (z, y, x * 2 + (1 - core))

    def shifted(axis, direction):
        to = lax.rem(coord[axis] + (1 if direction == 0 else RING - 1), RING)
        return ((z, y, to * 2 + core), (z, to, xc), (to, y, xc))[axis]

    def tell_neighbours(sem):
        for axis in range(3):
            for direction in WAYS:
                pl.semaphore_signal(sem, inc=1, device_id=shifted(axis, direction), device_id_type=MESH)
        pl.semaphore_signal(sem, inc=1, device_id=partner, device_id_type=MESH)

    barrier = pltpu.get_barrier_semaphore()
    tell_neighbours(barrier)

    def source(piece, part, which, row, n):
        if piece == 0:
            return wid[which].at[pl.ds(row, n)]
        side = 1 - core if piece == 1 else core
        return hid[which].at[pl.ds(row, n), pl.ds(pl.multiple_of((8 * part + 4 * side) * bm, 4 * bm), 4 * bm)]

    def landing(piece, part, slot, row, n):
        if piece == 0:
            return wid_v.at[part, pl.ds(slot * rows + row, n)]
        return hid_v.at[(piece - 1) * PARTS + part, pl.ds(slot * rows + row, n)]

    def relay(piece, part, direction):
        if piece == 0:
            return relay_wid.at[part, direction]
        return relay_hid.at[piece - 1, part, direction]

    def own(piece, part, which=0):
        return pltpu.make_async_copy(source(piece, part, which, 0, rows), landing(piece, part, 0, 0, rows), own_sem.at[piece, part])

    def near(piece, part, direction, which=0):
        return pltpu.make_async_remote_copy(
            src_ref=source(piece, part, which, 0, rows), dst_ref=landing(piece, part, 1 + 2 * direction, 0, rows),
            send_sem=near_send.at[piece, part, direction], recv_sem=near_recv.at[piece, part, direction],
            device_id=shifted(part, direction), device_id_type=MESH)

    def hop(piece, part, direction, which=0):
        return pltpu.make_async_remote_copy(
            src_ref=source(piece, part, which, direction * half_rows, half_rows), dst_ref=relay(piece, part, direction),
            send_sem=hop_send.at[piece, part, direction], recv_sem=hop_recv.at[piece, part, direction],
            device_id=shifted(part, direction), device_id_type=MESH)

    def forward(piece, part, direction):
        return pltpu.make_async_remote_copy(
            src_ref=relay(piece, part, direction), dst_ref=landing(piece, part, 2, direction * half_rows, half_rows),
            send_sem=fwd_send.at[piece, part, direction], recv_sem=fwd_recv.at[piece, part, direction],
            device_id=shifted(part, direction), device_id_type=MESH)

    def beyond(part, direction):
        return lax.rem(coord[part] + (1 if direction == 0 else RING - 1), RING)

    def round_by(direction, steps):
        return RING - steps if direction == 0 else steps

    def start_for(copy, owner, ready):
        for which in ready:
            @pl.when(owner == which)
            def _():
                copy(which).start()

    def start_hops(piece, ready):
        for part in range(PARTS):
            for direction in WAYS:
                start_for(functools.partial(hop, piece, part, direction), lax.rem(coord[part] + 2, RING), ready)

    def start_nears(piece, ready):
        for part in range(PARTS):
            for direction in WAYS:
                start_for(functools.partial(near, piece, part, direction), beyond(part, direction), ready)

    def start_own(piece):
        for part in range(PARTS):
            start_for(functools.partial(own, piece, part), coord[part], (0, 1, 2, 3))

    def pass_on(piece, ready=None):
        for part in range(PARTS):
            for direction in WAYS:
                def relay_one():
                    hop(piece, part, direction).wait_recv()
                    forward(piece, part, direction).start()

                if ready is None:
                    relay_one()
                    continue
                owner = beyond(part, direction)
                for which in ready:
                    pl.when(owner == which)(relay_one)

    def arrived(piece, part):
        own(piece, part).wait()
        for direction in WAYS:
            near(piece, part, direction).wait_recv()
            forward(piece, part, direction).wait_recv()

    tiles, lead = 12, weight_sem.shape[1] - 1

    def hidden(turn):
        side = jnp.where(turn < tiles // 2, 1 - core, core)
        rest = lax.rem(turn, tiles // 2)
        tile = 4 * lax.div(rest, 2) + 2 * side + lax.rem(rest, 2)
        return pl.ds(pl.multiple_of(tile * bn, bn), bn)

    def rounded(value):
        return value.astype(jnp.bfloat16)

    def widened(value):
        return value.astype(jnp.float32)

    def mm(left, right, transposed=False):
        return lax.dot_general(left, right, (((1,), (1 if transposed else 0,)), ((), ())), preferred_element_type=jnp.float32)

    def products(columns_v, rows_v, acts, out_tiles, total, a_one):
        def weight_copy(kind, weight, tile):
            slot = lax.rem(tile, lead + 1)
            if kind == 0:
                return pltpu.make_async_copy(weight.at[:, hidden(tile)], columns_v.at[slot], weight_sem.at[kind, slot])
            return pltpu.make_async_copy(weight.at[hidden(tile)], rows_v.at[slot], weight_sem.at[kind, slot])

        def tile_copy(index, ref, tile):
            return pltpu.make_async_copy(out_tiles.at[index], ref.at[:, hidden(tile)], tile_sem.at[index])

        def close_total(base, index, ref, sem):
            acts[index] = rounded(total[...] + widened(acts[base]))
            copy = pltpu.make_async_copy(acts.at[index], ref, act_sem.at[sem])
            copy.start()
            copy.wait()

        def sweep(weights, following, step, outs, midway):
            def turn(tile, carry):
                for kind, weight in weights:
                    @pl.when(tile < tiles - lead)
                    def _():
                        weight_copy(kind, weight, tile + lead).start()

                for kind, weight in following:
                    @pl.when(tile >= tiles - lead)
                    def _():
                        weight_copy(kind, weight, tile + lead - tiles).start()

                for kind, weight in weights:
                    weight_copy(kind, weight, tile).wait()
                slot = lax.rem(tile, 2)

                @pl.when(tile >= 2)
                def _():
                    for k, ref in enumerate(outs):
                        tile_copy(2 * k + slot, ref, tile).wait()

                step(tile, slot, lax.rem(tile, lead + 1))
                for k, ref in enumerate(outs):
                    tile_copy(2 * k + slot, ref, tile).start()
                return carry

            most = 2 * tiles // 3
            lax.fori_loop(0, most, turn, 0)
            midway()
            lax.fori_loop(most, tiles, turn, 0)
            for slot in WAYS:
                for k, ref in enumerate(outs):
                    tile_copy(2 * k + slot, ref, slot).wait()

        for tile in range(lead):
            weight_copy(0, w_one, tile).start()
            weight_copy(1, w_two, tile).start()
        loads = [pltpu.make_async_copy(ref, acts.at[k], act_sem.at[k]) for k, ref in enumerate((x_in, g_in))]
        for copy in loads:
            copy.start()
        total[...] = jnp.zeros(total.shape, jnp.float32)
        pl.semaphore_wait(barrier, 7)
        start_hops(0, (0, 3))
        start_nears(0, (0, 3))
        for copy in loads:
            copy.wait()

        def first_forward(tile, slot, load):
            pre = rounded(mm(acts[0], columns_v[load]))
            a_one[tile] = pre
            act = rounded(gelu_parts(widened(pre))[0])
            out_tiles[slot] = act
            total[...] = total[...] + mm(act, rows_v[load])

        def midway_one():
            start_hops(1, (1,))
            start_nears(1, (1,))

        with jax.named_scope("first_forward"):
            sweep(((0, w_one), (1, w_two)), ((0, w_three), (1, w_four)), first_forward, (hid[1],), midway_one)
            start_hops(2, (1,))
            close_total(0, 2, wid[2], 2)
        total[...] = jnp.zeros(total.shape, jnp.float32)
        start_hops(0, (2,))
        start_nears(0, (2,))
        start_nears(2, (1,))
        pass_on(0, (0, 3))

        def second_block(tile, slot, load):
            pre = widened(rounded(mm(acts[2], columns_v[load])))
            back = mm(acts[1], rows_v[load], True)
            act, slope = gelu_parts(pre)
            out_tiles[slot] = rounded(act)
            grad = rounded(back * slope)
            out_tiles[2 + slot] = grad
            total[...] = total[...] + mm(grad, columns_v[load], True)

        def midway_two():
            start_hops(1, (2, 3))
            start_nears(1, (2, 3))

        with jax.named_scope("second_block"):
            sweep(((0, w_three), (1, w_four)), ((1, w_two),), second_block, (hid[3], hid[2]), midway_two)
            start_hops(2, (2, 3))
            close_total(1, 0, wid[1], 3)
        start_hops(0, (1,))
        start_nears(0, (1,))
        start_nears(2, (2, 3))

        def first_backward(tile, slot, load):
            back = mm(acts[0], rows_v[load], True)
            out_tiles[slot] = rounded(back * gelu_parts(widened(a_one[tile]))[1])

        def midway_three():
            start_hops(1, (0,))
            start_nears(1, (0,))
            pass_on(1, (1,))
            pass_on(2, (1,))
            pass_on(0, (2,))

        with jax.named_scope("first_backward"):
            sweep(((1, w_two),), (), first_backward, (hid[0],), midway_three)
        start_hops(2, (0,))
        start_nears(2, (0,))

    width = wid_v.shape[-1]
    pl.run_scoped(
        products, pltpu.VMEM((lead + 1, width, bn), jnp.bfloat16), pltpu.VMEM((lead + 1, bn, width), jnp.bfloat16),
        pltpu.VMEM((3, rows, width), jnp.bfloat16), pltpu.VMEM((4, rows, bn), jnp.bfloat16), pltpu.VMEM((rows, width), jnp.float32),
        pltpu.VMEM((tiles, rows, bn), jnp.bfloat16))

    def sums(acc, ring1):
        def product(side, part, chunk, block, store):
            odd = lax.rem(pick(part, coord), 2)
            dims = (((0,), (0,)), ((), ()))

            @pl.when(odd == 1)
            def _():
                left = hid_v[side * PARTS + part, :, pl.ds(pl.multiple_of(chunk * bm, bm), bm)]
                right = wid_v[part, :, pl.ds(pl.multiple_of(block * bn, bn), bn)]
                store(lax.dot_general(left, right, dims, preferred_element_type=jnp.float32))

            @pl.when(odd == 0)
            def _():
                index = 3 * chunk + block
                left = wid_v[part, :, pl.ds(pl.multiple_of(lax.div(index, 2) * bm, bm), bm)]
                right = hid_v[side * PARTS + part, :, pl.ds(pl.multiple_of(lax.rem(index, 2) * bn, bn), bn)]
                store(lax.dot_general(left, right, dims, preferred_element_type=jnp.float32))

        def hand_over(part=0, chunk=0, block=0, slot=0):
            return pltpu.make_async_remote_copy(
                src_ref=stage.at[slot], dst_ref=acc.at[part, chunk, block], send_sem=stage_send.at[slot],
                recv_sem=stage_recv.at[part, chunk, block], device_id=partner, device_id_type=MESH)

        tell_neighbours(free_sem)
        with jax.named_scope("send_last"):
            pass_on(0, (1,))
            pass_on(1, (2, 3))
            pass_on(2, (2, 3))
            pass_on(1, (0,))
            for piece in range(PIECES):
                start_own(piece)
        with jax.named_scope("await_other"):
            pl.semaphore_wait(free_sem, 7)
            for piece in range(PIECES - 1):
                for part in range(PARTS):
                    arrived(piece, part)

        top, low = bm // 2, bm // 8

        def ring1_copy(part, direction, step, block):
            chunk = lax.rem(first[part] + round_by(direction, 1 + step), RING)
            return pltpu.make_async_remote_copy(
                src_ref=acc.at[part, chunk, block, pl.ds(direction * top, top)], dst_ref=ring1.at[part, direction, step, block],
                send_sem=r1_send.at[part, direction, block], recv_sem=r1_recv.at[part, direction, step, block],
                device_id=shifted((part + 1) % 3, direction), device_id_type=MESH)

        def place_of(count):
            part, rest = split(count, PARTS)
            early = rest < 2 * BLOCKS
            order = jnp.where(early, lax.rem(rest, 2), lax.div(rest, BLOCKS))
            block = jnp.where(early, lax.div(rest, 2), lax.rem(rest, BLOCKS))
            return order, part, lax.rem(pick(part, first) + pick(order, (3, 1, 2, 0)), RING), block

        blocks = CHUNKS * PARTS * BLOCKS

        def both_halves(count, carry):
            @pl.when(count < blocks)
            def _():
                _, part, chunk, block = place_of(count)
                slot = lax.rem(count, n_stage)

                @pl.when(count >= n_stage)
                def _():
                    hand_over(slot=slot).wait_send()

                def store(value):
                    stage[slot] = value

                product(0, part, chunk, block, store)
                hand_over(part, chunk, block, slot).start()

            @pl.when(count >= LAG)
            def _():
                order, part, chunk, block = place_of(count - LAG)
                hand_over(part, chunk, block).wait_recv()

                def store(value):
                    acc[part, chunk, block] = acc[part, chunk, block] + value

                product(1, part, chunk, block, store)
                for direction in WAYS:
                    for which in range(PARTS):
                        @pl.when((order == direction) & (part == which))
                        def _():
                            ring1_copy(which, direction, 0, block).start()

            return carry

        def ring1_step(step):
            for block in range(BLOCKS):
                for part in range(PARTS):
                    for direction in WAYS:
                        ring1_copy(part, direction, step, block).wait_recv()
                        chunk = lax.rem(first[part] + round_by(direction, 2 + step), RING)
                        share = acc.at[part, chunk, block, pl.ds(direction * top, top)]
                        share[...] = share[...] + ring1[part, direction, step, block]
                        ring1_copy(part, direction, step, block).wait_send()
                        if step < RING - 2:
                            ring1_copy(part, direction, step + 1, block).start()
                    if step == RING - 2:
                        for direction in WAYS:
                            ring2_copy(part, direction, 0, block).start()

        pass_on(2, (0,))
        with jax.named_scope("other_half"):
            lax.fori_loop(0, LAG, both_halves, 0)
        with jax.named_scope("await_own"):
            for part in range(PARTS):
                arrived(2, part)
        last = blocks - PARTS * BLOCKS
        with jax.named_scope("halves"):
            lax.fori_loop(LAG, last + LAG, both_halves, 0)
        def ring2_share(part, direction, block, place):
            row = pl.multiple_of(2 * low * place + direction * low, low)
            return acc.at[part, first[part], block, pl.ds(row, low)]

        def ring2_copy(part, direction, step, block):
            place = lax.rem(second[part] + round_by(direction, 1 + step), RING)
            return pltpu.make_async_remote_copy(
                src_ref=ring2_share(part, direction, block, place), dst_ref=ring2.at[part, direction, step, block],
                send_sem=r2_send.at[part, direction, block], recv_sem=r2_recv.at[part, direction, step, block],
                device_id=shifted((part + 2) % 3, direction), device_id_type=MESH)

        with jax.named_scope("ring1#step=0"):
            ring1_step(0)
        with jax.named_scope("last_chunk"):
            lax.fori_loop(last + LAG, blocks + LAG, both_halves, 0)
        for step in range(1, RING - 1):
            with jax.named_scope(f"ring1#step={step}"):
                ring1_step(step)

        with jax.named_scope("ring2"):
            for step in range(RING - 1):
                for block in range(BLOCKS):
                    for part in range(PARTS):
                        for direction in WAYS:
                            ring2_copy(part, direction, step, block).wait_recv()
                            place = lax.rem(second[part] + round_by(direction, 2 + step), RING)
                            share = ring2_share(part, direction, block, place)
                            value = share[...] + ring2[part, direction, step, block]
                            ring2_copy(part, direction, step, block).wait_send()
                            if step < RING - 2:
                                share[...] = value
                                ring2_copy(part, direction, step + 1, block).start()
                            else:
                                result[part, pl.ds(2 * low * block + direction * low, low)] = value * scale

        for slot in range(n_stage):
            hand_over(slot=slot).wait_send()

    pl.run_scoped(
        sums, pltpu.VMEM((PARTS, CHUNKS, BLOCKS, bm, bn), jnp.float32),
        pltpu.VMEM((PARTS, 2, RING - 1, BLOCKS, bm // 2, bn), jnp.float32))

    piece_rows = result.shape[1]
    cut = piece_rows // 16 * 8

    def after(place, by):
        return lax.rem(place + by, RING)

    def at(part, owner, chunk, quarter=None):
        view = gath.at[core, part, owner, chunk]
        return view if quarter is None else view.at[quarter]

    def send(src, dst, sem, recv, axis, direction):
        return pltpu.make_async_remote_copy(
            src_ref=src, dst_ref=dst, send_sem=sem, recv_sem=recv, device_id=shifted(axis, direction), device_id_type=MESH)

    def mine(part, chunk, quarter=None):
        view = own_out.at[part, chunk]
        return view if quarter is None else view.at[quarter]

    def quarter_copy(part, direction, leg):
        sem, recv = g_send.at[0, part], g1_recv.at[part, direction, leg]
        axis = (part + 2) % 3
        if leg == 0:
            return send(result.at[part], mine(part, first[part], second[part]), sem, recv, axis, direction)
        view = mine(part, first[part], after(second[part], 3 - 2 * direction))
        view = view.at[pl.ds(0, cut)] if direction == 0 else view.at[pl.ds(cut, piece_rows - cut)]
        return send(view, view, sem, recv, axis, direction)

    def chunk_copy(part, direction, leg):
        sem, recv = g_send.at[1, part], g2_recv.at[part, direction, leg]
        axis = (part + 1) % 3
        view = mine(part, first[part])
        if leg == 1:
            view = mine(part, after(first[part], 3 - 2 * direction), pl.ds(2 * direction, 2))
        return send(view, view, sem, recv, axis, direction)

    def owner_copy(part, direction, order, piece=None):
        chunk = after(first[part], ORDER[order])
        recv = g3_recv.at[part, direction, order + (piece or 0)]
        return send(mine(part, chunk, piece), at(part, coord[part], chunk, piece), g_send.at[2, part], recv, part, direction)

    def cross(part, owner, order, piece=None):
        view = at(part, owner, after(first[part], ORDER[order]), piece)
        return pltpu.make_async_remote_copy(
            src_ref=view, dst_ref=view, send_sem=cross_send, recv_sem=cross_recv, device_id=partner, device_id_type=MESH)

    def keep(part):
        return pltpu.make_async_copy(result.at[part], mine(part, first[part], second[part]), local_sem.at[part])

    final = CHUNKS - 1
    turns = [(order, part, direction) for order in range(final) for part in range(PARTS) for direction in WAYS]
    turns += [(final, part, direction) for direction in WAYS for part in range(PARTS)]

    def passing_in(turn):
        order, part, direction = turns[turn]
        view = at(part, beyond(part, 1 - direction), after(first[part], ORDER[order]), pl.ds(2 * direction, 2))
        slot = turn % 2
        return pltpu.make_async_copy(view, stage.at[pl.ds(2 * slot, 2), pl.ds(0, piece_rows)], pass_in.at[slot])

    def passing_out(turn):
        order, part, direction = turns[turn]
        chunk = after(first[part], ORDER[order])
        return [pltpu.make_async_copy(
            stage.at[2 * (turn % 2) + k, pl.ds(0, piece_rows)],
            passing[(2 * k + direction) * PARTS + part].at[chunk], pass_out.at[turn % 2, k]) for k in WAYS]

    def pass_further(turn):
        passing_in(turn).wait()
        for copy in passing_out(turn):
            copy.start()

    def passed(turn):
        for copy in passing_out(turn):
            copy.wait()

    with jax.named_scope("gather"):
        for part in range(PARTS):
            for direction in WAYS:
                quarter_copy(part, direction, 0).start()
            keep(part).start()
        for part in range(PARTS):
            for direction in WAYS:
                quarter_copy(part, direction, 0).wait_recv()
                quarter_copy(part, direction, 1).start()
        for part in range(PARTS):
            keep(part).wait()
            for direction in WAYS:
                quarter_copy(part, direction, 1).wait_recv()
            for direction in WAYS:
                chunk_copy(part, direction, 0).start()
            for direction in WAYS:
                owner_copy(part, direction, 0).start()
        for part in range(PARTS):
            for direction in WAYS:
                chunk_copy(part, direction, 0).wait_recv()
                chunk_copy(part, direction, 1).start()
            for order in (1, 2):
                for direction in WAYS:
                    owner_copy(part, direction, order).start()
        for part in range(PARTS):
            for direction in WAYS:
                chunk_copy(part, direction, 1).wait_recv()
            for direction in WAYS:
                for piece in range(RING):
                    owner_copy(part, direction, final, piece).start()
        def pass_start(turn):
            if turn > 1:
                passed(turn - 2)
            passing_in(turn).start()
            if turn > 0:
                pass_further(turn - 1)

        for order in range(final):
            for part in range(PARTS):
                for direction in WAYS:
                    owner_copy(part, direction, order).wait_recv()
                    cross(part, beyond(part, 1 - direction), order).start()
                    pass_start(turns.index((order, part, direction)))
        for piece in range(RING):
            for part in range(PARTS):
                for direction in WAYS:
                    owner_copy(part, direction, final, piece).wait_recv()
                    cross(part, beyond(part, 1 - direction), final, piece).start()
                    if piece == 2 * direction + 1:
                        pass_start(turns.index((final, part, direction)))
        pass_further(len(turns) - 1)
        for turn in range(len(turns) - 2, len(turns)):
            passed(turn)

    for piece in range(PIECES):
        for part in range(PARTS):
            for direction in WAYS:
                near(piece, part, direction).wait_send()
                hop(piece, part, direction).wait_send()
                forward(piece, part, direction).wait_send()

    def drain(view, sem):
        pltpu.make_async_copy(view, view, sem).wait()

    for part in range(PARTS):
        drain(gath.at[core, part, 0, 0, pl.ds(0, 3)], g_send.at[0, part])
        drain(gath.at[core, part, 0, pl.ds(0, 3)], g_send.at[1, part])
        drain(gath.at[core, part, pl.ds(0, 2)], g_send.at[2, part])
    drain(gath.at[core, :, pl.ds(0, 2)], cross_send)
    drain(gath.at[1 - core, :, pl.ds(0, 2)], cross_recv)


def reduce_grads(x_loc, g_loc, weights, n_dev):
    rows, width = x_loc.shape
    bm = width // 6
    bn = 2 * bm
    dma = pltpu.SemaphoreType.DMA
    any_spec = pl.BlockSpec(memory_space=pl.ANY)
    f32, bf16 = jnp.float32, jnp.bfloat16
    n_stage = 4
    piece_rows = BLOCKS * (bm // 4)
    outs = pl.pallas_call(
        functools.partial(reduce_kernel, rows, bm, 1.0 / n_dev),
        name="reduce_grads",
        out_shape=[
            jax.ShapeDtypeStruct((2, PARTS, RING, CHUNKS, RING, piece_rows, bn), f32),
            jax.ShapeDtypeStruct((PARTS, CHUNKS, RING, piece_rows, bn), f32),
            jax.ShapeDtypeStruct((PARTS, 2, rows // 2, width), bf16),
            jax.ShapeDtypeStruct((2, PARTS, 2, rows // 2, 4 * bm), bf16),
            jax.ShapeDtypeStruct((4, rows, 24 * bm), bf16),
            jax.ShapeDtypeStruct((2, rows, width), bf16),
            *[jax.ShapeDtypeStruct((CHUNKS, piece_rows, bn), f32)] * (4 * PARTS),
        ],
        in_specs=[any_spec] * 6,
        out_specs=[any_spec] * (6 + 4 * PARTS),
        scratch_shapes=[
            pltpu.VMEM((2 * PARTS, RING * rows, 4 * bm), bf16),
            pltpu.VMEM((PARTS, RING * rows, width), bf16),
            pltpu.VMEM((n_stage, bm, bn), f32),
            pltpu.VMEM((PARTS, 2, RING - 1, BLOCKS, bm // 8, bn), f32),
            pltpu.VMEM((PARTS, piece_rows, bn), f32),
            pltpu.SemaphoreType.REGULAR, dma((4,)), dma((2, LEAD + 1)), dma((4,)),
            dma((PIECES, PARTS)),
            *[dma((PIECES, PARTS, 2))] * 6,
            dma((n_stage,)), dma((PARTS, CHUNKS, BLOCKS)),
            dma((PARTS, 2, BLOCKS)), dma((PARTS, 2, RING - 1, BLOCKS)),
            dma((PARTS, 2, BLOCKS)), dma((PARTS, 2, RING - 1, BLOCKS)),
            dma((PARTS,)), dma((2,)), dma((2, 2)), dma((3, PARTS)),
            dma((PARTS, 2, 2)), dma((PARTS, 2, 2)), dma((PARTS, 2, CHUNKS + RING - 1)),
            dma, dma,
        ],
        compiler_params=pltpu.CompilerParams(collective_id=0, has_side_effects=True, vmem_limit_bytes=67043328),
        cost_estimate=pl.CostEstimate(flops=40 * rows * 24 * bm * width, bytes_accessed=200_000_000, transcendentals=0),
    )(x_loc, g_loc, *weights)
    return outs[0], outs[1], outs[6:]


def place_kernel(begin, end, depth, start_load, like, spots, n_src, *refs):
    srcs, dsts = refs[:n_src], refs[-7:-3]
    slots, in_sem, out_sem = refs[-3:]
    ahead = depth // 2

    def load(turn):
        slot = lax.rem(turn, depth)
        start_load(srcs, turn, slots.at[slot], in_sem.at[slot])

    def settle(turn, sem):
        slot = lax.rem(turn, depth)
        pltpu.make_async_copy(like(srcs), slots.at[slot], sem.at[slot]).wait()

    def store(turn):
        slot = lax.rem(turn, depth)
        owner, part, core, pieces = spots(turn)
        bn = slots.shape[-1]
        quarter_rows = bn // 8
        for which in range(RING):
            @pl.when(owner == which)
            def _():
                for k, (chunk, quarter) in enumerate(pieces):
                    for block in range(BLOCKS):
                        rows, cols = spot(bn // 2, which, part, core, chunk, quarter, block)
                        pltpu.make_async_copy(
                            slots.at[slot, k, pl.ds(block * quarter_rows, quarter_rows)], dsts[which].at[rows, cols], out_sem.at[slot]).start()

    def prime(turn, carry):
        load(turn)
        return carry

    def body(turn, carry):
        @pl.when(turn + ahead < end)
        def _():
            @pl.when(turn + ahead >= begin + depth)
            def _():
                settle(turn + ahead - depth, out_sem)

            load(turn + ahead)

        settle(turn, in_sem)
        store(turn)
        return carry

    def finish(turn, carry):
        settle(turn, out_sem)
        return carry

    lax.fori_loop(begin, begin + ahead, prime, 0)
    lax.fori_loop(begin, end, body, 0)
    lax.fori_loop(end - depth, end, finish, 0)


def spot(bm, which, part, core, chunk, quarter, block):
    bn = 2 * bm
    if which % 2:
        start = (8 * part + 4 * core + chunk) * bm
        col = block * bn
    else:
        index = 3 * chunk + block
        start = lax.div(index, 2) * bm
        col = (4 * part + 2 * core + lax.rem(index, 2)) * bn
    rows = bm // 4
    return pl.ds(pl.multiple_of(start + quarter * rows, rows), rows), pl.ds(pl.multiple_of(col, bn), bn)


def where_am_i():
    z, y, xc = lax.axis_index("z"), lax.axis_index("y"), lax.axis_index("xc")
    return (lax.div(xc, 2), y, z), lax.rem(xc, 2)


def place_kept(gathered, whole, group, shapes, earlier=()):
    lead = PARTS * CHUNKS * 2

    def unpack(turn):
        coords, core = where_am_i()
        half, rest = split(turn, 2)
        chunk, rest = split(rest, CHUNKS)
        part, rest = split(rest, PARTS)
        near = rest - 1
        by = jnp.where(near < 0, 0, 1 + 2 * near)
        source = jnp.where(near < 0, jnp.where(group == 0, core, 1 - core), group)
        return near, source, part, lax.rem(pick(part, coords) + by, RING), chunk, half

    def start_load(srcs, turn, slot, sem):
        near, core, part, owner, chunk, half = unpack(turn)

        @pl.when(near < 0)
        def _():
            pltpu.make_async_copy(srcs[1].at[part, chunk, pl.ds(2 * half, 2)], slot, sem).start()

        @pl.when(near >= 0)
        def _():
            pltpu.make_async_copy(srcs[0].at[core, part, owner, chunk, pl.ds(2 * half, 2)], slot, sem).start()

    def spots(turn):
        _, core, part, owner, chunk, half = unpack(turn)
        return owner, part, core, [(chunk, 2 * half + k) for k in WAYS]

    return place((gathered, whole), shapes, 0, 3 * lead, start_load, lambda srcs: srcs[1].at[0, 0, pl.ds(0, 2)], spots, earlier)


def place_passed(arrays, group, shapes, earlier):
    def start_load(srcs, turn, slot, sem):
        for k, src in enumerate(srcs):
            @pl.when(lax.div(turn, 2) == k)
            def _():
                pltpu.make_async_copy(src.at[pl.ds(2 * lax.rem(turn, 2), 2)], slot, sem).start()

    def spots(turn):
        coords, core = where_am_i()
        pair, rest = split(turn, 2)
        part, rest = split(rest, PARTS)
        way, other = split(rest, 2)
        owner = lax.rem(pick(part, coords) + 2, RING)
        return owner, part, jnp.where(other == 0, core, 1 - core), [(2 * pair + k, group + 2 * way) for k in WAYS]

    return place(arrays, shapes, 0, 2 * len(arrays), start_load, lambda srcs: srcs[0].at[pl.ds(0, 2)], spots, earlier)


def place(srcs, shapes, begin, end, start_load, like, spots, earlier):
    depth = 16
    piece_rows, bn = srcs[0].shape[-2:]
    moved = (end - begin) * 2 * piece_rows * bn
    return pl.pallas_call(
        functools.partial(place_kernel, begin, end, depth, start_load, like, spots, len(srcs)),
        name="place_grads",
        out_shape=[jax.ShapeDtypeStruct(s, jnp.float32) for s in shapes],
        in_specs=[pl.BlockSpec(memory_space=pl.ANY)] * (len(srcs) + len(earlier)),
        out_specs=[pl.BlockSpec(memory_space=pl.ANY)] * 4,
        scratch_shapes=[pltpu.VMEM((depth, 2, piece_rows, bn), jnp.float32), pltpu.SemaphoreType.DMA((depth,)), pltpu.SemaphoreType.DMA((depth,))],
        input_output_aliases={len(srcs) + k: k for k in range(len(earlier))},
        cost_estimate=pl.CostEstimate(flops=16 * moved, bytes_accessed=8 * moved, transcendentals=0),
    )(*srcs, *earlier)


def solution(mesh):
    n_dev = math.prod(mesh.shape.values())
    axes = ("z", "y", "xc")
    batch_spec = P(axes, None)
    whole_spec = P(None, None)

    def device_step(x_loc, g_loc, w_one, w_two, w_three, w_four):
        gathered, whole, passing = reduce_grads(x_loc, g_loc, (w_one, w_two, w_three, w_four), n_dev)
        shapes = (w_one.shape, w_two.shape, w_three.shape, w_four.shape)
        rings = [("xc", mesh.shape["xc"], 2), ("y", RING, 1), ("z", RING, 1)]
        cores = [(k, k ^ 1) for k in range(mesh.shape["xc"])]
        across = lax.ppermute(whole, "xc", cores)
        arrived = []
        for group in WAYS:
            arrived.append([])
            for way in WAYS:
                for part, (name, size, stride) in enumerate(rings):
                    step = stride if way == 0 else size - stride
                    source = passing[(2 * group + way) * PARTS + part]
                    arrived[group].append(lax.ppermute(source, name, [(k, (k + step) % size) for k in range(size)]))
        swapped = []
        grads = ()
        for group in WAYS:
            grads = place_kept(gathered, (whole, across)[group], group, shapes, grads)
            *grads, arrived[group], across = lax.optimization_barrier((*grads, arrived[group], across))
            swapped.append([lax.ppermute(a, "xc", cores) for a in arrived[group]])
        for group in WAYS:
            grads = place_passed((*arrived[group], *swapped[group]), group, shapes, grads)
        return tuple(grads)

    return jax.shard_map(
        device_step,
        mesh=mesh,
        in_specs=(batch_spec, batch_spec, whole_spec, whole_spec, whole_spec, whole_spec),
        out_specs=(whole_spec, whole_spec, whole_spec, whole_spec),
        check_vma=False,
    )
```
